256 devices in a mesh: slab: 128 (over y, x, z_hi, core), cell: 2 (over z_lo).
Axes of the slice: x: 4, y: 4, z: 8 (z_hi: 4, z_lo: 2; z = z_hi * 2 + z_lo), core: 2. Of those that a mesh axis runs over, the one named last changes fastest.
Arguments:
- cell_row: int32 [131072], P(('slab', 'cell')), may hold values from 0 to 2043, as said below
- cell_col: int32 [131072], P(('slab', 'cell')), may hold values from 0 to 2039
- cell_width: int32 [131072], P(('slab', 'cell')), may hold values from 1 to 8
- cell_height: int32 [131072], P(('slab', 'cell')), may hold values from 1 to 4
- cell_region: int32 [131072], P(('slab', 'cell')), may hold values from 0 to 3
- cell_offset: float32 [2, 131072], P(None, ('slab', 'cell')), may hold values from 0 to 1
Outputs:
- field_x: float32 [4, 2048, 2048], P(None, ('slab', 'cell'))
- field_y: float32 [4, 2048, 2048], P(None, ('slab', 'cell'))
- cell_force: float32 [2, 131072], P(None, ('slab', 'cell'))
- energy: float32 [], replicated
- overflow: float32 [], replicated
The draws below stay inside these ranges and needn't reach their ends.
Inputs may be any that keep to these rules, and one draw needn't show every extreme that they name: `cell_row`: cell i belongs to row slab s = i // 1024: its row lies in [s * 16, (s + 1) * 16); cells of the last slab lie at least 4 rows below the top of the grid.
All inputs are finite; a program needn't handle non-finite values.
Results may differ from the reference program's by a relative error of at most 0.0015.
Values may be sent and summed in bfloat16 or wider, within the bound.
A program may use at most 128 MiB of HBM per device.

```python
import jax
import jax.numpy as jnp
from jax import lax

M = 2048
REGIONS = 4
HMAX = 4
WMAX = 8
ROWS = 16
CELLS_SLAB = 1024
CELLS = 131072


def draw_cell_row(key, part):
    positions = jnp.arange(CELLS, dtype=jnp.int32)
    slab_index = positions // CELLS_SLAB
    top_slab = M // ROWS - 1
    row_room = jnp.where(slab_index == top_slab, ROWS - HMAX, ROWS)
    random_bits = jax.random.randint(key, (CELLS,), 0, 1 << 20, dtype=jnp.int32)
    offset_rows = jnp.where(positions == top_slab * CELLS_SLAB, row_room - 1, random_bits % row_room)
    return (slab_index * ROWS + offset_rows).astype(jnp.int32)


def draw_cell_width(key, part):
    slab_count = M // ROWS
    key_cap, key_pick, key_width = jax.random.split(jax.random.fold_in(key, 7), 3)
    slab_caps = 1 + jax.random.randint(key_cap, (slab_count,), 0, WMAX, dtype=jnp.int32)
    widest = jax.random.randint(key_pick, (), 0, slab_count, dtype=jnp.int32)
    slab_caps = jnp.where(jnp.arange(slab_count, dtype=jnp.int32) == widest, WMAX, slab_caps)
    positions = jnp.arange(CELLS, dtype=jnp.int32)
    owner_slab = positions // CELLS_SLAB
    random_bits = jax.random.randint(key_width, (CELLS,), 0, 1 << 20, dtype=jnp.int32)
    widths = 1 + random_bits % slab_caps[owner_slab]
    return jnp.where(positions == widest * CELLS_SLAB, WMAX, widths).astype(jnp.int32)


def set_ends(values, key, least, top_value):
    spot = [jax.random.randint(jax.random.fold_in(key, axis), (), 0, length) for axis, length in enumerate(values.shape)]
    widest = values.shape.index(max(values.shape))
    neighbour = spot[:widest] + [(spot[widest] + 1) % values.shape[widest]] + spot[widest + 1:]
    return values.at[tuple(spot)].set(least).at[tuple(neighbour)].set(top_value)


def block_scale(key, shape, cuts, low, largest):
    def one(axis_at, blocks):
        draws = jax.random.uniform(jax.random.fold_in(jax.random.fold_in(key, 6), axis_at), (blocks,), jnp.float32, low / len(cuts), largest / len(cuts))
        return jnp.repeat(jnp.exp(draws), shape[axis_at] // blocks).reshape((-1,) + (1,) * (len(shape) - axis_at - 1))

    gain = one(*cuts[0])
    for cut in cuts[1:]:
        gain = gain * one(*cut)
    return gain


def setup_inputs(seed: int = 0) -> dict:
    key_list = jax.random.split(jax.random.key(seed), 7)
    cell_row = draw_cell_row(jax.random.fold_in(key_list[6], 71), 0)
    cell_col = set_ends(jax.random.randint(key_list[1], (CELLS,), 0, M - WMAX), jax.random.fold_in(key_list[1], 1), 0, (M - WMAX) - 1).astype(jnp.int32)
    cell_width = draw_cell_width(jax.random.fold_in(key_list[6], 71), 0)
    cell_height = set_ends(jax.random.randint(key_list[3], (CELLS,), 1, HMAX + 1), jax.random.fold_in(key_list[3], 1), 1, HMAX).astype(jnp.int32)
    cell_region = set_ends(jax.random.randint(key_list[4], (CELLS,), 0, REGIONS), jax.random.fold_in(key_list[4], 1), 0, REGIONS - 1).astype(jnp.int32)
    cell_offset = jnp.clip(1.0 * jax.random.uniform(key_list[5], (2, CELLS), jnp.float32) ** block_scale(key_list[5], (2, CELLS), ((1, 256),), -0.2, 0.2), 0.0, 1.0)
    return dict(cell_row=cell_row, cell_col=cell_col, cell_width=cell_width, cell_height=cell_height, cell_region=cell_region, cell_offset=cell_offset)


def intersect(offset_bins, fraction, extent):
    high_edge = jnp.minimum(offset_bins + 1.0, fraction + extent)
    low_edge = jnp.maximum(offset_bins, fraction)
    return jnp.maximum(high_edge - low_edge, 0.0).astype(jnp.bfloat16)

def basis_weight(length):
    freq_index = jnp.arange(length)
    return jnp.where(freq_index == 0, jnp.sqrt(1.0 / length), jnp.sqrt(2.0 / length)).astype(jnp.float32)

def dct_forward(values, axis):
    length = values.shape[axis]
    moved = jnp.moveaxis(values, axis, -1)
    doubled = jnp.concatenate([moved, jnp.flip(moved, -1)], axis=-1)
    spectral = jnp.fft.fft(doubled, axis=-1)[..., :length]
    freq_axis = jnp.arange(length).astype(jnp.float32)
    twist = jnp.exp(-1j * (jnp.pi / (2 * length)) * freq_axis)
    result = jnp.real(spectral * twist) * (0.5 * basis_weight(length))
    return jnp.moveaxis(result, -1, axis)

def dct_inverse(values, axis, sine):
    length = values.shape[axis]
    moved = jnp.moveaxis(values, axis, -1)
    freq_axis = jnp.arange(length).astype(jnp.float32)
    twisted = moved * basis_weight(length) * jnp.exp(1j * (jnp.pi / (2 * length)) * freq_axis)
    padded = jnp.concatenate([twisted, jnp.zeros_like(twisted)], axis=-1)
    summed = jnp.fft.ifft(padded, axis=-1)[..., :length] * (2 * length)
    picked = jnp.imag(summed) if sine else jnp.real(summed)
    return jnp.moveaxis(picked, -1, axis)

def reference(cell_row, cell_col, cell_width, cell_height, cell_region, cell_offset):
    span_x = jnp.arange(WMAX + 1)
    span_y = jnp.arange(HMAX + 1)
    x_intersect = intersect(span_x[None, :].astype(jnp.float32), cell_offset[0][:, None], cell_width.astype(jnp.float32)[:, None])
    y_intersect = intersect(span_y[None, :].astype(jnp.float32), cell_offset[1][:, None], cell_height.astype(jnp.float32)[:, None])
    weight = y_intersect.astype(jnp.float32)[:, :, None] * x_intersect.astype(jnp.float32)[:, None, :]
    row_index = jnp.broadcast_to(cell_row[:, None, None] + span_y[None, :, None], weight.shape)
    col_index = jnp.broadcast_to(cell_col[:, None, None] + span_x[None, None, :], weight.shape)
    region_index = jnp.broadcast_to(cell_region[:, None, None], weight.shape)
    density = jnp.zeros((REGIONS, M, M), jnp.float32).at[region_index, row_index, col_index].add(weight)
    overflow = jnp.sum(jnp.maximum(density - 1.0, 0.0)) / jnp.sum(density)
    spectrum = dct_forward(dct_forward(density, 2), 1)
    freq_axis = jnp.arange(M).astype(jnp.float32)
    p_grid = freq_axis[:, None]
    q_grid = freq_axis[None, :]
    anchor = jnp.arange(M)[:, None] + jnp.arange(M)[None, :] == 0
    step_size = jnp.pi / M
    squared = p_grid * p_grid + q_grid * q_grid
    potential_hat = jnp.where(anchor, 0.0, spectrum / (step_size * step_size * jnp.where(anchor, 1.0, squared)))
    field_x = dct_inverse(dct_inverse(potential_hat * (step_size * q_grid), 2, True), 1, False)
    field_y = dct_inverse(dct_inverse(potential_hat * (step_size * p_grid), 2, False), 1, True)
    potential = dct_inverse(dct_inverse(potential_hat, 2, False), 1, False)
    energy = jnp.sum(density * potential) / (M * M)
    rounded_x = lax.optimization_barrier(field_x.astype(jnp.bfloat16)).astype(jnp.float32)
    rounded_y = lax.optimization_barrier(field_y.astype(jnp.bfloat16)).astype(jnp.float32)
    force_x = lax.optimization_barrier(jnp.sum(weight * rounded_x[region_index, row_index, col_index], axis=(1, 2)))
    force_y = lax.optimization_barrier(jnp.sum(weight * rounded_y[region_index, row_index, col_index], axis=(1, 2)))
    return (field_x, field_y, jnp.stack([force_x, force_y]), energy, overflow)
```

```python
import functools
import math

import jax
import jax.numpy as jnp
import numpy as np
from jax import lax
from jax.experimental import pallas as pl
from jax.experimental.pallas import tpu as pltpu
from jax.sharding import PartitionSpec as P

M = 2048
REGIONS = 4
SLABS = 128
CELLS_DEV = 512
BF = jnp.bfloat16
F32 = jnp.float32
MESH = pl.DeviceIdType.MESH
STEP = math.pi / M
R2 = math.sqrt(0.5)


def split_np(table):
    high = table.astype(np.float32).astype(BF)
    low = (table - high.astype(np.float64)).astype(np.float32).astype(BF)
    return np.stack([high, low])


def lanes_of(per_group, width):
    return np.repeat(per_group, width, axis=-1)


@functools.lru_cache(None)
def tables():
    pi = np.pi
    k2 = np.arange(64)[:, None]
    b = np.arange(128)[None, :]
    c1, s1 = np.cos(pi * k2 * (2 * b + 1) / 128), np.sin(pi * k2 * (2 * b + 1) / 128)
    c2, s2 = np.cos(pi * (k2 + 1) * (2 * b + 1) / 128), np.sin(pi * (k2 + 1) * (2 * b + 1) / 128)
    cm, sm = np.cos(pi * (2 * k2 + 1) * (2 * b + 1) / 256), np.sin(pi * (2 * k2 + 1) * (2 * b + 1) / 256)
    zero = np.zeros_like(c1)
    wc = np.block([[c1, s1], [c2, -s2]])
    wc0 = np.block([[c1, zero], [zero, cm]])
    ws = np.block([[s1, -c1], [s2, c2]])
    ws0 = np.block([[s1, zero], [zero, sm]])
    w_fwd = np.stack([split_np(wc), split_np(wc0)])
    w_inv = np.stack([split_np(w.T) for w in (ws, ws0, wc, wc0)]).reshape(2, 2, 2, 256, 128)
    kap = np.arange(16)
    ang = pi * kap[None, :] * (2 * np.arange(128)[:, None] + 1) / 4096
    tx = np.stack([lanes_of(np.cos(ang), 32), lanes_of(np.sin(ang), 32)]).astype(np.float32)
    a = np.arange(16)[:, None]
    j = np.arange(4)[None, :]
    wa = np.concatenate([np.cos(2 * pi * a * j / 32), np.sin(2 * pi * a * j / 32)])
    wa = lanes_of(wa, 32).astype(np.float32)
    p1 = np.arange(256)[:, None]
    d = np.arange(256)[None, :]
    cre, cim = np.cos(2 * pi * p1 * d / 512), -np.sin(2 * pi * p1 * d / 512)
    cim[0] = (-1.0) ** np.arange(256)
    cy = np.concatenate([cre, cim], 0)
    cy_fwd, cy_inv = split_np(cy), split_np(cy.T)
    r = np.arange(8)
    angy = pi * p1 * (2 * r[None, :] + 1) / 4096
    ty = np.stack([np.tile(np.cos(angy), (1, 16)), np.tile(np.sin(angy), (1, 16))]).astype(np.float32)
    p2 = np.arange(4)[None, :]
    rr = r[:, None]
    e0, e1 = pi * p2 * (2 * rr + 1) / 8, pi * (p2 + 1) * (2 * rr + 1) / 8
    em = pi * (2 * rr + 1) * (1 + 2 * p2) / 16
    z8 = np.zeros((8, 4))
    bc = (np.block([np.cos(e0), np.cos(e1)]), np.block([np.sin(e0), -np.sin(e1)]))
    bc0 = (np.block([np.cos(e0), z8]), np.block([z8, np.cos(em)]))
    bs = (np.block([np.sin(e0), np.sin(e1)]), np.block([-np.cos(e0), np.cos(e1)]))
    bs0 = (np.block([np.sin(e0), z8]), np.block([z8, np.sin(em)]))

    def wide(pair):
        return np.concatenate([np.kron(np.eye(16), part) for part in pair], 0)

    b_fwd = np.stack([split_np(wide(bc)), split_np(wide(bc0))])
    b_inv = np.stack([split_np(wide(m).T) for m in (bc, bc0, bs, bs0)]).reshape(2, 2, 2, 128, 256)
    join = np.tile(np.eye(32), (1, 4)).astype(np.float32).astype(BF)
    return w_fwd, w_inv, tx, wa, cy_fwd, cy_inv, ty, b_fwd, b_inv, join


def dot(x, y):
    return lax.dot_general(x, y, (((1,), (0,)), ((), ())), preferred_element_type=F32)


def dot_nt(x, y):
    return lax.dot_general(x, y, (((1,), (1,)), ((), ())), preferred_element_type=F32)


def split(x):
    high = x.astype(BF)
    return high, (x - high.astype(F32)).astype(BF)


def dot3(x, y):
    return dot(x[0], y[0]) + (dot(x[0], y[1]) + dot(x[1], y[0]))


def place():
    slab = lax.axis_index("slab")
    cell = lax.axis_index("cell")
    return slab, cell, lax.div(slab, 8), lax.rem(slab, 8) * 2 + cell


def device_at(plane, column):
    return (plane * 8 + lax.div(column, 2), lax.rem(column, 2))


def overlap(bins, low, high):
    return jnp.maximum(jnp.minimum(bins + 1.0, high) - jnp.maximum(bins, low), 0.0)


def kernel(
    cellp, w_fwd, w_inv, tx, wa, cy_fwd, cy_inv, ty, b_fwd, b_inv, join,
    field_x, field_y, force, sums,
    cb, xb, yr, d4, zs, s1, r1, us, vs, gs, s2, r2, ps, fb, pf, pr, e1, e2, es,
    col_sem, cell_s, cell_r, a1_s, a1_r, a2_s, a2_r, f_s, f_r, e_s, e_r,
):
    slab, cell, plane, column = place()
    me = plane * 16 + column
    has_prev = jnp.logical_and(cell == 0, slab > 0)
    barrier = pltpu.get_barrier_semaphore()

    def signal_at(sem, device):
        pl.semaphore_signal(sem, inc=1, device_id=device, device_id_type=MESH)

    for i in range(1, 16):
        signal_at(barrier, device_at(lax.rem(plane + i, 16), column))
        signal_at(barrier, device_at(plane, lax.rem(column + i, 16)))

    @pl.when(has_prev)
    def _():
        signal_at(barrier, (slab - 1, 0))
        signal_at(barrier, (slab - 1, 1))

    cb[cell] = cellp[...]

    def make_cells(slot):
        values = cb[slot]

        def rows(i, carry):
            base = i * 128
            bins = (lax.broadcasted_iota(jnp.int32, (128, 128), 0) + base).astype(F32)
            for block in range(4):
                part = values[:, block * 128 : block * 128 + 128]
                got = overlap(bins - part[0:1], part[1:2], part[2:3])
                xb[slot, pl.ds(pl.multiple_of(base, 128), 128), block * 128 : block * 128 + 128] = got.astype(BF)
            return carry

        lax.fori_loop(0, 16, rows, 0)
        low_row = slab * 16 + cell * 8
        bins = (lax.broadcasted_iota(jnp.int32, (8, CELLS_DEV), 0) + low_row).astype(F32)
        got = overlap(bins - values[3:4], values[4:5], values[5:6])
        for g in range(REGIONS):
            yr[slot, 8 * g : 8 * g + 8, :] = jnp.where(values[6:7] == float(g), got, 0.0)

    def add_density(slot, fresh):
        rows = yr[slot].astype(BF)
        rows = jnp.concatenate([rows] * 4, axis=0)
        for i in range(4):
            at = slice(512 * i, 512 * i + 512)
            got = dot_nt(xb[slot, at, :], rows)
            if fresh:
                d4[at, :] = got
            else:
                d4[at, :] += got

    mine, other = cell, 1 - cell
    make_cells(mine)
    has_next = slab < SLABS - 1
    pl.semaphore_wait(barrier, 30 + has_next.astype(jnp.int32))
    for i in range(1, 16):
        signal_at(col_sem, device_at(plane, lax.rem(column + i, 16)))

    def send(src, dst, s_sem, r_sem, device):
        return pltpu.make_async_remote_copy(
            src_ref=src, dst_ref=dst, send_sem=s_sem, recv_sem=r_sem, device_id=device, device_id_type=MESH
        )

    to_partner = send(cellp, cb.at[cell], cell_s.at[0], cell_r.at[cell], (slab, other))
    to_next = send(cellp, cb.at[2 + cell], cell_s.at[1], cell_r.at[2 + cell], (slab + 1, 0))
    to_partner.start()

    @pl.when(has_next)
    def _():
        to_next.start()

    add_density(mine, True)
    send(cellp, cb.at[other], cell_s.at[0], cell_r.at[other], (slab, other)).wait_recv()
    make_cells(other)
    add_density(other, False)

    @pl.when(has_prev)
    def _():
        for k in range(2):
            send(cellp, cb.at[2 + k], cell_s.at[0], cell_r.at[2 + k], (slab, other)).wait_recv()
            make_cells(2 + k)
            add_density(2 + k, False)

    def tally(i, carry):
        excess, area = carry
        got = d4[pl.ds(pl.multiple_of(i * 64, 64), 64), :].reshape(8, 8, 128)
        return excess + jnp.sum(jnp.maximum(got - 1.0, 0.0), axis=0), area + jnp.sum(got, axis=0)

    zero8 = jnp.zeros((8, 128), F32)
    excess, area = lax.fori_loop(0, 32, tally, (zero8, zero8))

    lane = lax.broadcasted_iota(jnp.int32, (1, 128), 1)
    first_group = lane < 32
    group_mask = first_group.astype(F32)

    def x_chunk(i, carry):
        at = pl.multiple_of(i * 16, 16)
        d = [d4[pl.ds(pl.multiple_of(128 * a + at, 16), 16), :] for a in range(16)]
        er = [d[m] * wa[m : m + 1, :] + d[m + 8] * wa[m + 8 : m + 9, :] for m in range(8)]
        ei = [-(d[m] * wa[16 + m : 17 + m, :] + d[m + 8] * wa[24 + m : 25 + m, :]) for m in range(8)]
        sr = [er[m] + er[m + 4] for m in range(4)]
        si = [ei[m] + ei[m + 4] for m in range(4)]
        tr = [er[m] - er[m + 4] for m in range(4)]
        ti = [ei[m] - ei[m + 4] for m in range(4)]
        ur = [tr[0], (tr[1] + ti[1]) * R2, ti[2], (ti[3] - tr[3]) * R2]
        ui = [ti[0], (ti[1] - tr[1]) * R2, -tr[2], -(tr[3] + ti[3]) * R2]

        def ends(re, im):
            ar, ai, br, bi = re[0] + re[2], im[0] + im[2], re[1] + re[3], im[1] + im[3]
            cr, ci, dr, di = re[0] - re[2], im[0] - im[2], re[1] - re[3], im[1] - im[3]
            return (ar + br, ai + bi), (cr + di, ci - dr), ar - br

        y0, y2, alternate = ends(sr, si)
        y1, y3, _ = ends(ur, ui)
        y0 = (y0[0], y0[1] + alternate * group_mask)
        for t, (re, im) in enumerate((y0, y1, y2, y3)):
            lanes = slice(128 * t, 128 * t + 128)
            c, s = tx[0, pl.ds(at, 16), lanes], tx[1, pl.ds(at, 16), lanes]
            for half, value in enumerate((re * c + im * s, im * c - re * s)):
                high, low = split(value)
                zs[0, pl.ds(half * 128 + at, 16), lanes] = high
                zs[1, pl.ds(half * 128 + at, 16), lanes] = low
        return carry

    lax.fori_loop(0, 8, x_chunk, 0)
    for t in range(4):
        lanes = slice(128 * t, 128 * t + 128)
        z = (zs[0, 0:256, lanes], zs[1, 0:256, lanes])
        got = dot3((w_fwd[0, 0], w_fwd[0, 1]), z)
        if t == 0:
            got = jnp.where(first_group, dot3((w_fwd[1, 0], w_fwd[1, 1]), z), got)
        s1[t // 2, 128 * (t % 2) : 128 * (t % 2) + 128, :] = got

    pl.semaphore_wait(col_sem, 15)

    def exchange(src, dst, s_sem, r_sem):
        def to(i, k):
            there, across = lax.rem(plane + i, 16), lax.rem(column + k, 16)
            send(
                src.at[:, there * 16 + across], dst.at[:, me], s_sem, r_sem, device_at(there, across)
            ).start()

        def planes(i, carry):
            for k in range(16):
                to(i, k)
            return carry

        lax.fori_loop(1, 16, planes, 0)
        for k in range(1, 16):
            to(0, k)
        dst[:, pl.ds(me, 1), :] = src[:, pl.ds(me, 1), :]

    def exchange_wait(src, dst, s_sem, r_sem):
        whole = send(src.at[:, pl.ds(0, 255)], dst.at[:, pl.ds(0, 255)], s_sem, r_sem, (slab, other))
        whole.wait_recv()
        whole.wait_send()

    exchange(s1, r1, a1_s, a1_r)
    exchange_wait(s1, r1, a1_s, a1_r)

    high, low = zip(*(split(r1[h]) for h in range(2)))
    whole = (jnp.concatenate(high, axis=1), jnp.concatenate(low, axis=1))
    us[...] = dot3((cy_fwd[0], cy_fwd[1]), whole)

    def y_chunk(i, carry):
        at = pl.multiple_of(i * 16, 16)
        c, s = ty[0, pl.ds(at, 16), :], ty[1, pl.ds(at, 16), :]
        for h in range(2):
            lanes = slice(128 * h, 128 * h + 128)
            re, im = us[pl.ds(at, 16), lanes], us[pl.ds(256 + at, 16), lanes]
            for half, value in enumerate((re * c + im * s, im * c - re * s)):
                parts = split(value)
                for k in range(2):
                    vs[k, pl.ds(256 * h + at, 16), 128 * half : 128 * half + 128] = parts[k]
        return carry

    lax.fori_loop(0, 16, y_chunk, 0)
    gs[...] = dot3((vs[0, 0:512], vs[1, 0:512]), (b_fwd[0, 0], b_fwd[0, 1]))
    top_row = lax.broadcasted_iota(jnp.int32, (16, 1), 0) == 0
    for h in range(2):
        at = slice(256 * h, 256 * h + 16)
        fixed = dot3((vs[0, at], vs[1, at]), (b_fwd[1, 0], b_fwd[1, 1]))
        gs[at, :] = jnp.where(top_row, fixed, gs[at, :])

    tile, k2c = lax.div(me, 128), lax.rem(me, 128)
    lower = k2c < 64
    group = lax.div(lane, 32)
    order = lax.rem(lane, 8)
    energy = zero8
    for h in range(2):
        kap = 4 * (tile + 2 * h) + group
        q = jnp.where(
            kap == 0,
            jnp.where(lower, 32 * k2c, 16 + 32 * (k2c - 64)),
            jnp.where(lower, kap + 32 * k2c, 32 - kap + 32 * (k2c - 64)),
        )
        qf = q.astype(F32)
        aq = jnp.where(q == 0, 1.0 / M, 2.0 / M)

        def scale(i, energy, h=h, qf=qf, aq=aq):
            at = pl.multiple_of(i * 16, 16)
            p1 = lax.broadcasted_iota(jnp.int32, (16, 128), 0) + at
            up = order < 4
            p = jnp.where(up, p1 + 512 * order, 512 - p1 + 512 * (order - 4))
            p = jnp.where(jnp.logical_and(p1 == 0, jnp.logical_not(up)), 256 + 512 * (order - 4), p)
            pf_ = p.astype(F32)
            k2 = pf_ * pf_ + qf * qf
            inverse = jnp.where(k2 == 0.0, 0.0, 1.0 / jnp.where(k2 == 0.0, 1.0, k2))
            value = gs[pl.ds(256 * h + at, 16), :]
            weighted = value * (jnp.where(p == 0, 1.0 / M, 2.0 / M) * aq * inverse)
            work = weighted * value
            base = weighted * (1.0 / STEP)
            for f, part in enumerate((base * qf, base * pf_)):
                parts = split(part)
                for k in range(2):
                    vs[k, pl.ds(512 * f + 256 * h + at, 16), 0:128] = parts[k]
            return energy + (work[0:8] + work[8:16])

        energy = lax.fori_loop(0, 16, scale, energy)

    for f in range(2):
        rows = slice(512 * f, 512 * f + 512)
        drive = (vs[0, rows, 0:128], vs[1, rows, 0:128])
        us[...] = dot3(drive, (b_inv[f, 0, 0], b_inv[f, 0, 1]))
        for h in range(2):
            at = slice(256 * h, 256 * h + 16)
            src = slice(512 * f + 256 * h, 512 * f + 256 * h + 16)
            fixed = dot3((vs[0, src, 0:128], vs[1, src, 0:128]), (b_inv[f, 1, 0], b_inv[f, 1, 1]))
            us[at, :] = jnp.where(top_row, fixed, us[at, :])

        def back_chunk(i, carry, f=f):
            at = pl.multiple_of(i * 16, 16)
            c, s = ty[0, pl.ds(at, 16), :], ty[1, pl.ds(at, 16), :]
            for h in range(2):
                re, im = us[pl.ds(256 * h + at, 16), 0:128], us[pl.ds(256 * h + at, 16), 128:256]
                lanes = slice(256 * f + 128 * h, 256 * f + 128 * h + 128)
                for half, value in enumerate((re * c - im * s, re * s + im * c)):
                    parts = split(value)
                    for k in range(2):
                        zs[k, pl.ds(256 * half + at, 16), lanes] = parts[k]
            return carry

        lax.fori_loop(0, 16, back_chunk, 0)
    for t in range(4):
        lanes = slice(128 * t, 128 * t + 128)
        s2[t] = dot3((cy_inv[0], cy_inv[1]), (zs[0, :, lanes], zs[1, :, lanes]))

    exchange(s2, r2, a2_s, a2_r)

    def total(x):
        return jnp.sum(jnp.sum(x, axis=1, keepdims=True), axis=0, keepdims=True)

    row = jnp.where(lane == 0, total(excess) * 0.25, jnp.where(lane == 1, total(area) * 0.25, total(energy) * (1.0 / (STEP * STEP * M * M))))
    es[0] = row
    e1[plane] = row
    for i in range(1, 16):
        send(es.at[0], e1.at[plane], e_s.at[0], e_r.at[0], device_at(lax.rem(plane + i, 16), column)).start()
    exchange_wait(s2, r2, a2_s, a2_r)
    sums_wait = send(e1.at[pl.ds(0, 15)], e1.at[pl.ds(0, 15)], e_s.at[0], e_r.at[0], (slab, other))
    sums_wait.wait_recv()
    sums_wait.wait_send()
    row = jnp.sum(e1[...], axis=0)
    es[1] = row
    e2[column] = row
    for i in range(1, 16):
        send(es.at[1], e2.at[column], e_s.at[1], e_r.at[1], device_at(plane, lax.rem(column + i, 16))).start()

    for f, out in enumerate((field_x, field_y)):
        for t in range(4):
            lanes = slice(128 * t, 128 * t + 128)
            o = split(r2[2 * f + t // 2, 128 * (t % 2) : 128 * (t % 2) + 128, :])
            got = dot3((w_inv[f, 0, 0], w_inv[f, 0, 1]), o)
            if t == 0:
                got = jnp.where(first_group, dot3((w_inv[f, 1, 0], w_inv[f, 1, 1]), o), got)
            d4[512 * t : 512 * t + 256, :] = got

        def out_chunk(i, carry):
            at = pl.multiple_of(i * 16, 16)
            yr_, yi_ = [], []
            for t in range(4):
                lanes = slice(128 * t, 128 * t + 128)
                c, s = tx[0, pl.ds(at, 16), lanes], tx[1, pl.ds(at, 16), lanes]
                re, im = d4[pl.ds(512 * t + at, 16), :], d4[pl.ds(512 * t + 128 + at, 16), :]
                yr_.append(re * c - im * s)
                yi_.append(re * s + im * c)
            mid = yi_[0] * group_mask

            def four(re, im):
                ar, ai, br, bi = re[0] + re[2], im[0] + im[2], re[1] + re[3], im[1] + im[3]
                cr, ci, dr, di = re[0] - re[2], im[0] - im[2], re[1] - re[3], im[1] - im[3]
                return (ar + br, ai + bi), (cr - di, ci + dr), (ar - br, ai - bi), (cr + di, ci - dr)

            m0, m2, m4, m6 = four(yr_, yi_)
            ur = [yr_[0], (yr_[1] - yi_[1]) * R2, -yi_[2], -(yr_[3] + yi_[3]) * R2]
            ui = [yi_[0], (yr_[1] + yi_[1]) * R2, yr_[2], (yr_[3] - yi_[3]) * R2]
            m1, m3, m5, m7 = four(ur, ui)
            for m, (re, im) in enumerate((m0, m1, m2, m3, m4, m5, m6, m7)):
                re = re + mid if m % 2 == 0 else re - mid
                for a in (m, m + 8):
                    parts = split(re * wa[a : a + 1, :] - im * wa[16 + a : 17 + a, :])
                    for k in range(2):
                        ps[k, pl.ds(128 * a + at, 16), :] = parts[k]
            return carry

        lax.fori_loop(0, 8, out_chunk, 0)
        for i in range(8):
            at = slice(256 * i, 256 * i + 256)
            got = dot_nt(join[...], ps[0, at, :]) + dot_nt(join[...], ps[1, at, :])
            for g in range(REGIONS):
                out[g, :, at] = got[8 * g : 8 * g + 8, :]
            fb[32 * f : 32 * f + 32, at] = got.astype(BF)

    def push(slot):
        got = dot(fb[...], xb[slot])
        rows = yr[slot].astype(BF).astype(F32)
        for f in range(2):
            pf[slot, f : f + 1, :] = jnp.sum(got[32 * f : 32 * f + 32, :] * rows, axis=0, keepdims=True)

    def give_back(slot, device, sem, into):
        return send(pf.at[slot], pr.at[into], f_s.at[sem], f_r.at[into], device)

    push(other)
    give_back(other, (slab, other), 0, 0).start()

    @pl.when(has_prev)
    def _():
        for k in range(2):
            push(2 + k)
            give_back(2 + k, (slab - 1, k), 1 + k, 1).start()

    push(mine)
    pr[2] = jnp.zeros((2, CELLS_DEV), F32)
    give_back(other, (slab, other), 0, 0).wait_recv()

    @pl.when(has_next)
    def _():
        give_back(other, (slab, other), 0, 1).wait_recv()

    @pl.when(jnp.logical_not(has_next))
    def _():
        pr[1] = jnp.zeros((2, CELLS_DEV), F32)

    force[...] = pf[mine] + pr[0] + pr[1]

    send(e2.at[pl.ds(0, 15)], e2.at[pl.ds(0, 15)], e_s.at[1], e_r.at[1], (slab, other)).wait()
    sums[...] = jnp.broadcast_to(jnp.sum(e2[...], axis=0), (8, 128))

    give_back(other, (slab, other), 0, 0).wait_send()
    to_partner.wait_send()

    @pl.when(has_prev)
    def _():
        for k in range(2):
            give_back(2 + k, (slab - 1, k), 1 + k, 1).wait_send()

    @pl.when(has_next)
    def _():
        to_next.wait_send()


def body(cell_row, cell_col, cell_width, cell_height, cell_region, cell_offset):
    off = cell_offset
    cellp = jnp.stack(
        [
            cell_col.astype(F32),
            off[0],
            off[0] + cell_width.astype(F32),
            cell_row.astype(F32),
            off[1],
            off[1] + cell_height.astype(F32),
            cell_region.astype(F32),
            off[0],
        ]
    )
    consts = [jnp.asarray(t) for t in tables()]
    vmem = pl.BlockSpec(memory_space=pltpu.VMEM)
    V = pltpu.VMEM
    D = pltpu.SemaphoreType.DMA
    scratch = [
        V((4, 8, CELLS_DEV), F32),
        V((4, M, CELLS_DEV), BF),
        V((4, 32, CELLS_DEV), F32),
        V((M, 128), F32),
        V((2, 512, 512), BF),
        V((2, 256, 128), F32),
        V((2, 256, 128), F32),
        V((512, 256), F32),
        V((2, 1024, 256), BF),
        V((512, 128), F32),
        V((4, 256, 128), F32),
        V((4, 256, 128), F32),
        V((2, M, 128), BF),
        V((64, M), BF),
        V((4, 2, CELLS_DEV), F32),
        V((3, 2, CELLS_DEV), F32),
        V((16, 1, 128), F32),
        V((16, 1, 128), F32),
        V((2, 1, 128), F32),
        pltpu.SemaphoreType.REGULAR,
        D((2,)), D((4,)),
        D, D, D, D,
        D((3,)), D((2,)),
        D((2,)), D((2,)),
    ]
    field_x, field_y, force, sums = pl.pallas_call(
        kernel,
        out_shape=(
            jax.ShapeDtypeStruct((REGIONS, 8, M), F32),
            jax.ShapeDtypeStruct((REGIONS, 8, M), F32),
            jax.ShapeDtypeStruct((2, CELLS_DEV), F32),
            jax.ShapeDtypeStruct((8, 128), F32),
        ),
        in_specs=[vmem] * (1 + len(consts)),
        out_specs=(vmem,) * 4,
        scratch_shapes=scratch,
        compiler_params=pltpu.CompilerParams(
            collective_id=0, has_side_effects=True, vmem_limit_bytes=60 * 1024 * 1024
        ),
        name="placement",
    )(cellp, *consts)
    overflow = sums[0, 0] / sums[0, 1]
    return (field_x, field_y, force, sums[0, 2], overflow)


def solution(mesh):
    both = ("slab", "cell")
    placed = (P(both),) * 5 + (P(None, both),)
    return jax.shard_map(
        body,
        mesh=mesh,
        in_specs=placed,
        out_specs=(P(None, both, None), P(None, both, None), P(None, both), P(), P()),
        check_vma=False,
    )
```

```python
import functools
import math

import jax
import jax.numpy as jnp
import numpy as np
from jax import lax
from jax.experimental import pallas as pl
from jax.experimental.pallas import tpu as pltpu
from jax.sharding import PartitionSpec as P

M = 2048
REGIONS = 4
SLABS = 128
CELLS_DEV = 512
BF = jnp.bfloat16
F32 = jnp.float32
I32 = jnp.int32
MESH = pl.DeviceIdType.MESH
STEP = math.pi / M


def c_add(x,y): return (x[0]+y[0], x[1]+y[1])
def c_sub(x,y): return (x[0]-y[0], x[1]-y[1])
def c_turn(x,angle):
    c,s=math.cos(angle),math.sin(angle)
    if abs(s)<1e-12: return x if c>0 else (-x[0],-x[1])
    if abs(c)<1e-12: return (-x[1],x[0]) if s>0 else (x[1],-x[0])
    if abs(abs(c)-abs(s))<1e-12:
        h=abs(c); a,b=x[0],x[1]
        sc,ss=(1 if c>0 else -1),(1 if s>0 else -1)
        def lin(p,a,q,b):
            if p>0: return (a+b)*h if q>0 else (a-b)*h
            return (b-a)*h if q>0 else (a+b)*(-h)
        return (lin(sc,a,-ss,b), lin(ss,a,sc,b))
    return (x[0]*c-x[1]*s, x[0]*s+x[1]*c)
def c_fft(xs,sign):
    n=len(xs)
    if n==1: return xs
    even,odd=c_fft(xs[0::2],sign),c_fft(xs[1::2],sign)
    out=[None]*n
    for k in range(n//2):
        t=c_turn(odd[k],sign*2*math.pi*k/n)
        out[k],out[k+n//2]=c_add(even[k],t),c_sub(even[k],t)
    return out
def real_spectrum(d):
    n=len(d)
    if n==2:
        return {0:d[0]+d[1],1:(d[0],-d[1]),2:d[0]-d[1]}
    half=n//2
    out={}
    z=[c_turn((d[a],-d[a+half]),-math.pi*a/n) for a in range(half)]
    f=c_fft(z,-1)
    for m in range(half):
        k=1+4*m
        if k<n: out[k]=f[m]
        else: out[2*n-k]=(f[m][0],-f[m][1])
    s=[d[a]+d[a+half] for a in range(half)]
    e=[d[a]-d[a+half] for a in range(half)]
    q=half//2
    z=[c_turn((e[a],-e[a+q]),-2*math.pi*a/n) for a in range(q)]
    f=c_fft(z,-1)
    for l in range(q):
        m=1+4*l
        if m<=half: out[2*m]=f[l]
        else: out[2*(n-m)]=(f[l][0],-f[l][1])
    sub=real_full(s)
    for l,v in sub.items(): out[4*l]=v
    return out
def real_full(s):
    n=len(s)
    if n==2: return {0:s[0]+s[1],1:s[0]-s[1]}
    half=n//2
    p=[s[a]+s[a+half] for a in range(half)]
    e=[s[a]-s[a+half] for a in range(half)]
    out={}
    for l,v in real_full(p).items(): out[2*l]=v
    q=half//2
    if q==0: return out
    z=[c_turn((e[a],-e[a+q]),-2*math.pi*a/n) for a in range(q)] if q else []
    f=c_fft(z,-1)
    for k in range(q):
        l=1+4*k
        if l<=half: out[l]=f[k]
        else: out[n-l]=(f[k][0],-f[k][1])
    return out
def real_full_back(v,n):
    if n==2: return [v[0]+v[1],v[0]-v[1]]
    half=n//2; q=half//2
    p=real_full_back({l//2:x for l,x in v.items() if l%2==0},half)
    if n==4:
        g=[v[1]]
    else:
        g=[v[1+4*k] if 1+4*k<=half else (v[n-1-4*k][0],-v[n-1-4*k][1]) for k in range(q)]
    f=c_fft(g,1)
    odd=[None]*half
    for a in range(q):
        t=c_turn(f[a],2*math.pi*a/n)
        odd[a],odd[a+q]=t[0],-t[1]
    out=[None]*n
    for a in range(half):
        out[a],out[a+half]=p[a]+odd[a],p[a]-odd[a]
    return out
def real_back(y,n):
    half=n//2
    even=real_full_back({k//2:v for k,v in y.items() if k%2==0},n)
    g=[y[1+4*m] if 1+4*m<n else (y[2*n-1-4*m][0],-y[2*n-1-4*m][1]) for m in range(half)]
    f=c_fft(g,1)
    out=[None]*n
    for a in range(half):
        t=c_turn(f[a],math.pi*a/n)
        out[a],out[a+half]=even[a]+t[0],even[a+half]-t[1]
    return out


def split_np(table):
    high = table.astype(np.float32).astype(BF)
    low = (table - high.astype(np.float64)).astype(np.float32).astype(BF)
    return np.stack([high, low])


@functools.lru_cache(None)
def tables():
    pi = np.pi
    k2 = np.arange(64)[:, None]
    b = np.arange(128)[None, :]
    c1, s1 = np.cos(pi * k2 * (2 * b + 1) / 128), np.sin(pi * k2 * (2 * b + 1) / 128)
    c2, s2 = np.cos(pi * (k2 + 1) * (2 * b + 1) / 128), np.sin(pi * (k2 + 1) * (2 * b + 1) / 128)
    cm, sm = np.cos(pi * (2 * k2 + 1) * (2 * b + 1) / 256), np.sin(pi * (2 * k2 + 1) * (2 * b + 1) / 256)
    zero = np.zeros_like(c1)
    wc = np.block([[c1, s1], [c2, -s2]])
    wc0 = np.block([[c1, zero], [zero, cm]])
    ws = np.block([[s1, -c1], [s2, c2]])
    ws0 = np.block([[s1, zero], [zero, sm]])
    w = np.stack([split_np(m) for m in (ws, ws0, wc, wc0)]).reshape(2, 2, 2, 128, 256)
    kap = np.arange(16)[:, None]
    ang = pi * kap * (2 * b + 1) / 4096
    tx = np.stack([np.cos(ang), np.sin(ang)]).astype(np.float32)
    p1 = np.arange(256)[:, None]
    d = np.arange(256)[None, :]
    cre, cim = np.cos(2 * pi * p1 * d / 512), -np.sin(2 * pi * p1 * d / 512)
    cim[0] = (-1.0) ** np.arange(256)
    cy = np.concatenate([cre, cim], 0)
    cy_fwd, cy_inv = split_np(cy), split_np(cy.T)
    r = np.arange(8)
    angy = pi * p1 * (2 * r[None, :] + 1) / 4096
    ty = np.stack([np.tile(np.cos(angy), (1, 16)), np.tile(np.sin(angy), (1, 16))]).astype(np.float32)
    p2 = np.arange(4)[None, :]
    rr = r[:, None]
    e0, e1 = pi * p2 * (2 * rr + 1) / 8, pi * (p2 + 1) * (2 * rr + 1) / 8
    em = pi * (2 * rr + 1) * (1 + 2 * p2) / 16
    z8 = np.zeros((8, 4))
    bc = (np.block([np.cos(e0), np.cos(e1)]), np.block([np.sin(e0), -np.sin(e1)]))
    bc0 = (np.block([np.cos(e0), z8]), np.block([z8, np.cos(em)]))
    bs = (np.block([np.sin(e0), np.sin(e1)]), np.block([-np.cos(e0), np.cos(e1)]))
    bs0 = (np.block([np.sin(e0), z8]), np.block([z8, np.sin(em)]))

    def wide(pair):
        return np.concatenate([np.kron(np.eye(16), part) for part in pair], 0)

    b_fwd = np.stack([np.concatenate(list(split_np(wide(m))), axis=1) for m in (bc, bc0)])
    b_inv = np.stack([split_np(wide(m).T) for m in (bc, bc0, bs, bs0)]).reshape(2, 2, 2, 128, 256)
    return w, tx, cy_fwd, cy_inv, ty, b_fwd, b_inv


def dot(x, y):
    return lax.dot_general(x, y, (((1,), (0,)), ((), ())), preferred_element_type=F32)


def dot_nt(x, y):
    return lax.dot_general(x, y, (((1,), (1,)), ((), ())), preferred_element_type=F32)


def split(x):
    high = x.astype(BF)
    return high, (x - high.astype(F32)).astype(BF)


def dot3(x, y):
    return dot(x[0], y[0]) + (dot(x[0], y[1]) + dot(x[1], y[0]))


def dot3_nt(x, y):
    return dot_nt(x[0], y[0]) + (dot_nt(x[0], y[1]) + dot_nt(x[1], y[0]))


def encode(x, y):
    top = jnp.maximum(jnp.maximum(jnp.abs(x), jnp.abs(y)), 2.0**-31)
    exponent = jnp.minimum(jnp.floor(jnp.log2(top)), 31.0)
    scale = jnp.exp2(11.0 - exponent)

    def code(v):
        return jnp.clip(jnp.round(v * scale), -4095.0, 4095.0).astype(I32)

    high = jnp.left_shift(exponent.astype(I32) + 32, 26)
    return high | jnp.left_shift(code(y) & 0x1FFF, 13) | (code(x) & 0x1FFF)


def decode(word):
    scale = jnp.exp2(lax.shift_right_logical(word, 26).astype(F32) - 43.0)
    x = lax.shift_right_arithmetic(jnp.left_shift(word, 19), 19).astype(F32)
    y = lax.shift_right_arithmetic(jnp.left_shift(word, 6), 19).astype(F32)
    return x * scale, y * scale


def place():
    slab = lax.axis_index("slab")
    cell = lax.axis_index("cell")
    return slab, cell, lax.div(slab, 8), lax.rem(slab, 8) * 2 + cell


def device_at(plane, column):
    return (plane * 8 + lax.div(column, 2), lax.rem(column, 2))


def overlap(bins, low, high):
    return jnp.maximum(jnp.minimum(bins + 1.0, high) - jnp.maximum(bins, low), 0.0)


def kernel(
    row_h, col_h, width_h, height_h, region_h, offset_h,
    w_h, tx_h, cyf_h, cyi_h, ty_h, bf_h, bi_h,
    field_x, field_y, force, sums,
    ci, co, pq, ym, yr, xb, d2, zs, s1, r1, us, vs, gs, aw, pt, s2, r2, zx, fb, pf, pr, e1, e2, es,
    w, w2, tx, cyf, cyi, ty, bf, bi, bi2,
    const_sem, in_sem, col_sem, cell_s, cell_r, a1_s, a1_r, a2_s, a2_r, f_s, f_r, e_s, e_r,
):
    slab, cell, plane, column = place()
    me = plane * 16 + column
    mine, other = cell, 1 - cell
    has_prev = jnp.logical_and(cell == 0, slab > 0)
    has_next = slab < SLABS - 1
    barrier = pltpu.get_barrier_semaphore()

    own = [
        pltpu.make_async_copy(src, ci.at[mine, k], in_sem.at[k])
        for k, src in enumerate((row_h, col_h, width_h, height_h, region_h))
    ]
    own.append(pltpu.make_async_copy(offset_h, co.at[mine], in_sem.at[5]))
    for copy in own:
        copy.start()

    def signal_at(sem, device):
        pl.semaphore_signal(sem, inc=1, device_id=device, device_id_type=MESH)

    @pl.when(has_prev)
    def _():
        signal_at(barrier, (slab - 1, 0))
        signal_at(barrier, (slab - 1, 1))

    for i in range(1, 16):
        signal_at(barrier, device_at(lax.rem(plane + i, 16), column))
        signal_at(barrier, device_at(plane, lax.rem(column + i, 16)))

    fetched = [
        pltpu.make_async_copy(src, dst, const_sem.at[k])
        for k, (src, dst) in enumerate(
            (
                (tx_h, tx), (w_h, w), (w_h.at[:, 0, 0], w2.at[:, 0:128]), (w_h.at[:, 0, 0], w2.at[:, 128:256]),
                (cyf_h, cyf), (ty_h, ty), (bf_h, bf), (bi_h, bi),
                (bi_h.at[:, 0, 0], bi2.at[:, 0:128]), (bi_h.at[:, 0, 0], bi2.at[:, 128:256]), (cyi_h, cyi),
            )
        )
    ]
    for copy in fetched:
        copy.start()
    for copy in own:
        copy.wait()

    low_row = slab * 16 + cell * 8

    def cell_row_of(slot, k, which):
        return ci[slot, which, k : k + 1, :]

    def make_cells(slot):
        bins = lax.broadcasted_iota(I32, (128, 128), 0).astype(F32)
        rows = (lax.broadcasted_iota(I32, (8, 128), 0) + low_row).astype(F32)
        for k in range(4):
            at = slice(128 * k, 128 * k + 128)
            far = slice(512 + 128 * k, 640 + 128 * k)
            col = cell_row_of(slot, k, 1)
            high_bits = lax.shift_right_logical(col, 7)
            low_bits = (col - high_bits * 128).astype(F32)
            start = co[slot, 0:1, at]
            end = start + cell_row_of(slot, k, 2).astype(F32)
            reach = bins - low_bits
            pq[slot, :, at] = overlap(reach, start, end).astype(BF)
            pq[slot, :, far] = overlap(reach + 128.0, start, end).astype(BF)
            start = co[slot, 1:2, at]
            end = start + cell_row_of(slot, k, 3).astype(F32)
            got = overlap(rows - cell_row_of(slot, k, 0).astype(F32), start, end)
            region = cell_row_of(slot, k, 4)
            parts = jnp.concatenate([jnp.where(region == g, got, 0.0) for g in range(REGIONS)], axis=0)
            yr[slot, :, at] = parts.astype(BF).astype(F32)
            for a in range(16):
                to = slice(32 * a, 32 * a + 32)
                ym[to, at] = jnp.where(high_bits == a, parts, 0.0).astype(BF)
                ym[to, far] = jnp.where(high_bits == a - 1, parts, 0.0).astype(BF)

    def add_density(slot, fresh):
        got = dot_nt(ym[...], pq[slot])
        d2[...] = got if fresh else d2[...] + got

    def send(src, dst, s_sem, r_sem, device):
        return pltpu.make_async_remote_copy(
            src_ref=src, dst_ref=dst, send_sem=s_sem, recv_sem=r_sem, device_id=device, device_id_type=MESH
        )

    make_cells(mine)
    pl.semaphore_wait(barrier, 30 + has_next.astype(I32))
    partner = (slab, other)
    give = [
        send(ci.at[mine], ci.at[mine], cell_s.at[0], cell_r.at[0, mine], partner),
        send(co.at[mine], co.at[mine], cell_s.at[1], cell_r.at[1, mine], partner),
    ]
    give_next = [
        send(ci.at[mine], ci.at[2 + mine], cell_s.at[2], cell_r.at[0, 2 + mine], (slab + 1, 0)),
        send(co.at[mine], co.at[2 + mine], cell_s.at[3], cell_r.at[1, 2 + mine], (slab + 1, 0)),
    ]
    for copy in give:
        copy.start()

    @pl.when(has_next)
    def _():
        for copy in give_next:
            copy.start()

    for i in range(1, 16):
        signal_at(col_sem, device_at(plane, lax.rem(column + i, 16)))

    def arrive(slot):
        send(ci.at[slot], ci.at[slot], cell_s.at[0], cell_r.at[0, slot], partner).wait_recv()
        send(co.at[slot], co.at[slot], cell_s.at[1], cell_r.at[1, slot], partner).wait_recv()

    add_density(mine, True)
    arrive(other)
    make_cells(other)
    add_density(other, False)

    @pl.when(has_prev)
    def _():
        for k in range(2):
            arrive(2 + k)
            make_cells(2 + k)
            add_density(2 + k, False)

    def tally(i, carry):
        excess, area = carry
        got = d2[pl.ds(pl.multiple_of(i * 64, 64), 64), :].reshape(8, 8, 128)
        return excess + jnp.sum(jnp.maximum(got - 1.0, 0.0), axis=0), area + jnp.sum(got, axis=0)

    zero8 = jnp.zeros((8, 128), F32)
    excess, area = lax.fori_loop(0, 8, tally, (zero8, zero8))
    lane = lax.broadcasted_iota(I32, (1, 128), 1)
    first_group = lane < 32

    fetched[0].wait()

    def x_chunk(i, carry):
        at = pl.multiple_of(i * 16, 16)
        got = real_spectrum([d2[pl.ds(pl.multiple_of(32 * a + at, 16), 16), :] for a in range(16)])
        for kap in range(16):
            if kap == 0:
                pair = (got[0], got[16])
            else:
                (re, im), c, s = got[kap], tx[0, kap : kap + 1, :], tx[1, kap : kap + 1, :]
                pair = (re * c + im * s, im * c - re * s)
            for half, value in enumerate(pair):
                parts = split(value)
                for k in range(2):
                    zs[k, pl.ds(pl.multiple_of(32 * kap + at, 16), 16), 128 * half : 128 * half + 128] = parts[k]
        return carry

    lax.fori_loop(0, 2, x_chunk, 0)
    fetched[1].wait()
    table, first = (w[1, 0, 0], w[1, 0, 1]), (w[1, 1, 0], w[1, 1, 1])
    got = dot3_nt(table, (zs[0, :, 0:256], zs[1, :, 0:256]))
    fixed = dot3_nt(first, (zs[0, 0:128, 0:256], zs[1, 0:128, 0:256]))
    tiles = [got[:, 128 * t : 128 * t + 128] for t in range(4)]
    tiles[0] = jnp.where(first_group, fixed, tiles[0])
    for t in range(2):
        s1[128 * t : 128 * t + 128, :] = encode(tiles[t], tiles[t + 2])

    pl.semaphore_wait(col_sem, 15)
    py, px = lax.div(plane, 4), lax.rem(plane, 4)
    z, core = lax.div(column, 4) * 2 + cell, lax.rem(lax.div(column, 2), 2)
    ys = [lax.rem(py + k, 4) for k in range(4)]
    xs = [lax.rem(px + k, 4) for k in range(4)]
    hops = [0, 1, 2, 1]
    near = sorted(((dy, dx, dc) for dy in range(4) for dx in range(4) for dc in range(2)), key=lambda d: -(hops[d[0]] + hops[d[1]] + 0.5 * d[2]))

    def exchange(at, src, dst, s_sem, r_sem):
        def ring(dz, skip_self):
            there = lax.rem(z + dz, 8)
            zh, zl = lax.div(there, 2), lax.rem(there, 2)
            for dy, dx, dc in near:
                if skip_self and dy == dx == dc == 0:
                    continue
                core_to = core if dc == 0 else 1 - core
                plane_to = ys[dy] * 4 + xs[dx]
                to = plane_to * 16 + (zh * 4 + zl + core_to * 2)
                send(at(src, to), at(dst, me), s_sem, r_sem, (plane_to * 8 + (zh * 2 + core_to), zl)).start()

        def step(i, carry):
            ring(4 + lax.div(i + 1, 2) * (1 - 2 * lax.rem(i, 2)), False)
            return carry

        lax.fori_loop(0, 7, step, 0)
        ring(0, True)

    def row_of(ref, m):
        return ref.at[pl.ds(m, 1)]

    def rows_of(ref, m):
        return ref.at[:, pl.ds(m, 1)]

    exchange(row_of, s1, r1, a1_s, a1_r)
    r1[pl.ds(me, 1), :] = s1[pl.ds(me, 1), :]

    tile, k2c = lax.div(me, 128), lax.rem(me, 128)
    lower = k2c < 64
    group = lax.div(lane, 32)
    order = lax.rem(lane, 8)

    def q_of(h):
        kap = 4 * (tile + 2 * h) + group
        return jnp.where(
            kap == 0,
            jnp.where(lower, 32 * k2c, 16 + 32 * (k2c - 64)),
            jnp.where(lower, kap + 32 * k2c, 32 - kap + 32 * (k2c - 64)),
        )

    qs = [q_of(h) for h in range(2)]

    def weigh(i, carry):
        at = pl.multiple_of(i * 16, 16)
        p1 = lax.broadcasted_iota(I32, (16, 128), 0) + at
        up = order < 4
        p = jnp.where(up, p1 + 512 * order, 512 - p1 + 512 * (order - 4))
        p = jnp.where(jnp.logical_and(p1 == 0, jnp.logical_not(up)), 256 + 512 * (order - 4), p)
        p_float = p.astype(F32)
        pt[pl.ds(at, 16), :] = p_float
        for h in range(2):
            q_float = qs[h].astype(F32)
            k2 = p_float * p_float + q_float * q_float
            scale = jnp.where(p == 0, 1.0 / M, 2.0 / M) * jnp.where(qs[h] == 0, 1.0 / M, 2.0 / M) * (1.0 / STEP)
            aw[pl.ds(256 * h + at, 16), :] = jnp.where(k2 == 0.0, 0.0, scale / jnp.where(k2 == 0.0, 1.0, k2))
        return carry

    lax.fori_loop(0, 16, weigh, 0)

    def make_profiles(slot):
        def block(a, carry):
            to = pl.ds(pl.multiple_of(a * 128, 128), 128)
            for k in range(4):
                at = slice(128 * k, 128 * k + 128)
                high_bits = lax.shift_right_logical(cell_row_of(slot, k, 1), 7)
                first = (high_bits == a).astype(F32).astype(BF)
                second = (high_bits == a - 1).astype(F32).astype(BF)
                xb[slot, to, at] = pq[slot, :, at] * first + pq[slot, :, 512 + 128 * k : 640 + 128 * k] * second
            return carry

        lax.fori_loop(0, 16, block, 0)

    make_profiles(mine)
    make_profiles(other)

    @pl.when(has_prev)
    def _():
        for k in range(2):
            make_profiles(2 + k)

    for copy in fetched[2:]:
        copy.wait()
    whole = send(s1.at[pl.ds(0, 255)], r1.at[pl.ds(0, 255)], a1_s, a1_r, partner)
    whole.wait_recv()
    whole.wait_send()

    high, low = zip(*(split(v) for v in decode(r1[...])))
    whole = (jnp.concatenate(high, axis=1), jnp.concatenate(low, axis=1))
    us[...] = dot3((cyf[0], cyf[1]), whole)

    def y_chunk(i, carry):
        at = pl.multiple_of(i * 16, 16)
        c, s = ty[0, pl.ds(at, 16), :], ty[1, pl.ds(at, 16), :]
        for h in range(2):
            lanes = slice(128 * h, 128 * h + 128)
            re, im = us[pl.ds(at, 16), lanes], us[pl.ds(256 + at, 16), lanes]
            for half, value in enumerate((re * c + im * s, im * c - re * s)):
                parts = split(value)
                for k in range(2):
                    vs[k, pl.ds(256 * h + at, 16), 128 * half : 128 * half + 128] = parts[k]
        return carry

    lax.fori_loop(0, 16, y_chunk, 0)

    def y_out(rows, table):
        got = dot(vs[0, rows], table)
        return got[:, 0:128] + (got[:, 128:256] + dot(vs[1, rows], table[:, 0:128]))

    gs[...] = y_out(slice(0, 512), bf[0])
    top_row = lax.broadcasted_iota(I32, (16, 1), 0) == 0
    for h in range(2):
        at = slice(256 * h, 256 * h + 16)
        gs[at, :] = jnp.where(top_row, y_out(at, bf[1]), gs[at, :])

    q_floats = [q.astype(F32) for q in qs]

    def scale_chunk(i, energy):
        at = pl.multiple_of(i * 16, 16)
        p_float = pt[pl.ds(at, 16), :]
        for h in range(2):
            value = gs[pl.ds(256 * h + at, 16), :]
            weighted = value * aw[pl.ds(256 * h + at, 16), :]
            work = weighted * value
            energy = energy + (work[0:8] + work[8:16])
            for f, part in enumerate((weighted * q_floats[h], weighted * p_float)):
                parts = split(part)
                for k in range(2):
                    vs[f, pl.ds(256 * h + at, 16), 128 * k : 128 * k + 128] = parts[k]
        return energy

    energy = lax.fori_loop(0, 16, scale_chunk, zero8)

    for f in range(2):
        us[...] = dot(vs[f], bi2[f]) + dot(vs[f, :, 0:128], bi[f, 0, 1])
        for h in range(2):
            at = slice(256 * h, 256 * h + 16)
            fixed = dot3((vs[f, at, 0:128], vs[f, at, 128:256]), (bi[f, 1, 0], bi[f, 1, 1]))
            us[at, :] = jnp.where(top_row, fixed, us[at, :])

        def back_chunk(i, carry, f=f):
            at = pl.multiple_of(i * 16, 16)
            c, s = ty[0, pl.ds(at, 16), :], ty[1, pl.ds(at, 16), :]
            for h in range(2):
                re, im = us[pl.ds(256 * h + at, 16), 0:128], us[pl.ds(256 * h + at, 16), 128:256]
                lanes = slice(256 * f + 128 * h, 256 * f + 128 * h + 128)
                for half, value in enumerate((re * c - im * s, re * s + im * c)):
                    parts = split(value)
                    for k in range(2):
                        zs[k, pl.ds(256 * half + at, 16), lanes] = parts[k]
            return carry

        lax.fori_loop(0, 16, back_chunk, 0)
    for f in range(2):
        lanes = slice(256 * f, 256 * f + 256)
        got = dot3((cyi[0], cyi[1]), (zs[0, :, lanes], zs[1, :, lanes]))
        s2[f] = encode(got[:, 0:128], got[:, 128:256])

    exchange(rows_of, s2, r2, a2_s, a2_r)
    r2[:, pl.ds(me, 1), :] = s2[:, pl.ds(me, 1), :]

    def total(x):
        return jnp.sum(jnp.sum(x, axis=1, keepdims=True), axis=0, keepdims=True)

    row = jnp.where(
        lane == 0, total(excess), jnp.where(lane == 1, total(area), total(energy) * (1.0 / (STEP * M * M)))
    )
    es[0] = row
    e1[plane] = row
    for i in range(1, 16):
        send(es.at[0], e1.at[plane], e_s.at[0], e_r.at[0], device_at(lax.rem(plane + i, 16), column)).start()
    whole = send(s2.at[:, pl.ds(0, 255)], r2.at[:, pl.ds(0, 255)], a2_s, a2_r, partner)
    whole.wait_recv()
    whole.wait_send()
    sums_wait = send(e1.at[pl.ds(0, 15)], e1.at[pl.ds(0, 15)], e_s.at[0], e_r.at[0], partner)
    sums_wait.wait_recv()
    sums_wait.wait_send()
    row = jnp.sum(e1[...], axis=0)
    es[1] = row
    e2[column] = row
    for i in range(1, 16):
        send(es.at[1], e2.at[column], e_s.at[1], e_r.at[1], device_at(plane, lax.rem(column + i, 16))).start()

    for f, out in enumerate((field_x, field_y)):
        for t in range(2):
            for h, value in enumerate(decode(r2[f, 128 * t : 128 * t + 128, :])):
                parts = split(value.T)
                for k in range(2):
                    rows = slice(128 * (t + 2 * h), 128 * (t + 2 * h) + 128)
                    zx[rows, 128 * k : 128 * k + 128] = parts[k]
        us[...] = dot(zx[...], w2[f]) + dot(zx[:, 0:128], w[f, 0, 1])
        us[0:32, :] = dot3((zx[0:32, 0:128], zx[0:32, 128:256]), (w[f, 1, 0], w[f, 1, 1]))

        def out_chunk(i, carry, f=f, out=out):
            at = pl.multiple_of(i * 16, 16)
            got = {}
            for kap in range(16):
                rows = pl.ds(pl.multiple_of(32 * kap + at, 16), 16)
                re, im = us[rows, 0:128], us[rows, 128:256]
                if kap == 0:
                    got[0], got[16] = re, im
                else:
                    c, s = tx[0, kap : kap + 1, :], tx[1, kap : kap + 1, :]
                    got[kap] = (re * c - im * s, re * s + im * c)
            for a, value in enumerate(real_back(got, 16)):
                lanes = slice(128 * a, 128 * a + 128)
                out[2 * i, :, lanes] = value[0:8]
                out[2 * i + 1, :, lanes] = value[8:16]
                fb[pl.ds(pl.multiple_of(32 * f + at, 16), 16), lanes] = value.astype(BF)
            return carry

        lax.fori_loop(0, 2, out_chunk, 0)

    def push(slot):
        got = dot(fb[...], xb[slot])
        for f in range(2):
            pf[slot, f : f + 1, :] = jnp.sum(got[32 * f : 32 * f + 32, :] * yr[slot], axis=0, keepdims=True)

    def give_back(slot, device, sem, into):
        return send(pf.at[slot], pr.at[into], f_s.at[sem], f_r.at[into], device)

    push(other)
    give_back(other, partner, 0, 0).start()

    @pl.when(has_prev)
    def _():
        for k in range(2):
            push(2 + k)
            give_back(2 + k, (slab - 1, k), 1 + k, 1).start()

    push(mine)

    @pl.when(jnp.logical_not(has_next))
    def _():
        pr[1] = jnp.zeros((2, CELLS_DEV), F32)

    give_back(other, partner, 0, 0).wait_recv()

    @pl.when(has_next)
    def _():
        give_back(other, partner, 0, 1).wait_recv()

    force[...] = pf[mine] + pr[0] + pr[1]

    send(e2.at[pl.ds(0, 15)], e2.at[pl.ds(0, 15)], e_s.at[1], e_r.at[1], partner).wait()
    sums[...] = jnp.sum(e2[...], axis=0)

    give_back(other, partner, 0, 0).wait_send()
    for copy in give:
        copy.wait_send()

    @pl.when(has_prev)
    def _():
        for k in range(2):
            give_back(2 + k, (slab - 1, k), 1 + k, 1).wait_send()

    @pl.when(has_next)
    def _():
        for copy in give_next:
            copy.wait_send()


def finish(field_x, field_y, force, sums, out_x, out_y, out_force, energy, overflow, sem):
    copies = [
        pltpu.make_async_copy(src, dst, sem.at[k])
        for k, (src, dst) in enumerate(((field_x, out_x), (field_y, out_y), (force, out_force)))
    ]
    for copy in copies:
        copy.start()
    row = sums[...]
    energy[...] = row[:, 2:3]
    overflow[...] = row[:, 0:1] / row[:, 1:2]
    for copy in copies:
        copy.wait()


def body(cell_row, cell_col, cell_width, cell_height, cell_region, cell_offset):
    consts = [jnp.asarray(t) for t in tables()]
    whole = [v.reshape(4, 128) for v in (cell_row, cell_col, cell_width, cell_height, cell_region)]
    vmem = pl.BlockSpec(memory_space=pltpu.VMEM)
    hbm = pl.BlockSpec(memory_space=pltpu.HBM)
    V = pltpu.VMEM
    D = pltpu.SemaphoreType.DMA
    scratch = [
        V((4, 5, 4, 128), I32),
        V((4, 2, CELLS_DEV), F32),
        V((4, 128, 1024), BF),
        V((512, 1024), BF),
        V((4, 32, CELLS_DEV), F32),
        V((4, M, CELLS_DEV), BF),
        V((512, 128), F32),
        V((2, 512, 512), BF),
        V((256, 128), I32),
        V((256, 128), I32),
        V((512, 256), F32),
        V((2, 512, 256), BF),
        V((512, 128), F32),
        V((512, 128), F32),
        V((256, 128), F32),
        V((2, 256, 128), I32),
        V((2, 256, 128), I32),
        V((512, 256), BF),
        V((64, M), BF),
        V((4, 2, CELLS_DEV), F32),
        V((2, 2, CELLS_DEV), F32),
        V((16, 1, 128), F32),
        V((16, 1, 128), F32),
        V((2, 1, 128), F32),
        V((2, 2, 2, 128, 256), BF),
        V((2, 256, 256), BF),
        V((2, 16, 128), F32),
        V((2, 512, 256), BF),
        V((2, 256, 512), BF),
        V((2, 256, 128), F32),
        V((2, 256, 256), BF),
        V((2, 2, 2, 128, 256), BF),
        V((2, 256, 256), BF),
        D((11,)), D((6,)),
        pltpu.SemaphoreType.REGULAR,
        D((4,)), D((2, 4)),
        D, D, D, D,
        D((3,)), D((2,)),
        D((2,)), D((2,)),
    ]
    field = (REGIONS, 8, M)
    results = pl.pallas_call(
        kernel,
        out_shape=(V(field, F32), V(field, F32), V((2, CELLS_DEV), F32), V((1, 128), F32)),
        in_specs=[hbm] * (6 + len(consts)),
        out_specs=(vmem,) * 4,
        scratch_shapes=scratch,
        compiler_params=pltpu.CompilerParams(
            collective_id=0, has_side_effects=True, vmem_limit_bytes=66300000
        ),
        name="placement",
    )(*whole, cell_offset, *consts)
    S = jax.ShapeDtypeStruct
    field_x, field_y, force, energy, overflow = pl.pallas_call(
        finish,
        out_shape=(S(field, F32), S(field, F32), S((2, CELLS_DEV), F32), S((1, 1), F32), S((1, 1), F32)),
        in_specs=[vmem] * 4,
        out_specs=(hbm, hbm, hbm, vmem, vmem),
        scratch_shapes=[D((3,))],
        compiler_params=pltpu.CompilerParams(vmem_limit_bytes=4 * 1024 * 1024),
        name="finish",
    )(*results)
    return (field_x, field_y, force, energy.reshape(()), overflow.reshape(()))


def solution(mesh):
    both = ("slab", "cell")
    placed = (P(both),) * 5 + (P(None, both),)
    return jax.shard_map(
        body,
        mesh=mesh,
        in_specs=placed,
        out_specs=(P(None, both, None), P(None, both, None), P(None, both), P(), P()),
        check_vma=False,
    )
```

```python
import functools
import math

import jax
import jax.numpy as jnp
import numpy as np
from jax import lax
from jax.experimental import pallas as pl
from jax.experimental.pallas import tpu as pltpu
from jax.sharding import PartitionSpec as P

M = 2048
REGIONS = 4
SLABS = 128
CELLS_DEV = 512
BF = jnp.bfloat16
F32 = jnp.float32
I32 = jnp.int32
MESH = pl.DeviceIdType.MESH
STEP = math.pi / M


def c_add(x,y): return (x[0]+y[0], x[1]+y[1])
def c_sub(x,y): return (x[0]-y[0], x[1]-y[1])
def c_turn(x,angle):
    c,s=math.cos(angle),math.sin(angle)
    if abs(s)<1e-12: return x if c>0 else (-x[0],-x[1])
    if abs(c)<1e-12: return (-x[1],x[0]) if s>0 else (x[1],-x[0])
    if abs(abs(c)-abs(s))<1e-12:
        h=abs(c); a,b=x[0],x[1]
        sc,ss=(1 if c>0 else -1),(1 if s>0 else -1)
        def lin(p,a,q,b):
            if p>0: return (a+b)*h if q>0 else (a-b)*h
            return (b-a)*h if q>0 else (a+b)*(-h)
        return (lin(sc,a,-ss,b), lin(ss,a,sc,b))
    return (x[0]*c-x[1]*s, x[0]*s+x[1]*c)
def c_fft(xs,sign):
    n=len(xs)
    if n==1: return xs
    even,odd=c_fft(xs[0::2],sign),c_fft(xs[1::2],sign)
    out=[None]*n
    for k in range(n//2):
        t=c_turn(odd[k],sign*2*math.pi*k/n)
        out[k],out[k+n//2]=c_add(even[k],t),c_sub(even[k],t)
    return out
def real_spectrum(d):
    n=len(d)
    if n==2:
        return {0:d[0]+d[1],1:(d[0],-d[1]),2:d[0]-d[1]}
    half=n//2
    out={}
    z=[c_turn((d[a],-d[a+half]),-math.pi*a/n) for a in range(half)]
    f=c_fft(z,-1)
    for m in range(half):
        k=1+4*m
        if k<n: out[k]=f[m]
        else: out[2*n-k]=(f[m][0],-f[m][1])
    s=[d[a]+d[a+half] for a in range(half)]
    e=[d[a]-d[a+half] for a in range(half)]
    q=half//2
    z=[c_turn((e[a],-e[a+q]),-2*math.pi*a/n) for a in range(q)]
    f=c_fft(z,-1)
    for l in range(q):
        m=1+4*l
        if m<=half: out[2*m]=f[l]
        else: out[2*(n-m)]=(f[l][0],-f[l][1])
    sub=real_full(s)
    for l,v in sub.items(): out[4*l]=v
    return out
def real_full(s):
    n=len(s)
    if n==2: return {0:s[0]+s[1],1:s[0]-s[1]}
    half=n//2
    p=[s[a]+s[a+half] for a in range(half)]
    e=[s[a]-s[a+half] for a in range(half)]
    out={}
    for l,v in real_full(p).items(): out[2*l]=v
    q=half//2
    if q==0: return out
    z=[c_turn((e[a],-e[a+q]),-2*math.pi*a/n) for a in range(q)] if q else []
    f=c_fft(z,-1)
    for k in range(q):
        l=1+4*k
        if l<=half: out[l]=f[k]
        else: out[n-l]=(f[k][0],-f[k][1])
    return out
def real_full_back(v,n):
    if n==2: return [v[0]+v[1],v[0]-v[1]]
    half=n//2; q=half//2
    p=real_full_back({l//2:x for l,x in v.items() if l%2==0},half)
    if n==4:
        g=[v[1]]
    else:
        g=[v[1+4*k] if 1+4*k<=half else (v[n-1-4*k][0],-v[n-1-4*k][1]) for k in range(q)]
    f=c_fft(g,1)
    odd=[None]*half
    for a in range(q):
        t=c_turn(f[a],2*math.pi*a/n)
        odd[a],odd[a+q]=t[0],-t[1]
    out=[None]*n
    for a in range(half):
        out[a],out[a+half]=p[a]+odd[a],p[a]-odd[a]
    return out
def real_back(y,n):
    half=n//2
    even=real_full_back({k//2:v for k,v in y.items() if k%2==0},n)
    g=[y[1+4*m] if 1+4*m<n else (y[2*n-1-4*m][0],-y[2*n-1-4*m][1]) for m in range(half)]
    f=c_fft(g,1)
    out=[None]*n
    for a in range(half):
        t=c_turn(f[a],math.pi*a/n)
        out[a],out[a+half]=even[a]+t[0],even[a+half]-t[1]
    return out


def split_np(table):
    high = table.astype(np.float32).astype(BF)
    low = (table - high.astype(np.float64)).astype(np.float32).astype(BF)
    return np.stack([high, low])


@functools.lru_cache(None)
def tables():
    pi = np.pi
    k2 = np.arange(64)[:, None]
    b = np.arange(128)[None, :]
    c1, s1 = np.cos(pi * k2 * (2 * b + 1) / 128), np.sin(pi * k2 * (2 * b + 1) / 128)
    c2, s2 = np.cos(pi * (k2 + 1) * (2 * b + 1) / 128), np.sin(pi * (k2 + 1) * (2 * b + 1) / 128)
    cm, sm = np.cos(pi * (2 * k2 + 1) * (2 * b + 1) / 256), np.sin(pi * (2 * k2 + 1) * (2 * b + 1) / 256)
    zero = np.zeros_like(c1)
    wc = np.block([[c1, s1], [c2, -s2]])
    wc0 = np.block([[c1, zero], [zero, cm]])
    ws = np.block([[s1, -c1], [s2, c2]])
    ws0 = np.block([[s1, zero], [zero, sm]])
    w = np.stack([split_np(m) for m in (ws, ws0, wc, wc0)]).reshape(2, 2, 2, 128, 256)
    kap = np.arange(16)[:, None]
    ang = pi * kap * (2 * b + 1) / 4096
    tx = np.stack([np.cos(ang), np.sin(ang)]).astype(np.float32)
    p1 = np.arange(256)[:, None]
    d = np.arange(256)[None, :]
    cre, cim = np.cos(2 * pi * p1 * d / 512), -np.sin(2 * pi * p1 * d / 512)
    cim[0] = (-1.0) ** np.arange(256)
    cy = np.concatenate([cre, cim], 0)[:, np.arange(256).reshape(128, 2).T.reshape(-1)]
    ours = np.arange(128).reshape(4, 4, 2, 4).transpose(0, 2, 1, 3).reshape(-1)
    cy_fwd, cy_inv = split_np(cy), split_np(cy.T)
    r = np.arange(8)
    angy = pi * p1 * (2 * r[None, :] + 1) / 4096
    ty = np.stack([np.tile(np.cos(angy), (1, 16)), np.tile(np.sin(angy), (1, 16))])[:, :, ours].astype(np.float32)
    p2 = np.arange(4)[None, :]
    rr = r[:, None]
    e0, e1 = pi * p2 * (2 * rr + 1) / 8, pi * (p2 + 1) * (2 * rr + 1) / 8
    em = pi * (2 * rr + 1) * (1 + 2 * p2) / 16
    z8 = np.zeros((8, 4))
    bc = (np.block([np.cos(e0), np.cos(e1)]), np.block([np.sin(e0), -np.sin(e1)]))
    bc0 = (np.block([np.cos(e0), z8]), np.block([z8, np.cos(em)]))
    bs = (np.block([np.sin(e0), np.sin(e1)]), np.block([-np.cos(e0), np.cos(e1)]))
    bs0 = (np.block([np.sin(e0), z8]), np.block([z8, np.sin(em)]))

    def wide(pair):
        return np.concatenate([np.kron(np.eye(16), part)[ours] for part in pair], 0)

    b_fwd = np.stack([np.concatenate(list(split_np(wide(m))), axis=1) for m in (bc, bc0)])
    b_inv = np.stack([split_np(wide(m).T) for m in (bc, bc0, bs, bs0)]).reshape(2, 2, 2, 128, 256)
    return w, tx, cy_fwd, cy_inv, ty, b_fwd, b_inv


def dot(x, y):
    return lax.dot_general(x, y, (((1,), (0,)), ((), ())), preferred_element_type=F32)


def dot_nt(x, y):
    return lax.dot_general(x, y, (((1,), (1,)), ((), ())), preferred_element_type=F32)


def split(x):
    high = x.astype(BF)
    return high, (x - high.astype(F32)).astype(BF)


def dot3(x, y):
    return dot(x[0], y[0]) + (dot(x[0], y[1]) + dot(x[1], y[0]))


def dot3_nt(x, y):
    return dot_nt(x[0], y[0]) + (dot_nt(x[0], y[1]) + dot_nt(x[1], y[0]))


def encode(x, y):
    top = jnp.maximum(jnp.maximum(jnp.abs(x), jnp.abs(y)), 2.0**-31)
    exponent = jnp.minimum(jnp.floor(jnp.log2(top)), 31.0)
    scale = jnp.exp2(11.0 - exponent)

    def code(v):
        return jnp.clip(jnp.round(v * scale), -4095.0, 4095.0).astype(I32)

    high = jnp.left_shift(exponent.astype(I32) + 32, 26)
    return high | jnp.left_shift(code(y) & 0x1FFF, 13) | (code(x) & 0x1FFF)


def decode(word):
    scale = jnp.exp2(lax.shift_right_logical(word, 26).astype(F32) - 43.0)
    x = lax.shift_right_arithmetic(jnp.left_shift(word, 19), 19).astype(F32)
    y = lax.shift_right_arithmetic(jnp.left_shift(word, 6), 19).astype(F32)
    return x * scale, y * scale


@functools.lru_cache(None)
def send_order():
    rng = np.random.default_rng(0)
    every = [(dz, dy, dx, dc) for dz in range(8) for dy in range(4) for dx in range(4) for dc in range(2)]
    every = [d for d in every if any(d)]
    hops = {d: min(d[0], 8 - d[0]) + min(d[1], 4 - d[1]) + min(d[2], 4 - d[2]) + 0.5 * d[3] for d in every}
    return sorted(every, key=lambda d: (-hops[d], rng.random()))


def place():
    slab = lax.axis_index("slab")
    cell = lax.axis_index("cell")
    return slab, cell, lax.div(slab, 8), lax.rem(slab, 8) * 2 + cell


def device_at(plane, column):
    return (plane * 8 + lax.div(column, 2), lax.rem(column, 2))


def overlap(bins, low, high):
    return jnp.maximum(jnp.minimum(bins + 1.0, high) - jnp.maximum(bins, low), 0.0)


def kernel(
    row_h, col_h, width_h, height_h, region_h, offset_h,
    w_h, tx_h, cyf_h, cyi_h, ty_h, bf_h, bi_h,
    field_x, field_y, force, sums,
    ci, co, pq, ym, yr, d2, zs, s1, r1, us, vs, gs, aw, pt, s2, r2, zx, fb, pf, pr, e1, e2, es,
    w, w2, tx, cyf, cyi, ty, bf, bi, bi2,
    const_sem, in_sem, met, cell_s, cell_r, a1_s, a1_r, a2_s, a2_r, f_s, f_r, e_s, e_r,
):
    slab, cell, plane, column = place()
    me = plane * 16 + column
    mine, other = cell, 1 - cell
    has_prev = jnp.logical_and(cell == 0, slab > 0)
    has_next = slab < SLABS - 1
    barrier = pltpu.get_barrier_semaphore()

    own = [
        pltpu.make_async_copy(src, ci.at[mine, k], in_sem.at[k])
        for k, src in enumerate((row_h, col_h, width_h, height_h, region_h))
    ]
    own.append(pltpu.make_async_copy(offset_h, co.at[mine], in_sem.at[5]))
    for copy in own:
        copy.start()

    def signal_at(sem, device):
        pl.semaphore_signal(sem, inc=1, device_id=device, device_id_type=MESH)

    @pl.when(has_prev)
    def _():
        signal_at(barrier, (slab - 1, 0))
        signal_at(barrier, (slab - 1, 1))

    py, px = lax.div(plane, 4), lax.rem(plane, 4)
    z, core = lax.div(column, 4) * 2 + cell, lax.rem(lax.div(column, 2), 2)
    ys = [lax.rem(py + k, 4) for k in range(4)]
    xs = [lax.rem(px + k, 4) for k in range(4)]

    plane_peers = [device_at(lax.rem(plane + i, 16), column) for i in range(1, 16)]
    column_peers = [device_at(plane, lax.rem(column + i, 16)) for i in range(1, 16)]
    for device in plane_peers + column_peers:
        signal_at(barrier, device)

    fetched = [
        pltpu.make_async_copy(src, dst, const_sem.at[k])
        for k, (src, dst) in enumerate(
            (
                (tx_h, tx), (w_h, w), (w_h.at[:, 0, 0], w2.at[:, 0:128]), (w_h.at[:, 0, 0], w2.at[:, 128:256]),
                (cyf_h, cyf), (ty_h, ty), (bf_h, bf), (bi_h, bi),
                (bi_h.at[:, 0, 0], bi2.at[:, 0:128]), (bi_h.at[:, 0, 0], bi2.at[:, 128:256]), (cyi_h, cyi),
            )
        )
    ]
    for copy in fetched:
        copy.start()
    for copy in own:
        copy.wait()

    low_row = slab * 16 + cell * 8

    def cell_row_of(slot, k, which):
        return ci[slot, which, k : k + 1, :]

    def make_cells(slot, halves, masked):
        bins = lax.broadcasted_iota(I32, (128, 128), 0).astype(F32)
        line = lax.broadcasted_iota(I32, (16, 128), 0)
        rows = (jnp.bitwise_and(line, 3) + low_row).astype(F32)
        region_of = lax.shift_right_logical(line, 2)
        for k in range(4):
            at = slice(128 * k, 128 * k + 128)
            col = cell_row_of(slot, k, 1)
            high_bits = lax.shift_right_logical(col, 7)
            low_bits = (col - high_bits * 128).astype(F32)
            start = co[slot, 0:1, at]
            end = start + cell_row_of(slot, k, 2).astype(F32)
            reach = bins - low_bits
            pq[slot, 0:128, at] = overlap(reach, start, end).astype(BF)
            pq[slot, 128:256, at] = overlap(reach + 128.0, start, end).astype(BF)
            start = co[slot, 1:2, at]
            end = start + cell_row_of(slot, k, 3).astype(F32)
            reach = rows - cell_row_of(slot, k, 0).astype(F32)
            here = cell_row_of(slot, k, 4) == region_of
            for half in range(halves):
                got = jnp.where(here, overlap(reach + 4.0 * half, start, end), 0.0)
                yr[slot, 16 * half : 16 * half + 16, at] = got.astype(BF).astype(F32)
                for a in range(16):
                    to = slice(256 * half + 16 * a, 256 * half + 16 * a + 16)
                    masked[to, at] = jnp.where(high_bits == a, got, 0.0).astype(BF)

    def send(src, dst, s_sem, r_sem, device):
        return pltpu.make_async_remote_copy(
            src_ref=src, dst_ref=dst, send_sem=s_sem, recv_sem=r_sem, device_id=device, device_id_type=MESH
        )

    pl.semaphore_wait(barrier, 30 + has_next.astype(I32))
    partner = (slab, other)
    give = [
        send(ci.at[mine], ci.at[mine], cell_s.at[0], cell_r.at[0, mine], partner),
        send(co.at[mine], co.at[mine], cell_s.at[1], cell_r.at[1, mine], partner),
    ]
    give_next = [
        send(ci.at[mine], ci.at[2 + mine], cell_s.at[2], cell_r.at[0, 2 + mine], (slab + 1, 0)),
        send(co.at[mine], co.at[2 + mine], cell_s.at[3], cell_r.at[1, 2 + mine], (slab + 1, 0)),
    ]
    for copy in give:
        copy.start()

    @pl.when(has_next)
    def _():
        for copy in give_next:
            copy.start()

    for device in column_peers:
        signal_at(met, device)

    def arrive(slot):
        send(ci.at[slot], ci.at[slot], cell_s.at[0], cell_r.at[0, slot], partner).wait_recv()
        send(co.at[slot], co.at[slot], cell_s.at[1], cell_r.at[1, slot], partner).wait_recv()

    make_cells(mine, 2, ym.at[0])
    d2[...] = dot_nt(ym[0], pq[mine])
    arrive(other)
    make_cells(other, 2, ym.at[0])
    d2[...] += dot_nt(ym[0], pq[other])

    @pl.when(has_prev)
    def _():
        for k in range(2):
            arrive(2 + k)
            make_cells(2 + k, 1, ym.at[k])
        d2[0:256, :] += dot_nt(ym[0, 0:256], pq[2]) + dot_nt(ym[1, 0:256], pq[3])

    zero8 = jnp.zeros((8, 128), F32)
    lane = lax.broadcasted_iota(I32, (1, 128), 1)
    first_group = lane < 32

    fetched[0].wait()

    excess = area = zero8
    for i in range(2):
        here = []
        for a in range(16):
            at = 256 * i + 16 * a
            value = d2[at : at + 16, 0:128]
            if a:
                value = value + d2[at - 16 : at, 128:256]
            here.append(value)
            over = jnp.maximum(value - 1.0, 0.0)
            excess = excess + (over[0:8] + over[8:16])
            area = area + (value[0:8] + value[8:16])
        got = real_spectrum(here)
        for kap in range(16):
            at = slice(32 * kap + 16 * i, 32 * kap + 16 * i + 16)
            if kap == 0:
                pair = (got[0], got[16])
            else:
                (re, im), c, s = got[kap], tx[0, kap : kap + 1, :], tx[1, kap : kap + 1, :]
                pair = (re * c + im * s, im * c - re * s)
            for half, value in enumerate(pair):
                parts = split(value)
                for k in range(2):
                    zs[k, at, 128 * half : 128 * half + 128] = parts[k]
    fetched[1].wait()
    table, first = (w[1, 0, 0], w[1, 0, 1]), (w[1, 1, 0], w[1, 1, 1])
    got = dot3_nt(table, (zs[0], zs[1]))
    fixed = dot3_nt(first, (zs[0, 0:128], zs[1, 0:128]))
    tiles = [got[:, 128 * t : 128 * t + 128] for t in range(4)]
    tiles[0] = jnp.where(first_group, fixed, tiles[0])
    for t in range(2):
        s1[128 * t : 128 * t + 128, :] = encode(tiles[t], tiles[t + 2])

    pl.semaphore_wait(met, 15)
    zs_there = [lax.rem(z + k, 8) for k in range(8)]
    z_parts = [(lax.div(k, 2), lax.rem(k, 2)) for k in zs_there]
    planes = [[ys[dy] * 4 + xs[dx] for dx in range(4)] for dy in range(4)]

    def exchange(src, dst, s_sem, r_sem):
        for dz, dy, dx, dc in send_order():
            zh, zl = z_parts[dz]
            core_to = core if dc == 0 else 1 - core
            slab_to = planes[dy][dx] * 8 + (zh * 2 + core_to)
            send(src(slab_to, zl), dst, s_sem, r_sem, (slab_to, zl)).start()

    exchange(lambda slab_to, cell_to: s1.at[pl.ds(slab_to * 2 + cell_to, 1)], r1.at[cell, pl.ds(slab, 1)], a1_s, a1_r.at[cell])
    r1[cell, pl.ds(slab, 1), :] = s1[pl.ds(me, 1), :]

    tile, k2c = lax.div(me, 128), lax.rem(me, 128)
    lower = k2c < 64
    group = lax.div(lane, 32)
    order = lax.rem(lane, 8)

    def q_of(h):
        kap = 4 * (tile + 2 * h) + group
        return jnp.where(
            kap == 0,
            jnp.where(lower, 32 * k2c, 16 + 32 * (k2c - 64)),
            jnp.where(lower, kap + 32 * k2c, 32 - kap + 32 * (k2c - 64)),
        )

    qs = [q_of(h) for h in range(2)]

    def weigh(i, carry):
        at = pl.multiple_of(i * 16, 16)
        p1 = lax.broadcasted_iota(I32, (16, 128), 0) + at
        up = order < 4
        p = jnp.where(up, p1 + 512 * order, 512 - p1 + 512 * (order - 4))
        p = jnp.where(jnp.logical_and(p1 == 0, jnp.logical_not(up)), 256 + 512 * (order - 4), p)
        p_float = p.astype(F32)
        pt[pl.ds(at, 16), :] = p_float
        for h in range(2):
            q_float = qs[h].astype(F32)
            k2 = p_float * p_float + q_float * q_float
            scale = jnp.where(p == 0, 1.0 / M, 2.0 / M) * jnp.where(qs[h] == 0, 1.0 / M, 2.0 / M) * (1.0 / STEP)
            aw[pl.ds(256 * h + at, 16), :] = jnp.where(k2 == 0.0, 0.0, scale / jnp.where(k2 == 0.0, 1.0, k2))
        return carry

    lax.fori_loop(0, 16, weigh, 0)

    for copy in fetched[2:]:
        copy.wait()
    def half_arrived(k):
        for count, here in ((127, cell == k), (128, cell != k)):

            @pl.when(here)
            def _(count=count):
                send(s1.at[pl.ds(0, count)], r1.at[k, pl.ds(0, count)], a1_s, a1_r.at[k], partner).wait_recv()

    def half_of(k):
        high, low = zip(*(split(v) for v in decode(r1[k])))
        whole = (jnp.concatenate(high, axis=1), jnp.concatenate(low, axis=1))
        at = slice(128 * k, 128 * k + 128)
        return dot3((cyf[0, :, at], cyf[1, :, at]), whole)

    half_arrived(1)
    us[...] = half_of(1)
    half_arrived(0)
    send(s1.at[pl.ds(0, 255)], s1.at[pl.ds(0, 255)], a1_s, a1_r.at[0], partner).wait_send()

    us[...] += half_of(0)

    def y_chunk(i, carry):
        at = i * 16
        c, s = ty[0, pl.ds(at, 16), :], ty[1, pl.ds(at, 16), :]
        for h in range(2):
            lanes = slice(128 * h, 128 * h + 128)
            re, im = us[pl.ds(at, 16), lanes], us[pl.ds(256 + at, 16), lanes]
            for half, value in enumerate((re * c + im * s, im * c - re * s)):
                parts = split(value)
                for k in range(2):
                    vs[k, pl.ds(256 * h + at, 16), 128 * half : 128 * half + 128] = parts[k]
        return carry

    for i in range(16):
        y_chunk(i, 0)

    def y_out(rows, table):
        got = dot(vs[0, rows], table)
        return got[:, 0:128] + (got[:, 128:256] + dot(vs[1, rows], table[:, 0:128]))

    gs[...] = y_out(slice(0, 512), bf[0])
    top_row = lax.broadcasted_iota(I32, (16, 1), 0) == 0
    for h in range(2):
        at = slice(256 * h, 256 * h + 16)
        gs[at, :] = jnp.where(top_row, y_out(at, bf[1]), gs[at, :])

    q_floats = [q.astype(F32) for q in qs]

    def scale_chunk(i, energy):
        at = i * 16
        p_float = pt[pl.ds(at, 16), :]
        for h in range(2):
            value = gs[pl.ds(256 * h + at, 16), :]
            weighted = value * aw[pl.ds(256 * h + at, 16), :]
            work = weighted * value
            energy = energy + (work[0:8] + work[8:16])
            for f, part in enumerate((weighted * q_floats[h], weighted * p_float)):
                parts = split(part)
                for k in range(2):
                    vs[f, pl.ds(256 * h + at, 16), 128 * k : 128 * k + 128] = parts[k]
        return energy

    energy = zero8
    for i in range(16):
        energy = scale_chunk(i, energy)

    def y_inverse(f):
        us[...] = dot(vs[f], bi2[f]) + dot(vs[f, :, 0:128], bi[f, 0, 1])
        for h in range(2):
            at = slice(256 * h, 256 * h + 16)
            fixed = dot3((vs[f, at, 0:128], vs[f, at, 128:256]), (bi[f, 1, 0], bi[f, 1, 1]))
            us[at, :] = jnp.where(top_row, fixed, us[at, :])
        for i in range(16):
            at = i * 16
            c, s = ty[0, at : at + 16, :], ty[1, at : at + 16, :]
            for h in range(2):
                re, im = us[256 * h + at : 256 * h + at + 16, 0:128], us[256 * h + at : 256 * h + at + 16, 128:256]
                for half, value in enumerate((re * c - im * s, re * s + im * c)):
                    parts = split(value)
                    for k in range(2):
                        zs[k, 256 * half + at : 256 * half + at + 16, 128 * h : 128 * h + 128] = parts[k]
        got = dot3((cyi[0], cyi[1]), (zs[0], zs[1]))
        s2[f] = encode(got[:, 0:128], got[:, 128:256]).reshape(2, 128, 128)

    for f in range(2):
        y_inverse(f)
        exchange(
            lambda slab_to, cell_to, f=f: s2.at[f, cell_to, pl.ds(slab_to, 1)], r2.at[f, pl.ds(me, 1)], a2_s.at[f], a2_r.at[f]
        )
        r2[f, pl.ds(me, 1), :] = s2[f, cell, pl.ds(slab, 1), :]

    def total(x):
        return jnp.sum(jnp.sum(x, axis=1, keepdims=True), axis=0, keepdims=True)

    row = jnp.where(
        lane == 0, total(excess), jnp.where(lane == 1, total(area), total(energy) * (1.0 / (STEP * M * M)))
    )
    es[0] = row
    e1[plane] = row
    for i in range(1, 16):
        send(es.at[0], e1.at[plane], e_s.at[0], e_r.at[0], device_at(lax.rem(plane + i, 16), column)).start()
    def push(slot, f, halves):
        got = dot(fb[f, 0 : 256 * halves], pq[slot])
        for k in range(4):
            at = slice(128 * k, 128 * k + 128)
            high_bits = lax.shift_right_logical(cell_row_of(slot, k, 1), 7)
            force = jnp.zeros((1, 128), F32)
            for half in range(halves):
                kept = got[256 * half : 256 * half + 16, at]
                for a in range(1, 16):
                    kept = jnp.where(high_bits == a, got[256 * half + 16 * a : 256 * half + 16 * a + 16, at], kept)
                force = force + jnp.sum(kept * yr[slot, 16 * half : 16 * half + 16, at], axis=0, keepdims=True)
            pf[slot, f : f + 1, at] = force

    def x_gather(f):
        for t in range(2):
            for h, value in enumerate(decode(r2[f, 128 * t : 128 * t + 128, :])):
                parts = split(value.T)
                for k in range(2):
                    for j in range(4):
                        for half in range(2):
                            to = 256 * half + 16 * (4 * (t + 2 * h) + j)
                            zx[to : to + 16, 128 * k : 128 * k + 128] = parts[k][32 * j + 16 * half : 32 * j + 16 * half + 16]

    def x_inverse(f, out, half):
        base = 256 * half
        rows, first = slice(base, base + 256), slice(base, base + 16)
        us[rows, :] = dot(zx[rows], w2[f]) + dot(zx[rows, 0:128], w[f, 0, 1])
        us[first, :] = dot3((zx[first, 0:128], zx[first, 128:256]), (w[f, 1, 0], w[f, 1, 1]))
        got = {}
        for kap in range(16):
            rows = slice(base + 16 * kap, base + 16 * kap + 16)
            re, im = us[rows, 0:128], us[rows, 128:256]
            if kap == 0:
                got[0], got[16] = re, im
            else:
                c, s = tx[0, kap : kap + 1, :], tx[1, kap : kap + 1, :]
                got[kap] = (re * c - im * s, re * s + im * c)
        for a, value in enumerate(real_back(got, 16)):
            lanes = slice(128 * a, 128 * a + 128)
            for g in range(REGIONS):
                out[g, 4 * half : 4 * half + 4, lanes] = value[4 * g : 4 * g + 4]
            near = value.astype(BF)
            fb[f, base + 16 * a : base + 16 * a + 16, 0:128] = near
            if a:
                fb[f, base + 16 * a - 16 : base + 16 * a, 128:256] = near
        fb[f, base + 240 : base + 256, 128:256] = jnp.zeros((16, 128), BF)

    def give_back(slot, device, sem, into):
        return send(pf.at[slot], pr.at[into], f_s.at[sem], f_r.at[into], device)

    def arrived(f):
        whole = send(r2.at[f, pl.ds(0, 255)], r2.at[f, pl.ds(0, 255)], a2_s.at[f], a2_r.at[f], partner)
        whole.wait_recv()
        whole.wait_send()

    arrived(0)
    x_gather(0)
    for half in range(2):
        x_inverse(0, field_x, half)

    @pl.when(has_prev)
    def _():
        for k in range(2):
            push(2 + k, 0, 1)

    push(other, 0, 2)
    push(mine, 0, 2)
    sums_wait = send(e1.at[pl.ds(0, 15)], e1.at[pl.ds(0, 15)], e_s.at[0], e_r.at[0], partner)
    sums_wait.wait_recv()
    sums_wait.wait_send()
    row = jnp.sum(e1[...], axis=0)
    es[1] = row
    e2[column] = row
    for i in range(1, 16):
        send(es.at[1], e2.at[column], e_s.at[1], e_r.at[1], device_at(plane, lax.rem(column + i, 16))).start()
    arrived(1)
    x_gather(1)
    x_inverse(1, field_y, 0)

    @pl.when(has_prev)
    def _():
        for k in range(2):
            push(2 + k, 1, 1)
            give_back(2 + k, (slab - 1, k), 1 + k, 1).start()

    x_inverse(1, field_y, 1)
    push(other, 1, 2)
    give_back(other, partner, 0, 0).start()
    push(mine, 1, 2)

    @pl.when(jnp.logical_not(has_next))
    def _():
        pr[1] = jnp.zeros((2, CELLS_DEV), F32)

    give_back(other, partner, 0, 0).wait_recv()

    @pl.when(has_next)
    def _():
        give_back(other, partner, 0, 1).wait_recv()

    force[...] = pf[mine] + pr[0] + pr[1]

    send(e2.at[pl.ds(0, 15)], e2.at[pl.ds(0, 15)], e_s.at[1], e_r.at[1], partner).wait()
    sums[...] = jnp.sum(e2[...], axis=0)

    give_back(other, partner, 0, 0).wait_send()
    for copy in give:
        copy.wait_send()

    @pl.when(has_prev)
    def _():
        for k in range(2):
            give_back(2 + k, (slab - 1, k), 1 + k, 1).wait_send()

    @pl.when(has_next)
    def _():
        for copy in give_next:
            copy.wait_send()


def finish(field_x, field_y, force, sums, out_x, out_y, out_force, energy, overflow, small, sem):
    row = sums[...]
    small[0] = row[:, 2:3]
    small[1] = row[:, 0:1] / row[:, 1:2]
    pairs = ((field_x, out_x), (field_y, out_y), (force, out_force), (small.at[0], energy), (small.at[1], overflow))
    copies = [pltpu.make_async_copy(src, dst, sem.at[k]) for k, (src, dst) in enumerate(pairs)]
    for copy in copies:
        copy.start()
    for copy in copies:
        copy.wait()


def body(cell_row, cell_col, cell_width, cell_height, cell_region, cell_offset):
    consts = [jnp.asarray(t) for t in tables()]
    whole = [v.reshape(4, 128) for v in (cell_row, cell_col, cell_width, cell_height, cell_region)]
    vmem = pl.BlockSpec(memory_space=pltpu.VMEM)
    hbm = pl.BlockSpec(memory_space=pltpu.HBM)
    V = pltpu.VMEM
    D = pltpu.SemaphoreType.DMA
    scratch = [
        V((4, 5, 4, 128), I32),
        V((4, 2, CELLS_DEV), F32),
        V((4, 256, 512), BF),
        V((2, 512, 512), BF),
        V((4, 32, CELLS_DEV), F32),
        V((512, 256), F32),
        V((2, 512, 256), BF),
        V((256, 128), I32),
        V((2, 128, 128), I32),
        V((512, 256), F32),
        V((2, 512, 256), BF),
        V((512, 128), F32),
        V((512, 128), F32),
        V((256, 128), F32),
        V((2, 2, 128, 128), I32),
        V((2, 256, 128), I32),
        V((512, 256), BF),
        V((2, 512, 256), BF),
        V((4, 2, CELLS_DEV), F32),
        V((2, 2, CELLS_DEV), F32),
        V((16, 1, 128), F32),
        V((16, 1, 128), F32),
        V((2, 1, 128), F32),
        V((2, 2, 2, 128, 256), BF),
        V((2, 256, 256), BF),
        V((2, 16, 128), F32),
        V((2, 512, 256), BF),
        V((2, 256, 512), BF),
        V((2, 256, 128), F32),
        V((2, 256, 256), BF),
        V((2, 2, 2, 128, 256), BF),
        V((2, 256, 256), BF),
        D((11,)), D((6,)),
        pltpu.SemaphoreType.REGULAR,
        D((4,)), D((2, 4)),
        D, D((2,)), D((2,)), D((2,)),
        D((3,)), D((2,)),
        D((2,)), D((2,)),
    ]
    field = (REGIONS, 8, M)
    results = pl.pallas_call(
        kernel,
        out_shape=(V(field, F32), V(field, F32), V((2, CELLS_DEV), F32), V((1, 128), F32)),
        in_specs=[hbm] * (6 + len(consts)),
        out_specs=(vmem,) * 4,
        scratch_shapes=scratch,
        compiler_params=pltpu.CompilerParams(
            collective_id=0, has_side_effects=True, vmem_limit_bytes=66300000
        ),
        name="placement",
    )(*whole, cell_offset, *consts)
    S = jax.ShapeDtypeStruct
    field_x, field_y, force, energy, overflow = pl.pallas_call(
        finish,
        out_shape=(S(field, F32), S(field, F32), S((2, CELLS_DEV), F32), S((1, 1), F32), S((1, 1), F32)),
        in_specs=[vmem] * 4,
        out_specs=(hbm,) * 5,
        scratch_shapes=[V((2, 1, 1), F32), D((5,))],
        compiler_params=pltpu.CompilerParams(vmem_limit_bytes=4 * 1024 * 1024),
        name="finish",
    )(*results)
    return (field_x, field_y, force, energy.reshape(()), overflow.reshape(()))


def solution(mesh):
    both = ("slab", "cell")
    placed = (P(both),) * 5 + (P(None, both),)
    return jax.shard_map(
        body,
        mesh=mesh,
        in_specs=placed,
        out_specs=(P(None, both, None), P(None, both, None), P(None, both), P(), P()),
        check_vma=False,
    )
```

```python
import functools
import math

import jax
import jax.numpy as jnp
import numpy as np
from jax import lax
from jax.experimental import pallas as pl
from jax.experimental.pallas import tpu as pltpu
from jax.sharding import PartitionSpec as P

M = 2048
REGIONS = 4
SLABS = 128
CELLS_DEV = 512
BF = jnp.bfloat16
F32 = jnp.float32
I32 = jnp.int32
MESH = pl.DeviceIdType.MESH
STEP = math.pi / M
FAR = 98
NEXT = 14


def c_add(x,y): return (x[0]+y[0], x[1]+y[1])
def c_sub(x,y): return (x[0]-y[0], x[1]-y[1])
def c_turn(x,angle):
    c,s=math.cos(angle),math.sin(angle)
    if abs(s)<1e-12: return x if c>0 else (-x[0],-x[1])
    if abs(c)<1e-12: return (-x[1],x[0]) if s>0 else (x[1],-x[0])
    if abs(abs(c)-abs(s))<1e-12:
        h=abs(c); a,b=x[0],x[1]
        sc,ss=(1 if c>0 else -1),(1 if s>0 else -1)
        def lin(p,a,q,b):
            if p>0: return (a+b)*h if q>0 else (a-b)*h
            return (b-a)*h if q>0 else (a+b)*(-h)
        return (lin(sc,a,-ss,b), lin(ss,a,sc,b))
    return (x[0]*c-x[1]*s, x[0]*s+x[1]*c)
def c_fft(xs,sign):
    n=len(xs)
    if n==1: return xs
    even,odd=c_fft(xs[0::2],sign),c_fft(xs[1::2],sign)
    out=[None]*n
    for k in range(n//2):
        t=c_turn(odd[k],sign*2*math.pi*k/n)
        out[k],out[k+n//2]=c_add(even[k],t),c_sub(even[k],t)
    return out
def real_spectrum(d):
    n=len(d)
    if n==2:
        return {0:d[0]+d[1],1:(d[0],-d[1]),2:d[0]-d[1]}
    half=n//2
    out={}
    z=[c_turn((d[a],-d[a+half]),-math.pi*a/n) for a in range(half)]
    f=c_fft(z,-1)
    for m in range(half):
        k=1+4*m
        if k<n: out[k]=f[m]
        else: out[2*n-k]=(f[m][0],-f[m][1])
    s=[d[a]+d[a+half] for a in range(half)]
    e=[d[a]-d[a+half] for a in range(half)]
    q=half//2
    z=[c_turn((e[a],-e[a+q]),-2*math.pi*a/n) for a in range(q)]
    f=c_fft(z,-1)
    for l in range(q):
        m=1+4*l
        if m<=half: out[2*m]=f[l]
        else: out[2*(n-m)]=(f[l][0],-f[l][1])
    sub=real_full(s)
    for l,v in sub.items(): out[4*l]=v
    return out
def real_full(s):
    n=len(s)
    if n==2: return {0:s[0]+s[1],1:s[0]-s[1]}
    half=n//2
    p=[s[a]+s[a+half] for a in range(half)]
    e=[s[a]-s[a+half] for a in range(half)]
    out={}
    for l,v in real_full(p).items(): out[2*l]=v
    q=half//2
    if q==0: return out
    z=[c_turn((e[a],-e[a+q]),-2*math.pi*a/n) for a in range(q)] if q else []
    f=c_fft(z,-1)
    for k in range(q):
        l=1+4*k
        if l<=half: out[l]=f[k]
        else: out[n-l]=(f[k][0],-f[k][1])
    return out
def real_full_back(v,n):
    if n==2: return [v[0]+v[1],v[0]-v[1]]
    half=n//2; q=half//2
    p=real_full_back({l//2:x for l,x in v.items() if l%2==0},half)
    if n==4:
        g=[v[1]]
    else:
        g=[v[1+4*k] if 1+4*k<=half else (v[n-1-4*k][0],-v[n-1-4*k][1]) for k in range(q)]
    f=c_fft(g,1)
    odd=[None]*half
    for a in range(q):
        t=c_turn(f[a],2*math.pi*a/n)
        odd[a],odd[a+q]=t[0],-t[1]
    out=[None]*n
    for a in range(half):
        out[a],out[a+half]=p[a]+odd[a],p[a]-odd[a]
    return out
def real_back(y,n):
    half=n//2
    even=real_full_back({k//2:v for k,v in y.items() if k%2==0},n)
    g=[y[1+4*m] if 1+4*m<n else (y[2*n-1-4*m][0],-y[2*n-1-4*m][1]) for m in range(half)]
    f=c_fft(g,1)
    out=[None]*n
    for a in range(half):
        t=c_turn(f[a],math.pi*a/n)
        out[a],out[a+half]=even[a]+t[0],even[a+half]-t[1]
    return out


def split_np(table):
    high = table.astype(np.float32).astype(BF)
    low = (table - high.astype(np.float64)).astype(np.float32).astype(BF)
    return np.stack([high, low])


@functools.lru_cache(None)
def tables():
    pi = np.pi
    k2 = np.arange(64)[:, None]
    b = np.arange(128)[None, :]
    c1, s1 = np.cos(pi * k2 * (2 * b + 1) / 128), np.sin(pi * k2 * (2 * b + 1) / 128)
    c2, s2 = np.cos(pi * (k2 + 1) * (2 * b + 1) / 128), np.sin(pi * (k2 + 1) * (2 * b + 1) / 128)
    cm, sm = np.cos(pi * (2 * k2 + 1) * (2 * b + 1) / 256), np.sin(pi * (2 * k2 + 1) * (2 * b + 1) / 256)
    zero = np.zeros_like(c1)
    wc = np.block([[c1, s1], [c2, -s2]])
    wc0 = np.block([[c1, zero], [zero, cm]])
    ws = np.block([[s1, -c1], [s2, c2]])
    ws0 = np.block([[s1, zero], [zero, sm]])
    w = np.stack([split_np(m) for m in (ws, ws0, wc, wc0)]).reshape(2, 2, 2, 128, 256)
    kap = np.arange(16)[:, None]
    ang = pi * kap * (2 * b + 1) / 4096
    tx = np.stack([np.cos(ang), np.sin(ang)]).astype(np.float32)
    p1 = np.arange(256)[:, None]
    d = np.arange(256)[None, :]
    cre, cim = np.cos(2 * pi * p1 * d / 512), -np.sin(2 * pi * p1 * d / 512)
    cim[0] = (-1.0) ** np.arange(256)
    cy = np.concatenate([cre, cim], 0)[:, np.arange(256).reshape(128, 2).T.reshape(-1)]
    ours = np.arange(128).reshape(4, 4, 2, 4).transpose(0, 2, 1, 3).reshape(-1)
    cy_fwd, cy_inv = split_np(cy), split_np(cy.T)
    r = np.arange(8)
    angy = pi * p1 * (2 * r[None, :] + 1) / 4096
    ty = np.stack([np.tile(np.cos(angy), (1, 16)), np.tile(np.sin(angy), (1, 16))])[:, :, ours].astype(np.float32)
    p2 = np.arange(4)[None, :]
    rr = r[:, None]
    e0, e1 = pi * p2 * (2 * rr + 1) / 8, pi * (p2 + 1) * (2 * rr + 1) / 8
    em = pi * (2 * rr + 1) * (1 + 2 * p2) / 16
    z8 = np.zeros((8, 4))
    bc = (np.block([np.cos(e0), np.cos(e1)]), np.block([np.sin(e0), -np.sin(e1)]))
    bc0 = (np.block([np.cos(e0), z8]), np.block([z8, np.cos(em)]))
    bs = (np.block([np.sin(e0), np.sin(e1)]), np.block([-np.cos(e0), np.cos(e1)]))
    bs0 = (np.block([np.sin(e0), z8]), np.block([z8, np.sin(em)]))

    def wide(pair):
        return np.concatenate([np.kron(np.eye(16), part)[ours] for part in pair], 0)

    b_fwd = np.stack([np.concatenate(list(split_np(wide(m))), axis=1) for m in (bc, bc0)])
    b_inv = np.stack([split_np(wide(m).T) for m in (bc, bc0, bs, bs0)]).reshape(2, 2, 2, 128, 256)
    return w, tx, cy_fwd, cy_inv, ty, b_fwd, b_inv


def dot(x, y):
    return lax.dot_general(x, y, (((1,), (0,)), ((), ())), preferred_element_type=F32)


def dot_nt(x, y):
    return lax.dot_general(x, y, (((1,), (1,)), ((), ())), preferred_element_type=F32)


def split(x):
    high = x.astype(BF)
    return high, (x - high.astype(F32)).astype(BF)


def dot3(x, y):
    return dot(x[0], y[0]) + (dot(x[0], y[1]) + dot(x[1], y[0]))


def dot3_nt(x, y):
    return dot_nt(x[0], y[0]) + (dot_nt(x[0], y[1]) + dot_nt(x[1], y[0]))


def encode(x, y):
    top = jnp.maximum(jnp.maximum(jnp.abs(x), jnp.abs(y)), 2.0**-31)
    exponent = jnp.minimum(jnp.floor(jnp.log2(top)), 31.0)
    scale = jnp.exp2(11.0 - exponent)

    def code(v):
        return jnp.clip(jnp.round(v * scale), -4095.0, 4095.0).astype(I32)

    high = jnp.left_shift(exponent.astype(I32) + 32, 26)
    return high | jnp.left_shift(code(y) & 0x1FFF, 13) | (code(x) & 0x1FFF)


def decode(word):
    scale = jnp.exp2(lax.shift_right_logical(word, 26).astype(F32) - 43.0)
    x = lax.shift_right_arithmetic(jnp.left_shift(word, 19), 19).astype(F32)
    y = lax.shift_right_arithmetic(jnp.left_shift(word, 6), 19).astype(F32)
    return x * scale, y * scale


@functools.lru_cache(None)
def send_order():
    rng = np.random.default_rng(0)
    every = [(dz, dy, dx, dc) for dz in range(8) for dy in range(4) for dx in range(4) for dc in range(2)]
    every = [d for d in every if any(d)]
    hops = {d: min(d[0], 8 - d[0]) + min(d[1], 4 - d[1]) + min(d[2], 4 - d[2]) + 0.5 * d[3] for d in every}
    return sorted(every, key=lambda d: (-hops[d], rng.random()))


def in_two(count, base=0):
    return [slice(base + k * count // 2, base + (k + 1) * count // 2) for k in range(2)]


def place():
    slab = lax.axis_index("slab")
    cell = lax.axis_index("cell")
    return slab, cell, lax.div(slab, 8), lax.rem(slab, 8) * 2 + cell


def device_at(plane, column):
    return (plane * 8 + lax.div(column, 2), lax.rem(column, 2))


def overlap(bins, low, high):
    return jnp.maximum(jnp.minimum(bins + 1.0, high) - jnp.maximum(bins, low), 0.0)


def kernel(
    row_h, col_h, width_h, height_h, region_h, offset_h,
    w_h, tx_h, cyf_h, cyi_h, ty_h, bf_h, bi_h,
    field_x, field_y, force, sums,
    ci, co, pq, ym, yr, d2, zs, s1, r1, us, vs, tops, gs, aw, pt, s2, r2, zx, fb, pf, pr, e1, e2, es,
    w, w2, tx, cyf, cyi, ty, bf, bi, bi2,
    const_sem, in_sem, met, cell_s, cell_r, a1_s, a1_r, a2_s, a2_r, f_s, f_r, e_s, e_r,
):
    slab, cell, plane, column = place()
    me = plane * 16 + column
    mine, other = cell, 1 - cell
    has_prev = jnp.logical_and(cell == 0, slab > 0)
    has_next = slab < SLABS - 1
    barrier = pltpu.get_barrier_semaphore()

    own = [
        pltpu.make_async_copy(src, ci.at[mine, k], in_sem.at[k])
        for k, src in enumerate((row_h, col_h, width_h, height_h, region_h))
    ]
    own.append(pltpu.make_async_copy(offset_h, co.at[mine], in_sem.at[5]))
    for copy in own:
        copy.start()

    def signal_at(sem, device):
        pl.semaphore_signal(sem, inc=1, device_id=device, device_id_type=MESH)

    plane_peers = [device_at(lax.rem(plane + i, 16), column) for i in (10, 6, 9, 11, 5, 7, 8, 2, 14, 13, 3, 4, 12, 1, 15)]
    column_peers = [device_at(plane, lax.rem(column + i, 16)) for i in (8, 7, 9, 6, 10, 5, 11, 4, 12, 3, 13, 2, 14, 1, 15)]
    for device in plane_peers + column_peers:
        signal_at(barrier, device)

    @pl.when(has_prev)
    def _():
        signal_at(barrier, (slab - 1, 0))
        signal_at(barrier, (slab - 1, 1))

    py, px = lax.div(plane, 4), lax.rem(plane, 4)
    z, core = lax.div(column, 4) * 2 + cell, lax.rem(lax.div(column, 2), 2)
    ys = [lax.rem(py + k, 4) for k in range(4)]
    xs = [lax.rem(px + k, 4) for k in range(4)]

    for copy in own:
        copy.wait()

    low_row = slab * 16 + cell * 8

    def cell_row_of(slot, k, which):
        return ci[slot, which, k : k + 1, :]

    def make_cells(slot, halves, masked):
        bins = lax.broadcasted_iota(I32, (128, 128), 0).astype(F32)
        line = lax.broadcasted_iota(I32, (16, 128), 0)
        rows = (jnp.bitwise_and(line, 3) + low_row).astype(F32)
        region_of = lax.shift_right_logical(line, 2)
        for k in range(4):
            at = slice(128 * k, 128 * k + 128)
            col = cell_row_of(slot, k, 1)
            high_bits = lax.shift_right_logical(col, 7)
            low_bits = (col - high_bits * 128).astype(F32)
            start = co[slot, 0:1, at]
            end = start + cell_row_of(slot, k, 2).astype(F32)
            reach = bins - low_bits
            pq[slot, 0:128, at] = overlap(reach, start, end).astype(BF)
            pq[slot, 128:256, at] = overlap(reach + 128.0, start, end).astype(BF)
            start = co[slot, 1:2, at]
            end = start + cell_row_of(slot, k, 3).astype(F32)
            reach = rows - cell_row_of(slot, k, 0).astype(F32)
            here = cell_row_of(slot, k, 4) == region_of
            for half in range(halves):
                got = jnp.where(here, overlap(reach + 4.0 * half, start, end), 0.0)
                yr[slot, 16 * half : 16 * half + 16, at] = got.astype(BF).astype(F32)
                for a in range(16):
                    to = slice(256 * half + 16 * a, 256 * half + 16 * a + 16)
                    masked[to, at] = jnp.where(high_bits == a, got, 0.0).astype(BF)

    def send(src, dst, s_sem, r_sem, device):
        return pltpu.make_async_remote_copy(
            src_ref=src, dst_ref=dst, send_sem=s_sem, recv_sem=r_sem, device_id=device, device_id_type=MESH
        )

    pl.semaphore_wait(barrier, 30 + has_next.astype(I32))
    partner = (slab, other)
    give = [
        send(ci.at[mine], ci.at[mine], cell_s.at[0], cell_r.at[0, mine], partner),
        send(co.at[mine], co.at[mine], cell_s.at[1], cell_r.at[1, mine], partner),
    ]
    give_next = [
        send(ci.at[mine], ci.at[2 + mine], cell_s.at[2], cell_r.at[0, 2 + mine], (slab + 1, 0)),
        send(co.at[mine], co.at[2 + mine], cell_s.at[3], cell_r.at[1, 2 + mine], (slab + 1, 0)),
    ]
    for copy in give:
        copy.start()

    @pl.when(has_next)
    def _():
        for copy in give_next:
            copy.start()

    for device in column_peers:
        signal_at(met, device)

    fetched = [
        pltpu.make_async_copy(src, dst, const_sem.at[k])
        for k, (src, dst) in enumerate(
            (
                (tx_h, tx), (w_h, w), (w_h.at[:, 0, 0], w2.at[:, 0:128]), (w_h.at[:, 0, 0], w2.at[:, 128:256]),
                (cyf_h, cyf), (ty_h, ty), (bf_h, bf), (bi_h, bi),
                (bi_h.at[:, 0, 0], bi2.at[:, 0:128]), (bi_h.at[:, 0, 0], bi2.at[:, 128:256]), (cyi_h, cyi),
            )
        )
    ]
    for copy in fetched:
        copy.start()

    def arrive(slot):
        send(ci.at[slot], ci.at[slot], cell_s.at[0], cell_r.at[0, slot], partner).wait_recv()
        send(co.at[slot], co.at[slot], cell_s.at[1], cell_r.at[1, slot], partner).wait_recv()

    make_cells(mine, 2, ym.at[0])
    for rows in in_two(512):
        d2[rows] = dot_nt(ym[0, rows], pq[mine])
    arrive(other)
    make_cells(other, 2, ym.at[0])
    for rows in in_two(512):
        d2[rows] += dot_nt(ym[0, rows], pq[other])

    @pl.when(has_prev)
    def _():
        for k in range(2):
            arrive(2 + k)
            make_cells(2 + k, 1, ym.at[k])
        d2[0:256, :] += dot_nt(ym[0, 0:256], pq[2]) + dot_nt(ym[1, 0:256], pq[3])

    zero8 = jnp.zeros((8, 128), F32)
    lane = lax.broadcasted_iota(I32, (1, 128), 1)
    first_group = lane < 32

    fetched[0].wait()

    excess = area = zero8
    for i in range(2):
        here = []
        for a in range(16):
            at = 256 * i + 16 * a
            value = d2[at : at + 16, 0:128]
            if a:
                value = value + d2[at - 16 : at, 128:256]
            here.append(value)
            over = jnp.maximum(value - 1.0, 0.0)
            excess = excess + (over[0:8] + over[8:16])
            area = area + (value[0:8] + value[8:16])
        got = real_spectrum(here)
        for kap in range(16):
            at = slice(32 * kap + 16 * i, 32 * kap + 16 * i + 16)
            if kap == 0:
                pair = (got[0], got[16])
            else:
                (re, im), c, s = got[kap], tx[0, kap : kap + 1, :], tx[1, kap : kap + 1, :]
                pair = (re * c + im * s, im * c - re * s)
            for half, value in enumerate(pair):
                parts = split(value)
                for k in range(2):
                    zs[k, at, 128 * half : 128 * half + 128] = parts[k]
    fetched[1].wait()
    table, first = (w[1, 0, 0], w[1, 0, 1]), (w[1, 1, 0], w[1, 1, 1])
    got = dot3_nt(table, (zs[0], zs[1]))
    fixed = dot3_nt(first, (zs[0, 0:128], zs[1, 0:128]))
    tiles = [got[:, 128 * t : 128 * t + 128] for t in range(4)]
    tiles[0] = jnp.where(first_group, fixed, tiles[0])
    for t in range(2):
        s1[128 * t : 128 * t + 128, :] = encode(tiles[t], tiles[t + 2])

    pl.semaphore_wait(met, 15)
    planes = [[ys[dy] * 4 + xs[dx] for dx in range(4)] for dy in range(4)]
    z_there = [lax.rem(z + k, 8) for k in range(8)]
    z_parts = [(lax.div(k, 2), lax.rem(k, 2)) for k in z_there]

    def exchange(src, dst, s_sem, r_sem, part=slice(None)):
        for dz, dy, dx, dc in send_order()[part]:
            zh, zl = z_parts[dz]
            slab_to = planes[dy][dx] * 8 + (zh * 2 + (core if dc == 0 else 1 - core))
            send(src(slab_to, zl), dst, s_sem, r_sem, (slab_to, zl)).start()

    exchange(lambda slab_to, cell_to: s1.at[pl.ds(slab_to * 2 + cell_to, 1)], r1.at[cell, pl.ds(slab, 1)], a1_s, a1_r.at[cell])
    r1[cell, pl.ds(slab, 1), :] = s1[pl.ds(me, 1), :]

    tile, k2c = lax.div(me, 128), lax.rem(me, 128)
    lower = k2c < 64
    group = lax.div(lane, 32)
    order = lax.rem(lane, 8)

    def q_of(h):
        kap = 4 * (tile + 2 * h) + group
        return jnp.where(
            kap == 0,
            jnp.where(lower, 32 * k2c, 16 + 32 * (k2c - 64)),
            jnp.where(lower, kap + 32 * k2c, 32 - kap + 32 * (k2c - 64)),
        )

    qs = [q_of(h) for h in range(2)]

    def weigh(i, carry):
        at = pl.multiple_of(i * 16, 16)
        p1 = lax.broadcasted_iota(I32, (16, 128), 0) + at
        up = order < 4
        p = jnp.where(up, p1 + 512 * order, 512 - p1 + 512 * (order - 4))
        p = jnp.where(jnp.logical_and(p1 == 0, jnp.logical_not(up)), 256 + 512 * (order - 4), p)
        p_float = p.astype(F32)
        pt[pl.ds(at, 16), :] = p_float
        for h in range(2):
            q_float = qs[h].astype(F32)
            k2 = p_float * p_float + q_float * q_float
            scale = jnp.where(p == 0, 1.0 / M, 2.0 / M) * jnp.where(qs[h] == 0, 1.0 / M, 2.0 / M) * (1.0 / STEP)
            aw[pl.ds(256 * h + at, 16), :] = jnp.where(k2 == 0.0, 0.0, scale / jnp.where(k2 == 0.0, 1.0, k2))
        return carry

    lax.fori_loop(0, 16, weigh, 0)

    for copy in fetched[2:]:
        copy.wait()
    def half_arrived(k):
        for count, here in ((127, cell == k), (128, cell != k)):

            @pl.when(here)
            def _(count=count):
                send(s1.at[pl.ds(0, count)], r1.at[k, pl.ds(0, count)], a1_s, a1_r.at[k], partner).wait_recv()

    def half_of(k):
        high, low = zip(*(split(v) for v in decode(r1[k])))
        whole = (jnp.concatenate(high, axis=1), jnp.concatenate(low, axis=1))
        at = slice(128 * k, 128 * k + 128)
        return [(rows, dot3((cyf[0, rows, at], cyf[1, rows, at]), whole)) for rows in in_two(512)]

    half_arrived(1)
    for rows, got in half_of(1):
        us[rows] = got
    half_arrived(0)
    send(s1.at[pl.ds(0, 255)], s1.at[pl.ds(0, 255)], a1_s, a1_r.at[0], partner).wait_send()

    for rows, got in half_of(0):
        us[rows] += got

    def y_chunk(i, carry):
        at = i * 16
        c, s = ty[0, pl.ds(at, 16), :], ty[1, pl.ds(at, 16), :]
        for h in range(2):
            lanes = slice(128 * h, 128 * h + 128)
            re, im = us[pl.ds(at, 16), lanes], us[pl.ds(256 + at, 16), lanes]
            for half, value in enumerate((re * c + im * s, im * c - re * s)):
                parts = split(value)
                for k in range(2):
                    vs[k, pl.ds(256 * h + at, 16), 128 * half : 128 * half + 128] = parts[k]
        return carry

    for i in range(16):
        y_chunk(i, 0)

    def y_out(rows, table):
        got = dot(vs[0, rows], table)
        return got[:, 0:128] + (got[:, 128:256] + dot(vs[1, rows], table[:, 0:128]))

    for rows in in_two(512):
        gs[rows] = y_out(rows, bf[0])
    top_row = lax.broadcasted_iota(I32, (16, 1), 0) == 0
    for h in range(2):
        at = slice(256 * h, 256 * h + 16)
        gs[at, :] = jnp.where(top_row, y_out(at, bf[1]), gs[at, :])

    q_floats = [q.astype(F32) for q in qs]

    def scale_chunk(i, energy):
        at = i * 16
        p_float = pt[pl.ds(at, 16), :]
        for h in range(2):
            value = gs[pl.ds(256 * h + at, 16), :]
            weighted = value * aw[pl.ds(256 * h + at, 16), :]
            work = weighted * value
            energy = energy + (work[0:8] + work[8:16])
            for f, part in enumerate((weighted * q_floats[h], weighted * p_float)):
                parts = split(part)
                for k in range(2):
                    vs[f, pl.ds(256 * h + at, 16), 128 * k : 128 * k + 128] = parts[k]
        return energy

    energy = zero8
    for i in range(16):
        energy = scale_chunk(i, energy)

    def top_rows(f, h):
        at = slice(256 * h, 256 * h + 16)
        return dot3((vs[f, at, 0:128], vs[f, at, 128:256]), (bi[f, 1, 0], bi[f, 1, 1]))

    def turned(values, c, s):
        re, im = values[:, 0:128], values[:, 128:256]
        return [split(value) for value in (re * c - im * s, re * s + im * c)]

    def keep_turned(values, h, at):
        for half in range(2):
            for k in range(2):
                zs[k, pl.ds(256 * half + at, values[half][k].shape[0]), 128 * h : 128 * h + 128] = values[half][k]

    def copies_of(f):
        return (
            lambda slab_to, cell_to: s2.at[f, cell_to, pl.ds(slab_to, 1)], r2.at[f, pl.ds(me, 1)], a2_s.at[f], a2_r.at[f]
        )

    for rows in in_two(512):
        us[rows] = dot(vs[0, rows], bi2[0]) + dot(vs[0, rows, 0:128], bi[0, 0, 1])
    for h in range(2):
        at = slice(256 * h, 256 * h + 16)
        us[at, :] = jnp.where(top_row, top_rows(0, h), us[at, :])
        tops[h] = top_rows(1, h)
    for i in range(16):
        for h in range(2):
            at = slice(16 * i, 16 * i + 16)
            keep_turned(turned(us[256 * h + 16 * i : 256 * h + 16 * i + 16, :], ty[0, at, :], ty[1, at, :]), h, 16 * i)
    for k, rows in enumerate(in_two(256)):
        got = dot3((cyi[0, rows], cyi[1, rows]), (zs[0], zs[1]))
        s2[0, k] = encode(got[:, 0:128], got[:, 128:256])
    r2[0, pl.ds(me, 1), :] = s2[0, cell, pl.ds(slab, 1), :]

    for i in range(2):
        at = 128 * i
        rows = [vs[1, 256 * h + at : 256 * h + at + 128, :] for h in range(2)]
        c, s = ty[0, at : at + 128, :], ty[1, at : at + 128, :]
        top = [tops[h] for h in range(2)]
        got = [dot(r, bi2[1]) + dot(r[:, 0:128], bi[1, 0, 1]) for r in rows]
        values = []
        for h in range(2):
            value = got[h]
            if i == 0:
                value = jnp.concatenate([jnp.where(top_row, top[h], value[0:16]), value[16:]], axis=0)
            values.append(turned(value, c, s))
        exchange(*copies_of(0), part=slice(FAR // 2 * i, FAR // 2 * i + FAR // 2))
        for h in range(2):
            keep_turned(values[h], h, at)

    for k, rows in enumerate(in_two(256)):
        got = dot3((cyi[0, rows], cyi[1, rows]), (zs[0], zs[1]))
        s2[1, k] = encode(got[:, 0:128], got[:, 128:256])
    exchange(*copies_of(1), part=slice(0, NEXT))
    exchange(*copies_of(0), part=slice(FAR, None))
    exchange(*copies_of(1), part=slice(NEXT, None))
    r2[1, pl.ds(me, 1), :] = s2[1, cell, pl.ds(slab, 1), :]

    def total(x):
        return jnp.sum(jnp.sum(x, axis=1, keepdims=True), axis=0, keepdims=True)

    row = jnp.where(
        lane == 0, total(excess), jnp.where(lane == 1, total(area), total(energy) * (1.0 / (STEP * M * M)))
    )
    es[0] = row
    e1[plane] = row
    for i in range(1, 16):
        send(es.at[0], e1.at[plane], e_s.at[0], e_r.at[0], device_at(lax.rem(plane + i, 16), column)).start()
    def push(slot, f, halves):
        got = dot(fb[f, 0 : 256 * halves], pq[slot])
        for k in range(4):
            at = slice(128 * k, 128 * k + 128)
            high_bits = lax.shift_right_logical(cell_row_of(slot, k, 1), 7)
            force = jnp.zeros((1, 128), F32)
            for half in range(halves):
                kept = got[256 * half : 256 * half + 16, at]
                for a in range(1, 16):
                    kept = jnp.where(high_bits == a, got[256 * half + 16 * a : 256 * half + 16 * a + 16, at], kept)
                force = force + jnp.sum(kept * yr[slot, 16 * half : 16 * half + 16, at], axis=0, keepdims=True)
            pf[slot, f : f + 1, at] = force

    def x_gather(f):
        for t in range(2):
            for h, value in enumerate(decode(r2[f, 128 * t : 128 * t + 128, :])):
                parts = split(value.T)
                for k in range(2):
                    for j in range(4):
                        for half in range(2):
                            to = 256 * half + 16 * (4 * (t + 2 * h) + j)
                            zx[to : to + 16, 128 * k : 128 * k + 128] = parts[k][32 * j + 16 * half : 32 * j + 16 * half + 16]

    def x_product(f, halves):
        base, count = 256 * halves[0], 256 * len(halves)
        for rows in in_two(count, base):
            us[rows, :] = dot(zx[rows], w2[f]) + dot(zx[rows, 0:128], w[f, 0, 1])
        for half in halves:
            first = slice(256 * half, 256 * half + 16)
            us[first, :] = dot3((zx[first, 0:128], zx[first, 128:256]), (w[f, 1, 0], w[f, 1, 1]))

    def x_inverse(f, out, half):
        base = 256 * half
        got = {}
        for kap in range(16):
            rows = slice(base + 16 * kap, base + 16 * kap + 16)
            re, im = us[rows, 0:128], us[rows, 128:256]
            if kap == 0:
                got[0], got[16] = re, im
            else:
                c, s = tx[0, kap : kap + 1, :], tx[1, kap : kap + 1, :]
                got[kap] = (re * c - im * s, re * s + im * c)
        for a, value in enumerate(real_back(got, 16)):
            lanes = slice(128 * a, 128 * a + 128)
            for g in range(REGIONS):
                out[g, 4 * half : 4 * half + 4, lanes] = value[4 * g : 4 * g + 4]
            near = value.astype(BF)
            fb[f, base + 16 * a : base + 16 * a + 16, 0:128] = near
            if a:
                fb[f, base + 16 * a - 16 : base + 16 * a, 128:256] = near
        fb[f, base + 240 : base + 256, 128:256] = jnp.zeros((16, 128), BF)

    def give_back(slot, device, sem, into):
        return send(pf.at[slot], pr.at[into], f_s.at[sem], f_r.at[into], device)

    def arrived(f):
        whole = send(r2.at[f, pl.ds(0, 255)], r2.at[f, pl.ds(0, 255)], a2_s.at[f], a2_r.at[f], partner)
        whole.wait_recv()
        whole.wait_send()

    arrived(0)
    x_gather(0)
    x_product(0, (0, 1))
    for half in range(2):
        x_inverse(0, field_x, half)

    @pl.when(has_prev)
    def _():
        for k in range(2):
            push(2 + k, 0, 1)

    push(other, 0, 2)
    push(mine, 0, 2)
    sums_wait = send(e1.at[pl.ds(0, 15)], e1.at[pl.ds(0, 15)], e_s.at[0], e_r.at[0], partner)
    sums_wait.wait_recv()
    sums_wait.wait_send()
    row = jnp.sum(e1[...], axis=0)
    es[1] = row
    e2[column] = row
    for i in range(1, 16):
        send(es.at[1], e2.at[column], e_s.at[1], e_r.at[1], device_at(plane, lax.rem(column + i, 16))).start()
    arrived(1)
    x_gather(1)
    x_product(1, (0,))
    x_inverse(1, field_y, 0)

    @pl.when(has_prev)
    def _():
        for k in range(2):
            push(2 + k, 1, 1)
        for k in range(2):
            give_back(2 + k, (slab - 1, k), 1 + k, 1).start()

    x_product(1, (1,))
    x_inverse(1, field_y, 1)
    push(other, 1, 2)
    give_back(other, partner, 0, 0).start()
    push(mine, 1, 2)

    @pl.when(jnp.logical_not(has_next))
    def _():
        pr[1] = jnp.zeros((2, CELLS_DEV), F32)

    give_back(other, partner, 0, 0).wait_recv()

    @pl.when(has_next)
    def _():
        give_back(other, partner, 0, 1).wait_recv()

    force[...] = pf[mine] + pr[0] + pr[1]

    send(e2.at[pl.ds(0, 15)], e2.at[pl.ds(0, 15)], e_s.at[1], e_r.at[1], partner).wait()
    sums[...] = jnp.sum(e2[...], axis=0)

    give_back(other, partner, 0, 0).wait_send()
    for copy in give:
        copy.wait_send()

    @pl.when(has_prev)
    def _():
        for k in range(2):
            give_back(2 + k, (slab - 1, k), 1 + k, 1).wait_send()

    @pl.when(has_next)
    def _():
        for copy in give_next:
            copy.wait_send()


def finish(field_x, field_y, force, sums, out_x, out_y, out_force, energy, overflow, small, sem):
    row = sums[...]
    small[0] = row[:, 2:3]
    small[1] = row[:, 0:1] / row[:, 1:2]
    pairs = ((field_x, out_x), (field_y, out_y), (force, out_force), (small.at[0], energy), (small.at[1], overflow))
    copies = [pltpu.make_async_copy(src, dst, sem.at[k]) for k, (src, dst) in enumerate(pairs)]
    for copy in copies:
        copy.start()
    for copy in copies:
        copy.wait()


def body(cell_row, cell_col, cell_width, cell_height, cell_region, cell_offset):
    consts = [jnp.asarray(t) for t in tables()]
    whole = [v.reshape(4, 128) for v in (cell_row, cell_col, cell_width, cell_height, cell_region)]
    vmem = pl.BlockSpec(memory_space=pltpu.VMEM)
    hbm = pl.BlockSpec(memory_space=pltpu.HBM)
    V = pltpu.VMEM
    D = pltpu.SemaphoreType.DMA
    scratch = [
        V((4, 5, 4, 128), I32),
        V((4, 2, CELLS_DEV), F32),
        V((4, 256, 512), BF),
        V((2, 512, 512), BF),
        V((4, 32, CELLS_DEV), F32),
        V((512, 256), F32),
        V((2, 512, 256), BF),
        V((256, 128), I32),
        V((2, 128, 128), I32),
        V((512, 256), F32),
        V((2, 512, 256), BF),
        V((2, 16, 256), F32),
        V((512, 128), F32),
        V((512, 128), F32),
        V((256, 128), F32),
        V((2, 2, 128, 128), I32),
        V((2, 256, 128), I32),
        V((512, 256), BF),
        V((2, 512, 256), BF),
        V((4, 2, CELLS_DEV), F32),
        V((2, 2, CELLS_DEV), F32),
        V((16, 1, 128), F32),
        V((16, 1, 128), F32),
        V((2, 1, 128), F32),
        V((2, 2, 2, 128, 256), BF),
        V((2, 256, 256), BF),
        V((2, 16, 128), F32),
        V((2, 512, 256), BF),
        V((2, 256, 512), BF),
        V((2, 256, 128), F32),
        V((2, 256, 256), BF),
        V((2, 2, 2, 128, 256), BF),
        V((2, 256, 256), BF),
        D((11,)), D((6,)),
        pltpu.SemaphoreType.REGULAR,
        D((4,)), D((2, 4)),
        D, D((2,)), D((2,)), D((2,)),
        D((3,)), D((2,)),
        D((2,)), D((2,)),
    ]
    field = (REGIONS, 8, M)
    results = pl.pallas_call(
        kernel,
        out_shape=(V(field, F32), V(field, F32), V((2, CELLS_DEV), F32), V((1, 128), F32)),
        in_specs=[hbm] * (6 + len(consts)),
        out_specs=(vmem,) * 4,
        scratch_shapes=scratch,
        compiler_params=pltpu.CompilerParams(
            collective_id=0, has_side_effects=True, vmem_limit_bytes=66300000
        ),
        name="placement",
    )(*whole, cell_offset, *consts)
    S = jax.ShapeDtypeStruct
    field_x, field_y, force, energy, overflow = pl.pallas_call(
        finish,
        out_shape=(S(field, F32), S(field, F32), S((2, CELLS_DEV), F32), S((1, 1), F32), S((1, 1), F32)),
        in_specs=[vmem] * 4,
        out_specs=(hbm,) * 5,
        scratch_shapes=[V((2, 1, 1), F32), D((5,))],
        compiler_params=pltpu.CompilerParams(vmem_limit_bytes=4 * 1024 * 1024),
        name="finish",
    )(*results)
    return (field_x, field_y, force, energy.reshape(()), overflow.reshape(()))


def solution(mesh):
    both = ("slab", "cell")
    placed = (P(both),) * 5 + (P(None, both),)
    return jax.shard_map(
        body,
        mesh=mesh,
        in_specs=placed,
        out_specs=(P(None, both, None), P(None, both, None), P(None, both), P(), P()),
        check_vma=False,
    )
```

```python
import functools
import math

import jax
import jax.numpy as jnp
import numpy as np
from jax import lax
from jax.experimental import pallas as pl
from jax.experimental.pallas import tpu as pltpu
from jax.sharding import PartitionSpec as P

M = 2048
REGIONS = 4
SLABS = 128
CELLS_DEV = 512
BF = jnp.bfloat16
F32 = jnp.float32
I32 = jnp.int32
MESH = pl.DeviceIdType.MESH
STEP = math.pi / M
FAR = 98
NEXT = 14


def c_add(x,y): return (x[0]+y[0], x[1]+y[1])
def c_sub(x,y): return (x[0]-y[0], x[1]-y[1])
def c_turn(x,angle):
    c,s=math.cos(angle),math.sin(angle)
    if abs(s)<1e-12: return x if c>0 else (-x[0],-x[1])
    if abs(c)<1e-12: return (-x[1],x[0]) if s>0 else (x[1],-x[0])
    if abs(abs(c)-abs(s))<1e-12:
        h=abs(c); a,b=x[0],x[1]
        sc,ss=(1 if c>0 else -1),(1 if s>0 else -1)
        def lin(p,a,q,b):
            if p>0: return (a+b)*h if q>0 else (a-b)*h
            return (b-a)*h if q>0 else (a+b)*(-h)
        return (lin(sc,a,-ss,b), lin(ss,a,sc,b))
    return (x[0]*c-x[1]*s, x[0]*s+x[1]*c)
def c_fft(xs,sign):
    n=len(xs)
    if n==1: return xs
    even,odd=c_fft(xs[0::2],sign),c_fft(xs[1::2],sign)
    out=[None]*n
    for k in range(n//2):
        t=c_turn(odd[k],sign*2*math.pi*k/n)
        out[k],out[k+n//2]=c_add(even[k],t),c_sub(even[k],t)
    return out
def real_spectrum(d):
    n=len(d)
    if n==2:
        return {0:d[0]+d[1],1:(d[0],-d[1]),2:d[0]-d[1]}
    half=n//2
    out={}
    z=[c_turn((d[a],-d[a+half]),-math.pi*a/n) for a in range(half)]
    f=c_fft(z,-1)
    for m in range(half):
        k=1+4*m
        if k<n: out[k]=f[m]
        else: out[2*n-k]=(f[m][0],-f[m][1])
    s=[d[a]+d[a+half] for a in range(half)]
    e=[d[a]-d[a+half] for a in range(half)]
    q=half//2
    z=[c_turn((e[a],-e[a+q]),-2*math.pi*a/n) for a in range(q)]
    f=c_fft(z,-1)
    for l in range(q):
        m=1+4*l
        if m<=half: out[2*m]=f[l]
        else: out[2*(n-m)]=(f[l][0],-f[l][1])
    sub=real_full(s)
    for l,v in sub.items(): out[4*l]=v
    return out
def real_full(s):
    n=len(s)
    if n==2: return {0:s[0]+s[1],1:s[0]-s[1]}
    half=n//2
    p=[s[a]+s[a+half] for a in range(half)]
    e=[s[a]-s[a+half] for a in range(half)]
    out={}
    for l,v in real_full(p).items(): out[2*l]=v
    q=half//2
    if q==0: return out
    z=[c_turn((e[a],-e[a+q]),-2*math.pi*a/n) for a in range(q)] if q else []
    f=c_fft(z,-1)
    for k in range(q):
        l=1+4*k
        if l<=half: out[l]=f[k]
        else: out[n-l]=(f[k][0],-f[k][1])
    return out
def real_full_back(v,n):
    if n==2: return [v[0]+v[1],v[0]-v[1]]
    half=n//2; q=half//2
    p=real_full_back({l//2:x for l,x in v.items() if l%2==0},half)
    if n==4:
        g=[v[1]]
    else:
        g=[v[1+4*k] if 1+4*k<=half else (v[n-1-4*k][0],-v[n-1-4*k][1]) for k in range(q)]
    f=c_fft(g,1)
    odd=[None]*half
    for a in range(q):
        t=c_turn(f[a],2*math.pi*a/n)
        odd[a],odd[a+q]=t[0],-t[1]
    out=[None]*n
    for a in range(half):
        out[a],out[a+half]=p[a]+odd[a],p[a]-odd[a]
    return out
def real_back(y,n):
    half=n//2
    even=real_full_back({k//2:v for k,v in y.items() if k%2==0},n)
    g=[y[1+4*m] if 1+4*m<n else (y[2*n-1-4*m][0],-y[2*n-1-4*m][1]) for m in range(half)]
    f=c_fft(g,1)
    out=[None]*n
    for a in range(half):
        t=c_turn(f[a],math.pi*a/n)
        out[a],out[a+half]=even[a]+t[0],even[a+half]-t[1]
    return out


def split_np(table):
    high = table.astype(np.float32).astype(BF)
    low = (table - high.astype(np.float64)).astype(np.float32).astype(BF)
    return np.stack([high, low])


@functools.lru_cache(None)
def tables():
    pi = np.pi
    k2 = np.arange(64)[:, None]
    b = np.arange(128)[None, :]
    c1, s1 = np.cos(pi * k2 * (2 * b + 1) / 128), np.sin(pi * k2 * (2 * b + 1) / 128)
    c2, s2 = np.cos(pi * (k2 + 1) * (2 * b + 1) / 128), np.sin(pi * (k2 + 1) * (2 * b + 1) / 128)
    cm, sm = np.cos(pi * (2 * k2 + 1) * (2 * b + 1) / 256), np.sin(pi * (2 * k2 + 1) * (2 * b + 1) / 256)
    zero = np.zeros_like(c1)
    wc = np.block([[c1, s1], [c2, -s2]])
    wc0 = np.block([[c1, zero], [zero, cm]])
    ws = np.block([[s1, -c1], [s2, c2]])
    ws0 = np.block([[s1, zero], [zero, sm]])
    w = np.stack([split_np(m) for m in (ws, ws0, wc, wc0)]).reshape(2, 2, 2, 128, 256)
    wt = np.stack([np.concatenate(list(split_np(m.T)), axis=1) for m in (wc, wc0)])
    kap = np.arange(16)[:, None]
    ang = pi * kap * (2 * b + 1) / 4096
    tx = np.stack([np.cos(ang), np.sin(ang)]).astype(np.float32)
    p1 = np.arange(256)[:, None]
    d = np.arange(256)[None, :]
    cre, cim = np.cos(2 * pi * p1 * d / 512), -np.sin(2 * pi * p1 * d / 512)
    cim[0] = (-1.0) ** np.arange(256)
    cy = np.concatenate([cre, cim], 0)[:, np.arange(256).reshape(128, 2).T.reshape(-1)]
    ours = np.arange(128).reshape(4, 4, 2, 4).transpose(0, 2, 1, 3).reshape(-1)
    cy_fwd = split_np(cy)
    r = np.arange(8)
    angy = pi * p1 * (2 * r[None, :] + 1) / 4096
    ty = np.stack([np.tile(np.cos(angy), (1, 16)), np.tile(np.sin(angy), (1, 16))])[:, :, ours].astype(np.float32)
    p2 = np.arange(4)[None, :]
    rr = r[:, None]
    e0, e1 = pi * p2 * (2 * rr + 1) / 8, pi * (p2 + 1) * (2 * rr + 1) / 8
    em = pi * (2 * rr + 1) * (1 + 2 * p2) / 16
    z8 = np.zeros((8, 4))
    bc = (np.block([np.cos(e0), np.cos(e1)]), np.block([np.sin(e0), -np.sin(e1)]))
    bc0 = (np.block([np.cos(e0), z8]), np.block([z8, np.cos(em)]))
    bs = (np.block([np.sin(e0), np.sin(e1)]), np.block([-np.cos(e0), np.cos(e1)]))
    bs0 = (np.block([np.sin(e0), z8]), np.block([z8, np.sin(em)]))

    def wide(pair):
        return np.concatenate([np.kron(np.eye(16), part)[ours] for part in pair], 0)

    b_fwd = np.stack([np.concatenate(list(split_np(wide(m))), axis=1) for m in (bc, bc0)])
    b_inv = np.stack([split_np(wide(m).T) for m in (bc, bc0, bs, bs0)]).reshape(2, 2, 2, 128, 256)
    return w, wt, tx, cy_fwd, ty, b_fwd, b_inv


def dot(x, y):
    return lax.dot_general(x, y, (((1,), (0,)), ((), ())), preferred_element_type=F32)


def dot_nt(x, y):
    return lax.dot_general(x, y, (((1,), (1,)), ((), ())), preferred_element_type=F32)


def split(x):
    high = x.astype(BF)
    return high, (x - high.astype(F32)).astype(BF)


def dot3(x, y):
    return dot(x[0], y[0]) + (dot(x[0], y[1]) + dot(x[1], y[0]))


def dot3_nt(x, y):
    return dot_nt(x[0], y[0]) + (dot_nt(x[0], y[1]) + dot_nt(x[1], y[0]))


def encode(x, y):
    top = jnp.maximum(jnp.maximum(jnp.abs(x), jnp.abs(y)), 2.0**-31)
    exponent = jnp.minimum(jnp.floor(jnp.log2(top)), 31.0)
    scale = jnp.exp2(11.0 - exponent)

    def code(v):
        return jnp.clip(jnp.round(v * scale), -4095.0, 4095.0).astype(I32)

    high = jnp.left_shift(exponent.astype(I32) + 32, 26)
    return high | jnp.left_shift(code(y) & 0x1FFF, 13) | (code(x) & 0x1FFF)


def decode(word):
    scale = jnp.exp2(lax.shift_right_logical(word, 26).astype(F32) - 43.0)
    x = lax.shift_right_arithmetic(jnp.left_shift(word, 19), 19).astype(F32)
    y = lax.shift_right_arithmetic(jnp.left_shift(word, 6), 19).astype(F32)
    return x * scale, y * scale


@functools.lru_cache(None)
def send_order():
    rng = np.random.default_rng(0)
    every = [(dz, dy, dx, dc) for dz in range(8) for dy in range(4) for dx in range(4) for dc in range(2)]
    every = [d for d in every if any(d)]
    hops = {d: min(d[0], 8 - d[0]) + min(d[1], 4 - d[1]) + min(d[2], 4 - d[2]) + 0.5 * d[3] for d in every}
    return sorted(every, key=lambda d: (-hops[d], rng.random()))


def in_two(count, base=0):
    return [slice(base + k * count // 2, base + (k + 1) * count // 2) for k in range(2)]


def place():
    slab = lax.axis_index("slab")
    cell = lax.axis_index("cell")
    return slab, cell, lax.div(slab, 8), lax.rem(slab, 8) * 2 + cell


def device_at(plane, column):
    return (plane * 8 + lax.div(column, 2), lax.rem(column, 2))


def overlap(bins, low, high):
    return jnp.maximum(jnp.minimum(bins + 1.0, high) - jnp.maximum(bins, low), 0.0)


def kernel(
    row_h, col_h, width_h, height_h, region_h, offset_h,
    w_h, wt_h, tx_h, cyf_h, ty_h, bf_h, bi_h,
    field_x, field_y, force, sums,
    ci, co, pq, ym, yr, d2, zs, s1, r1, us, vs, gs, aw, pt, s2, r2, zx, fb, pf, pr, e1, e2, es,
    w, w2, wt, tx, cyf, cyi, ty, bf, bi, bi2,
    const_sem, in_sem, met, cell_s, cell_r, a1_s, a1_r, a2_s, a2_r, f_s, f_r, e_s, e_r,
):
    slab, cell, plane, column = place()
    me = plane * 16 + column
    mine, other = cell, 1 - cell
    has_prev = jnp.logical_and(cell == 0, slab > 0)
    has_next = slab < SLABS - 1
    barrier = pltpu.get_barrier_semaphore()

    own = [
        pltpu.make_async_copy(src, ci.at[mine, k], in_sem.at[k])
        for k, src in enumerate((row_h, col_h, width_h, height_h, region_h))
    ]
    own.append(pltpu.make_async_copy(offset_h, co.at[mine], in_sem.at[5]))
    for copy in own:
        copy.start()

    def signal_at(sem, device):
        pl.semaphore_signal(sem, inc=1, device_id=device, device_id_type=MESH)

    py, px = lax.div(plane, 4), lax.rem(plane, 4)
    ys = [lax.rem(py + k, 4) for k in range(4)]
    xs = [lax.rem(px + k, 4) for k in range(4)]
    x_line = [device_at(py * 4 + xs[k], column) for k in (2, 1, 3)]
    y_line = [device_at(ys[k] * 4 + px, column) for k in (2, 1, 3)]
    column_peers = [device_at(plane, lax.rem(column + i, 16)) for i in (8, 7, 9, 6, 10, 5, 11, 4, 12, 3, 13, 2, 14, 1, 15)]
    for device in column_peers + x_line + y_line:
        signal_at(barrier, device)

    @pl.when(has_prev)
    def _():
        signal_at(barrier, (slab - 1, 0))
        signal_at(barrier, (slab - 1, 1))

    z, core = lax.div(column, 4) * 2 + cell, lax.rem(lax.div(column, 2), 2)

    for copy in own:
        copy.wait()

    low_row = slab * 16 + cell * 8

    def cell_row_of(slot, k, which):
        return ci[slot, which, k : k + 1, :]

    def make_cells(slot, halves, masked):
        bins = lax.broadcasted_iota(I32, (128, 128), 0).astype(F32).astype(BF)
        line = lax.broadcasted_iota(I32, (16, 128), 0)
        rows = (jnp.bitwise_and(line, 3) + low_row).astype(F32)
        region_of = lax.shift_right_logical(line, 2)
        for k in range(4):
            at = slice(128 * k, 128 * k + 128)
            col = cell_row_of(slot, k, 1)
            high_bits = lax.shift_right_logical(col, 7)
            low_bits = (col - high_bits * 128).astype(F32).astype(BF)
            start = co[slot, 0:1, at]
            width = cell_row_of(slot, k, 2).astype(F32)
            first = (1.0 - start).astype(BF)
            last = ((start + width) - width).astype(BF)
            width = width.astype(BF)
            reach = bins - low_bits
            for far in range(2):
                if far:
                    reach = reach + BF(128.0)
                got = jnp.minimum(reach + first, (width - reach) + last)
                pq[slot, 128 * far : 128 * far + 128, at] = jnp.clip(got, BF(0.0), BF(1.0))
            start = co[slot, 1:2, at]
            end = start + cell_row_of(slot, k, 3).astype(F32)
            reach = rows - cell_row_of(slot, k, 0).astype(F32)
            here = cell_row_of(slot, k, 4) == region_of
            for half in range(halves):
                got = jnp.where(here, overlap(reach + 4.0 * half, start, end), 0.0)
                yr[slot, 16 * half : 16 * half + 16, at] = got.astype(BF).astype(F32)
                for a in range(16):
                    to = slice(256 * half + 16 * a, 256 * half + 16 * a + 16)
                    masked[to, at] = jnp.where(high_bits == a, got, 0.0).astype(BF)

    def send(src, dst, s_sem, r_sem, device):
        return pltpu.make_async_remote_copy(
            src_ref=src, dst_ref=dst, send_sem=s_sem, recv_sem=r_sem, device_id=device, device_id_type=MESH
        )

    pl.semaphore_wait(barrier, 21 + has_next.astype(I32))
    partner = (slab, other)
    give = [
        send(ci.at[mine], ci.at[mine], cell_s.at[0], cell_r.at[0, mine], partner),
        send(co.at[mine], co.at[mine], cell_s.at[1], cell_r.at[1, mine], partner),
    ]
    give_next = [
        send(ci.at[mine], ci.at[2 + mine], cell_s.at[2], cell_r.at[0, 2 + mine], (slab + 1, 0)),
        send(co.at[mine], co.at[2 + mine], cell_s.at[3], cell_r.at[1, 2 + mine], (slab + 1, 0)),
    ]
    for copy in give:
        copy.start()

    @pl.when(has_next)
    def _():
        for copy in give_next:
            copy.start()

    for device in x_line:
        signal_at(met.at[0], device)

    fetched = [
        pltpu.make_async_copy(src, dst, const_sem.at[k])
        for k, (src, dst) in enumerate(
            (
                (tx_h, tx), (wt_h, wt), (w_h, w), (w_h.at[:, 0, 0], w2.at[:, 0:128]), (w_h.at[:, 0, 0], w2.at[:, 128:256]),
                (cyf_h, cyf), (ty_h, ty), (bf_h, bf), (bi_h, bi),
                (bi_h.at[:, 0, 0], bi2.at[:, 0:128]), (bi_h.at[:, 0, 0], bi2.at[:, 128:256]),
            )
        )
    ]
    for copy in fetched:
        copy.start()

    def arrive(slot):
        send(ci.at[slot], ci.at[slot], cell_s.at[0], cell_r.at[0, slot], partner).wait_recv()
        send(co.at[slot], co.at[slot], cell_s.at[1], cell_r.at[1, slot], partner).wait_recv()

    make_cells(mine, 2, ym.at[0])
    for rows in in_two(512):
        d2[rows] = dot_nt(ym[0, rows], pq[mine])
    arrive(other)
    pl.semaphore_wait(met.at[0], 3)
    for device in y_line:
        signal_at(met.at[1], device)
    make_cells(other, 2, ym.at[0])
    for rows in in_two(512):
        d2[rows] += dot_nt(ym[0, rows], pq[other])

    zero8 = jnp.zeros((8, 128), F32)
    lane = lax.broadcasted_iota(I32, (1, 128), 1)
    first_group = lane < 32

    def x_forward(half, excess, area):
        here = []
        for a in range(16):
            at = 256 * half + 16 * a
            value = d2[at : at + 16, 0:128]
            if a:
                value = value + d2[at - 16 : at, 128:256]
            here.append(value)
            over = jnp.maximum(value - 1.0, 0.0)
            excess = excess + (over[0:8] + over[8:16])
            area = area + (value[0:8] + value[8:16])
        got = real_spectrum(here)
        for kap in range(16):
            at = slice(256 * half + 16 * kap, 256 * half + 16 * kap + 16)
            if kap == 0:
                pair = (got[0], got[16])
            else:
                (re, im), c, s = got[kap], tx[0, kap : kap + 1, :], tx[1, kap : kap + 1, :]
                pair = (re * c + im * s, im * c - re * s)
            for part, value in enumerate(pair):
                parts = split(value)
                for k in range(2):
                    zs[k, at, 128 * part : 128 * part + 128] = parts[k]

        def product(rows, kind):
            got = dot(zs[0, rows], wt[kind])
            return got[:, 0:128] + (got[:, 128:256] + dot(zs[1, rows], wt[kind, :, 0:128]))

        for rows in in_two(256, 256 * half):
            gs[rows] = product(rows, 0)
        first = slice(256 * half, 256 * half + 16)
        gs[first] = product(first, 1)
        return excess, area

    fetched[0].wait()
    fetched[1].wait()
    excess, area = x_forward(1, zero8, zero8)

    @pl.when(has_prev)
    def _():
        for k in range(2):
            arrive(2 + k)
        for k in range(2):
            make_cells(2 + k, 1, ym.at[1 + k])
        for rows in in_two(256):
            d2[rows] += dot_nt(ym[1, rows], pq[2]) + dot_nt(ym[2, rows], pq[3])

    excess, area = x_forward(0, excess, area)
    tiles = []
    for t in range(4):
        rows = [gs[256 * half + 16 * kap : 256 * half + 16 * kap + 16] for kap in range(4 * t, 4 * t + 4) for half in range(2)]
        tiles.append(jnp.concatenate(rows, axis=0).T)
    for t in range(2):
        s1[128 * t : 128 * t + 128, :] = encode(tiles[t], tiles[t + 2])

    pl.semaphore_wait(met.at[1], 3)
    planes = [[ys[dy] * 4 + xs[dx] for dx in range(4)] for dy in range(4)]
    z_there = [lax.rem(z + k, 8) for k in range(8)]
    z_parts = [(lax.div(k, 2), lax.rem(k, 2)) for k in z_there]

    def exchange(src, dst, s_sem, r_sem, part=slice(None)):
        for dz, dy, dx, dc in send_order()[part]:
            zh, zl = z_parts[dz]
            slab_to = planes[dy][dx] * 8 + (zh * 2 + (core if dc == 0 else 1 - core))
            send(src(slab_to, zl), dst, s_sem, r_sem, (slab_to, zl)).start()

    exchange(lambda slab_to, cell_to: s1.at[pl.ds(slab_to * 2 + cell_to, 1)], r1.at[cell, pl.ds(slab, 1)], a1_s, a1_r.at[cell])
    r1[cell, pl.ds(slab, 1), :] = s1[pl.ds(me, 1), :]

    tile, k2c = lax.div(me, 128), lax.rem(me, 128)
    lower = k2c < 64
    group = lax.div(lane, 32)
    order = lax.rem(lane, 8)

    def q_of(h):
        kap = 4 * (tile + 2 * h) + group
        return jnp.where(
            kap == 0,
            jnp.where(lower, 32 * k2c, 16 + 32 * (k2c - 64)),
            jnp.where(lower, kap + 32 * k2c, 32 - kap + 32 * (k2c - 64)),
        )

    qs = [q_of(h) for h in range(2)]

    def weigh(i, carry):
        at = pl.multiple_of(i * 16, 16)
        p1 = lax.broadcasted_iota(I32, (16, 128), 0) + at
        up = order < 4
        p = jnp.where(up, p1 + 512 * order, 512 - p1 + 512 * (order - 4))
        p = jnp.where(jnp.logical_and(p1 == 0, jnp.logical_not(up)), 256 + 512 * (order - 4), p)
        p_float = p.astype(F32)
        pt[pl.ds(at, 16), :] = p_float
        for h in range(2):
            q_float = qs[h].astype(F32)
            k2 = p_float * p_float + q_float * q_float
            scale = jnp.where(p == 0, 1.0 / M, 2.0 / M) * jnp.where(qs[h] == 0, 1.0 / M, 2.0 / M) * (1.0 / STEP)
            aw[pl.ds(256 * h + at, 16), :] = jnp.where(k2 == 0.0, 0.0, scale / jnp.where(k2 == 0.0, 1.0, k2))
        return carry

    lax.fori_loop(0, 16, weigh, 0)

    for copy in fetched[2:]:
        copy.wait()
    for k in range(2):
        for i in range(4):
            for j in range(2):
                rows, lanes = slice(128 * i, 128 * i + 128), slice(128 * j, 128 * j + 128)
                cyi[k, lanes, rows] = cyf[k, rows, lanes].T
    def half_arrived(k):
        for count, here in ((127, cell == k), (128, cell != k)):

            @pl.when(here)
            def _(count=count):
                send(s1.at[pl.ds(0, count)], r1.at[k, pl.ds(0, count)], a1_s, a1_r.at[k], partner).wait_recv()

    def half_of(k):
        high, low = zip(*(split(v) for v in decode(r1[k])))
        whole = (jnp.concatenate(high, axis=1), jnp.concatenate(low, axis=1))
        at = slice(128 * k, 128 * k + 128)
        return [(rows, dot3((cyf[0, rows, at], cyf[1, rows, at]), whole)) for rows in in_two(512)]

    half_arrived(1)
    for rows, got in half_of(1):
        us[rows] = got
    half_arrived(0)
    send(s1.at[pl.ds(0, 255)], s1.at[pl.ds(0, 255)], a1_s, a1_r.at[0], partner).wait_send()

    for rows, got in half_of(0):
        us[rows] += got

    def y_chunk(i, carry):
        at = i * 16
        c, s = ty[0, pl.ds(at, 16), :], ty[1, pl.ds(at, 16), :]
        for h in range(2):
            lanes = slice(128 * h, 128 * h + 128)
            re, im = us[pl.ds(at, 16), lanes], us[pl.ds(256 + at, 16), lanes]
            for half, value in enumerate((re * c + im * s, im * c - re * s)):
                parts = split(value)
                for k in range(2):
                    vs[k, pl.ds(256 * h + at, 16), 128 * half : 128 * half + 128] = parts[k]
        return carry

    for i in range(16):
        y_chunk(i, 0)

    def y_out(rows, table):
        got = dot(vs[0, rows], table)
        return got[:, 0:128] + (got[:, 128:256] + dot(vs[1, rows], table[:, 0:128]))

    for rows in in_two(512):
        gs[rows] = y_out(rows, bf[0])
    top_row = lax.broadcasted_iota(I32, (16, 1), 0) == 0
    for h in range(2):
        at = slice(256 * h, 256 * h + 16)
        gs[at, :] = jnp.where(top_row, y_out(at, bf[1]), gs[at, :])

    q_floats = [q.astype(F32) for q in qs]

    def scale_chunk(i, energy):
        at = i * 16
        p_float = pt[pl.ds(at, 16), :]
        for h in range(2):
            value = gs[pl.ds(256 * h + at, 16), :]
            weighted = value * aw[pl.ds(256 * h + at, 16), :]
            work = weighted * value
            energy = energy + (work[0:8] + work[8:16])
            for f, part in enumerate((weighted * q_floats[h], weighted * p_float)):
                parts = split(part)
                for k in range(2):
                    vs[f, pl.ds(256 * h + at, 16), 128 * k : 128 * k + 128] = parts[k]
        return energy

    energy = zero8
    for i in range(16):
        energy = scale_chunk(i, energy)

    def top_rows(f, h):
        at = slice(256 * h, 256 * h + 16)
        return dot3((vs[f, at, 0:128], vs[f, at, 128:256]), (bi[f, 1, 0], bi[f, 1, 1]))

    def turned(values, c, s):
        re, im = values[:, 0:128], values[:, 128:256]
        return [split(value) for value in (re * c - im * s, re * s + im * c)]

    def keep_turned(values, h, at):
        for half in range(2):
            for k in range(2):
                zs[k, pl.ds(256 * half + at, values[half][k].shape[0]), 128 * h : 128 * h + 128] = values[half][k]

    def copies_of(f):
        return (
            lambda slab_to, cell_to: s2.at[f, cell_to, pl.ds(slab_to, 1)], r2.at[f, pl.ds(me, 1)], a2_s.at[f], a2_r.at[f]
        )

    for rows in in_two(512):
        us[rows] = dot(vs[0, rows], bi2[0]) + dot(vs[0, rows, 0:128], bi[0, 0, 1])
    for h in range(2):
        at = slice(256 * h, 256 * h + 16)
        us[at, :] = jnp.where(top_row, top_rows(0, h), us[at, :])
    for i in range(16):
        for h in range(2):
            at = slice(16 * i, 16 * i + 16)
            keep_turned(turned(us[256 * h + 16 * i : 256 * h + 16 * i + 16, :], ty[0, at, :], ty[1, at, :]), h, 16 * i)
    def back_in_y(f):
        for k, rows in enumerate(in_two(256)):
            got = dot3((cyi[0, rows], cyi[1, rows]), (zs[0], zs[1]))
            s2[f, k] = encode(got[:, 0:128], got[:, 128:256])

    back_in_y(0)
    r2[0, pl.ds(me, 1), :] = s2[0, cell, pl.ds(slab, 1), :]

    for i in range(2):
        at = 128 * i
        rows = [vs[1, 256 * h + at : 256 * h + at + 128, :] for h in range(2)]
        c, s = ty[0, at : at + 128, :], ty[1, at : at + 128, :]
        top = [top_rows(1, h) for h in range(2)] if i == 0 else None
        got = [dot(r, bi2[1]) + dot(r[:, 0:128], bi[1, 0, 1]) for r in rows]
        values = []
        for h in range(2):
            value = got[h]
            if i == 0:
                value = jnp.concatenate([jnp.where(top_row, top[h], value[0:16]), value[16:]], axis=0)
            values.append(turned(value, c, s))
        exchange(*copies_of(0), part=slice(FAR // 2 * i, FAR // 2 * i + FAR // 2))
        for h in range(2):
            keep_turned(values[h], h, at)

    back_in_y(1)
    exchange(*copies_of(1), part=slice(0, NEXT))
    exchange(*copies_of(0), part=slice(FAR, None))
    exchange(*copies_of(1), part=slice(NEXT, None))
    r2[1, pl.ds(me, 1), :] = s2[1, cell, pl.ds(slab, 1), :]

    def total(x):
        return jnp.sum(jnp.sum(x, axis=1, keepdims=True), axis=0, keepdims=True)

    row = jnp.where(
        lane == 0, total(excess), jnp.where(lane == 1, total(area), total(energy) * (1.0 / (STEP * M * M)))
    )
    es[0] = row
    e1[plane] = row
    for i in range(1, 16):
        send(es.at[0], e1.at[plane], e_s.at[0], e_r.at[0], device_at(lax.rem(plane + i, 16), column)).start()
    def push(slot, f, halves):
        got = dot(fb[f, 0 : 256 * halves], pq[slot])
        for k in range(4):
            at = slice(128 * k, 128 * k + 128)
            high_bits = lax.shift_right_logical(cell_row_of(slot, k, 1), 7)
            force = jnp.zeros((1, 128), F32)
            for half in range(halves):
                kept = got[256 * half : 256 * half + 16, at]
                for a in range(1, 16):
                    kept = jnp.where(high_bits == a, got[256 * half + 16 * a : 256 * half + 16 * a + 16, at], kept)
                force = force + jnp.sum(kept * yr[slot, 16 * half : 16 * half + 16, at], axis=0, keepdims=True)
            pf[slot, f : f + 1, at] = force

    def x_gather(f):
        for t in range(2):
            for h, value in enumerate(decode(r2[f, 128 * t : 128 * t + 128, :])):
                parts = split(value.T)
                for k in range(2):
                    for j in range(4):
                        for half in range(2):
                            to = 256 * half + 16 * (4 * (t + 2 * h) + j)
                            zx[to : to + 16, 128 * k : 128 * k + 128] = parts[k][32 * j + 16 * half : 32 * j + 16 * half + 16]

    def x_product(f, halves):
        base, count = 256 * halves[0], 256 * len(halves)
        for rows in in_two(count, base):
            us[rows, :] = dot(zx[rows], w2[f]) + dot(zx[rows, 0:128], w[f, 0, 1])
        for half in halves:
            first = slice(256 * half, 256 * half + 16)
            us[first, :] = dot3((zx[first, 0:128], zx[first, 128:256]), (w[f, 1, 0], w[f, 1, 1]))

    def x_inverse(f, out, half):
        base = 256 * half
        got = {}
        for kap in range(16):
            rows = slice(base + 16 * kap, base + 16 * kap + 16)
            re, im = us[rows, 0:128], us[rows, 128:256]
            if kap == 0:
                got[0], got[16] = re, im
            else:
                c, s = tx[0, kap : kap + 1, :], tx[1, kap : kap + 1, :]
                got[kap] = (re * c - im * s, re * s + im * c)
        for a, value in enumerate(real_back(got, 16)):
            lanes = slice(128 * a, 128 * a + 128)
            for g in range(REGIONS):
                out[g, 4 * half : 4 * half + 4, lanes] = value[4 * g : 4 * g + 4]
            near = value.astype(BF)
            fb[f, base + 16 * a : base + 16 * a + 16, 0:128] = near
            if a:
                fb[f, base + 16 * a - 16 : base + 16 * a, 128:256] = near
        fb[f, base + 240 : base + 256, 128:256] = jnp.zeros((16, 128), BF)

    def give_back(slot, device, sem, into):
        return send(pf.at[slot], pr.at[into], f_s.at[sem], f_r.at[into], device)

    def arrived(f):
        whole = send(r2.at[f, pl.ds(0, 255)], r2.at[f, pl.ds(0, 255)], a2_s.at[f], a2_r.at[f], partner)
        whole.wait_recv()
        whole.wait_send()

    arrived(0)
    x_gather(0)
    x_product(0, (0, 1))
    for half in range(2):
        x_inverse(0, field_x, half)

    @pl.when(has_prev)
    def _():
        for k in range(2):
            push(2 + k, 0, 1)

    push(other, 0, 2)
    push(mine, 0, 2)
    sums_wait = send(e1.at[pl.ds(0, 15)], e1.at[pl.ds(0, 15)], e_s.at[0], e_r.at[0], partner)
    sums_wait.wait_recv()
    sums_wait.wait_send()
    row = jnp.sum(e1[...], axis=0)
    es[1] = row
    e2[column] = row
    for i in range(1, 16):
        send(es.at[1], e2.at[column], e_s.at[1], e_r.at[1], device_at(plane, lax.rem(column + i, 16))).start()
    arrived(1)
    x_gather(1)
    x_product(1, (0,))
    x_inverse(1, field_y, 0)

    @pl.when(has_prev)
    def _():
        for k in range(2):
            push(2 + k, 1, 1)
        for k in range(2):
            give_back(2 + k, (slab - 1, k), 1 + k, 1).start()

    x_product(1, (1,))
    x_inverse(1, field_y, 1)
    push(other, 1, 2)
    give_back(other, partner, 0, 0).start()
    push(mine, 1, 2)

    @pl.when(jnp.logical_not(has_next))
    def _():
        pr[1] = jnp.zeros((2, CELLS_DEV), F32)

    give_back(other, partner, 0, 0).wait_recv()

    @pl.when(has_next)
    def _():
        give_back(other, partner, 0, 1).wait_recv()

    force[...] = pf[mine] + pr[0] + pr[1]

    send(e2.at[pl.ds(0, 15)], e2.at[pl.ds(0, 15)], e_s.at[1], e_r.at[1], partner).wait()
    sums[...] = jnp.sum(e2[...], axis=0)

    give_back(other, partner, 0, 0).wait_send()
    for copy in give:
        copy.wait_send()

    @pl.when(has_prev)
    def _():
        for k in range(2):
            give_back(2 + k, (slab - 1, k), 1 + k, 1).wait_send()

    @pl.when(has_next)
    def _():
        for copy in give_next:
            copy.wait_send()


def finish(field_x, field_y, force, sums, out_x, out_y, out_force, energy, overflow, small, sem):
    pairs = ((field_x, out_x), (field_y, out_y), (force, out_force), (small.at[0], energy), (small.at[1], overflow))
    copies = [pltpu.make_async_copy(src, dst, sem.at[k]) for k, (src, dst) in enumerate(pairs)]
    for copy in copies[:3]:
        copy.start()
    row = sums[...]
    small[0] = row[:, 2:3]
    small[1] = row[:, 0:1] / row[:, 1:2]
    for copy in copies[3:]:
        copy.start()
    for copy in copies:
        copy.wait()


def body(cell_row, cell_col, cell_width, cell_height, cell_region, cell_offset):
    consts = [jnp.asarray(t) for t in tables()]
    whole = [v.reshape(4, 128) for v in (cell_row, cell_col, cell_width, cell_height, cell_region)]
    vmem = pl.BlockSpec(memory_space=pltpu.VMEM)
    hbm = pl.BlockSpec(memory_space=pltpu.HBM)
    V = pltpu.VMEM
    D = pltpu.SemaphoreType.DMA
    scratch = [
        V((4, 5, 4, 128), I32),
        V((4, 2, CELLS_DEV), F32),
        V((4, 256, 512), BF),
        V((3, 512, 512), BF),
        V((4, 32, CELLS_DEV), F32),
        V((512, 256), F32),
        V((2, 512, 256), BF),
        V((256, 128), I32),
        V((2, 128, 128), I32),
        V((512, 256), F32),
        V((2, 512, 256), BF),
        V((512, 128), F32),
        V((512, 128), F32),
        V((256, 128), F32),
        V((2, 2, 128, 128), I32),
        V((2, 256, 128), I32),
        V((512, 256), BF),
        V((2, 512, 256), BF),
        V((4, 2, CELLS_DEV), F32),
        V((2, 2, CELLS_DEV), F32),
        V((16, 1, 128), F32),
        V((16, 1, 128), F32),
        V((2, 1, 128), F32),
        V((2, 2, 2, 128, 256), BF),
        V((2, 256, 256), BF),
        V((2, 256, 256), BF),
        V((2, 16, 128), F32),
        V((2, 512, 256), BF),
        V((2, 256, 512), BF),
        V((2, 256, 128), F32),
        V((2, 256, 256), BF),
        V((2, 2, 2, 128, 256), BF),
        V((2, 256, 256), BF),
        D((11,)), D((6,)),
        pltpu.SemaphoreType.REGULAR((2,)),
        D((4,)), D((2, 4)),
        D, D((2,)), D((2,)), D((2,)),
        D((3,)), D((2,)),
        D((2,)), D((2,)),
    ]
    field = (REGIONS, 8, M)
    results = pl.pallas_call(
        kernel,
        out_shape=(V(field, F32), V(field, F32), V((2, CELLS_DEV), F32), V((1, 128), F32)),
        in_specs=[hbm] * (6 + len(consts)),
        out_specs=(vmem,) * 4,
        scratch_shapes=scratch,
        compiler_params=pltpu.CompilerParams(
            collective_id=0, has_side_effects=True, vmem_limit_bytes=66300000
        ),
        name="placement",
    )(*whole, cell_offset, *consts)
    S = jax.ShapeDtypeStruct
    field_x, field_y, force, energy, overflow = pl.pallas_call(
        finish,
        out_shape=(S(field, F32), S(field, F32), S((2, CELLS_DEV), F32), S((1, 1), F32), S((1, 1), F32)),
        in_specs=[vmem] * 4,
        out_specs=(hbm,) * 5,
        scratch_shapes=[V((2, 1, 1), F32), D((5,))],
        compiler_params=pltpu.CompilerParams(vmem_limit_bytes=4 * 1024 * 1024),
        name="finish",
    )(*results)
    return (field_x, field_y, force, energy.reshape(()), overflow.reshape(()))


def solution(mesh):
    both = ("slab", "cell")
    placed = (P(both),) * 5 + (P(None, both),)
    return jax.shard_map(
        body,
        mesh=mesh,
        in_specs=placed,
        out_specs=(P(None, both, None), P(None, both, None), P(None, both), P(), P()),
        check_vma=False,
    )
```

```python
import functools
import math

import jax
import jax.numpy as jnp
import numpy as np
from jax import lax
from jax.experimental import pallas as pl
from jax.experimental.pallas import tpu as pltpu
from jax.sharding import PartitionSpec as P

M = 2048
REGIONS = 4
SLABS = 128
CELLS_DEV = 512
BF = jnp.bfloat16
F32 = jnp.float32
I32 = jnp.int32
MESH = pl.DeviceIdType.MESH
STEP = math.pi / M
FAR = 98
NEXT = 14
NEAR = 1
LEAD = 4


def c_add(x,y): return (x[0]+y[0], x[1]+y[1])
def c_sub(x,y): return (x[0]-y[0], x[1]-y[1])
def c_turn(x,angle):
    c,s=math.cos(angle),math.sin(angle)
    if abs(s)<1e-12: return x if c>0 else (-x[0],-x[1])
    if abs(c)<1e-12: return (-x[1],x[0]) if s>0 else (x[1],-x[0])
    if abs(abs(c)-abs(s))<1e-12:
        h=abs(c); a,b=x[0],x[1]
        sc,ss=(1 if c>0 else -1),(1 if s>0 else -1)
        def lin(p,a,q,b):
            if p>0: return (a+b)*h if q>0 else (a-b)*h
            return (b-a)*h if q>0 else (a+b)*(-h)
        return (lin(sc,a,-ss,b), lin(ss,a,sc,b))
    return (x[0]*c-x[1]*s, x[0]*s+x[1]*c)
def c_fft(xs,sign):
    n=len(xs)
    if n==1: return xs
    even,odd=c_fft(xs[0::2],sign),c_fft(xs[1::2],sign)
    out=[None]*n
    for k in range(n//2):
        t=c_turn(odd[k],sign*2*math.pi*k/n)
        out[k],out[k+n//2]=c_add(even[k],t),c_sub(even[k],t)
    return out
def real_spectrum(d):
    n=len(d)
    if n==2:
        return {0:d[0]+d[1],1:(d[0],-d[1]),2:d[0]-d[1]}
    half=n//2
    out={}
    z=[c_turn((d[a],-d[a+half]),-math.pi*a/n) for a in range(half)]
    f=c_fft(z,-1)
    for m in range(half):
        k=1+4*m
        if k<n: out[k]=f[m]
        else: out[2*n-k]=(f[m][0],-f[m][1])
    s=[d[a]+d[a+half] for a in range(half)]
    e=[d[a]-d[a+half] for a in range(half)]
    q=half//2
    z=[c_turn((e[a],-e[a+q]),-2*math.pi*a/n) for a in range(q)]
    f=c_fft(z,-1)
    for l in range(q):
        m=1+4*l
        if m<=half: out[2*m]=f[l]
        else: out[2*(n-m)]=(f[l][0],-f[l][1])
    sub=real_full(s)
    for l,v in sub.items(): out[4*l]=v
    return out
def real_full(s):
    n=len(s)
    if n==2: return {0:s[0]+s[1],1:s[0]-s[1]}
    half=n//2
    p=[s[a]+s[a+half] for a in range(half)]
    e=[s[a]-s[a+half] for a in range(half)]
    out={}
    for l,v in real_full(p).items(): out[2*l]=v
    q=half//2
    if q==0: return out
    z=[c_turn((e[a],-e[a+q]),-2*math.pi*a/n) for a in range(q)] if q else []
    f=c_fft(z,-1)
    for k in range(q):
        l=1+4*k
        if l<=half: out[l]=f[k]
        else: out[n-l]=(f[k][0],-f[k][1])
    return out
def real_full_back(v,n):
    if n==2: return [v[0]+v[1],v[0]-v[1]]
    half=n//2; q=half//2
    p=real_full_back({l//2:x for l,x in v.items() if l%2==0},half)
    if n==4:
        g=[v[1]]
    else:
        g=[v[1+4*k] if 1+4*k<=half else (v[n-1-4*k][0],-v[n-1-4*k][1]) for k in range(q)]
    f=c_fft(g,1)
    odd=[None]*half
    for a in range(q):
        t=c_turn(f[a],2*math.pi*a/n)
        odd[a],odd[a+q]=t[0],-t[1]
    out=[None]*n
    for a in range(half):
        out[a],out[a+half]=p[a]+odd[a],p[a]-odd[a]
    return out
def real_back(y,n):
    half=n//2
    even=real_full_back({k//2:v for k,v in y.items() if k%2==0},n)
    g=[y[1+4*m] if 1+4*m<n else (y[2*n-1-4*m][0],-y[2*n-1-4*m][1]) for m in range(half)]
    f=c_fft(g,1)
    out=[None]*n
    for a in range(half):
        t=c_turn(f[a],math.pi*a/n)
        out[a],out[a+half]=even[a]+t[0],even[a+half]-t[1]
    return out


def split_np(table):
    high = table.astype(np.float32).astype(BF)
    low = (table - high.astype(np.float64)).astype(np.float32).astype(BF)
    return np.stack([high, low])


@functools.lru_cache(None)
def tables():
    pi = np.pi
    k2 = np.arange(64)[:, None]
    b = np.arange(128)[None, :]
    c1, s1 = np.cos(pi * k2 * (2 * b + 1) / 128), np.sin(pi * k2 * (2 * b + 1) / 128)
    c2, s2 = np.cos(pi * (k2 + 1) * (2 * b + 1) / 128), np.sin(pi * (k2 + 1) * (2 * b + 1) / 128)
    cm, sm = np.cos(pi * (2 * k2 + 1) * (2 * b + 1) / 256), np.sin(pi * (2 * k2 + 1) * (2 * b + 1) / 256)
    zero = np.zeros_like(c1)
    wc = np.block([[c1, s1], [c2, -s2]])
    wc0 = np.block([[c1, zero], [zero, cm]])
    ws = np.block([[s1, -c1], [s2, c2]])
    ws0 = np.block([[s1, zero], [zero, sm]])
    w = np.stack([split_np(m) for m in (ws, ws0, wc, wc0)]).reshape(2, 2, 2, 128, 256)
    wt = np.stack([np.concatenate(list(split_np(m.T)), axis=1) for m in (wc, wc0)])
    kap = np.arange(16)[:, None]
    ang = pi * kap * (2 * b + 1) / 4096
    tx = np.stack([np.cos(ang), np.sin(ang)]).astype(np.float32)
    p1 = np.arange(256)[:, None]
    d = np.arange(256)[None, :]
    cre, cim = np.cos(2 * pi * p1 * d / 512), -np.sin(2 * pi * p1 * d / 512)
    cim[0] = (-1.0) ** np.arange(256)
    cy = np.concatenate([cre, cim], 0)[:, np.arange(256).reshape(128, 2).T.reshape(-1)]
    ours = np.arange(128).reshape(4, 4, 2, 4).transpose(0, 2, 1, 3).reshape(-1)
    cy_fwd = split_np(cy)
    r = np.arange(8)
    angy = pi * p1 * (2 * r[None, :] + 1) / 4096
    ty = np.stack([np.tile(np.cos(angy), (1, 16)), np.tile(np.sin(angy), (1, 16))])[:, :, ours].astype(np.float32)
    p2 = np.arange(4)[None, :]
    rr = r[:, None]
    e0, e1 = pi * p2 * (2 * rr + 1) / 8, pi * (p2 + 1) * (2 * rr + 1) / 8
    em = pi * (2 * rr + 1) * (1 + 2 * p2) / 16
    z8 = np.zeros((8, 4))
    bc = (np.block([np.cos(e0), np.cos(e1)]), np.block([np.sin(e0), -np.sin(e1)]))
    bc0 = (np.block([np.cos(e0), z8]), np.block([z8, np.cos(em)]))
    bs = (np.block([np.sin(e0), np.sin(e1)]), np.block([-np.cos(e0), np.cos(e1)]))
    bs0 = (np.block([np.sin(e0), z8]), np.block([z8, np.sin(em)]))

    def wide(pair):
        return np.concatenate([np.kron(np.eye(16), part)[ours] for part in pair], 0)

    b_fwd = np.stack([np.concatenate(list(split_np(wide(m))), axis=1) for m in (bc, bc0)])
    b_inv = np.stack([split_np(wide(m).T) for m in (bc, bc0, bs, bs0)]).reshape(2, 2, 2, 128, 256)
    return w, wt, tx, cy_fwd, ty, b_fwd, b_inv


def dot(x, y):
    return lax.dot_general(x, y, (((1,), (0,)), ((), ())), preferred_element_type=F32)


def dot_nt(x, y):
    return lax.dot_general(x, y, (((1,), (1,)), ((), ())), preferred_element_type=F32)


def split(x):
    high = x.astype(BF)
    return high, (x - high.astype(F32)).astype(BF)


def dot3(x, y):
    return dot(x[0], y[0]) + (dot(x[0], y[1]) + dot(x[1], y[0]))


def dot3_nt(x, y):
    return dot_nt(x[0], y[0]) + (dot_nt(x[0], y[1]) + dot_nt(x[1], y[0]))


def encode(x, y):
    top = jnp.maximum(jnp.maximum(jnp.abs(x), jnp.abs(y)), 2.0**-31)
    exponent = jnp.minimum(jnp.floor(jnp.log2(top)), 31.0)
    scale = jnp.exp2(11.0 - exponent)

    def code(v):
        return jnp.clip(jnp.round(v * scale), -4095.0, 4095.0).astype(I32)

    high = jnp.left_shift(exponent.astype(I32) + 32, 26)
    return high | jnp.left_shift(code(y) & 0x1FFF, 13) | (code(x) & 0x1FFF)


def decode(word):
    scale = jnp.exp2(lax.shift_right_logical(word, 26).astype(F32) - 43.0)
    x = lax.shift_right_arithmetic(jnp.left_shift(word, 19), 19).astype(F32)
    y = lax.shift_right_arithmetic(jnp.left_shift(word, 6), 19).astype(F32)
    return x * scale, y * scale


@functools.lru_cache(None)
def send_order():
    rng = np.random.default_rng(0)
    every = [(dz, dy, dx, dc) for dz in range(8) for dy in range(4) for dx in range(4) for dc in range(2)]
    every = [d for d in every if any(d)]
    hops = {d: min(d[0], 8 - d[0]) + min(d[1], 4 - d[1]) + min(d[2], 4 - d[2]) + 0.5 * d[3] for d in every}
    return sorted(every, key=lambda d: (-hops[d], rng.random()))


def in_two(count, base=0):
    return [slice(base + k * count // 2, base + (k + 1) * count // 2) for k in range(2)]


@functools.lru_cache(None)
def first_devices():
    def reach(value, count):
        return min(value, count - value)

    found = []
    for slab in range(SLABS):
        for cell in range(2):
            y, x, z = slab // 32, slab // 8 % 4, slab // 2 % 4 * 2 + cell
            plane = reach(y, 4) + reach(x, 4)
            if reach(y, 4) + min(x, 1) + (0 if z < 3 else 3 if z == 3 else reach(z, 8)) <= NEAR:
                own = slab in (1, 2) and (slab, cell) != (2, 1)
                found.append((0 if own and plane == 0 else 1 + plane + reach(z, 8) - 0.5 * (slab % 2), slab, cell))
    return [(slab, cell) for _, slab, cell in sorted(found)]


def place():
    slab = lax.axis_index("slab")
    cell = lax.axis_index("cell")
    return slab, cell, lax.div(slab, 8), lax.rem(slab, 8) * 2 + cell


def device_at(plane, column):
    return (plane * 8 + lax.div(column, 2), lax.rem(column, 2))


def overlap(bins, low, high):
    return jnp.maximum(jnp.minimum(bins + 1.0, high) - jnp.maximum(bins, low), 0.0)


def kernel(
    row_h, col_h, width_h, height_h, region_h, offset_h,
    w_h, wt_h, tx_h, cyf_h, ty_h, bf_h, bi_h,
    field_x, field_y, force, sums,
    ci, co, pq, ym, yr, d2, zs, s1, r1, us, vs, gs, aw, pt, s2, r2, zx, fb, pf, pr, e1, e2, es,
    w, w2, wt, tx, cyf, cyi, ty, bf, bi, bi2,
    const_sem, in_sem, met, cell_s, cell_r, a1_s, a1_r, a2_s, a2_r, f_s, f_r, e_s, e_r,
):
    slab, cell, plane, column = place()
    me = plane * 16 + column
    mine, other = cell, 1 - cell
    has_prev = jnp.logical_and(cell == 0, slab > 0)
    has_next = slab < SLABS - 1
    barrier = pltpu.get_barrier_semaphore()

    own = [
        pltpu.make_async_copy(src, ci.at[mine, k], in_sem.at[k])
        for k, src in enumerate((row_h, col_h, width_h, height_h, region_h))
    ]
    own.append(pltpu.make_async_copy(offset_h, co.at[mine], in_sem.at[5]))
    for copy in own:
        copy.start()

    def signal_at(sem, device):
        pl.semaphore_signal(sem, inc=1, device_id=device, device_id_type=MESH)

    py, px = lax.div(plane, 4), lax.rem(plane, 4)
    ys = [lax.rem(py + k, 4) for k in range(4)]
    xs = [lax.rem(px + k, 4) for k in range(4)]
    x_line = [device_at(py * 4 + xs[k], column) for k in (2, 1, 3)]
    y_line = [device_at(ys[k] * 4 + px, column) for k in (2, 1, 3)]
    column_peers = [device_at(plane, lax.rem(column + i, 16)) for i in (8, 7, 9, 6, 10, 5, 11, 4, 12, 3, 13, 2, 14, 1, 15)]
    for device in column_peers + x_line + y_line:
        signal_at(barrier, device)

    @pl.when(has_prev)
    def _():
        signal_at(barrier, (slab - 1, 0))
        signal_at(barrier, (slab - 1, 1))

    z, core = lax.div(column, 4) * 2 + cell, lax.rem(lax.div(column, 2), 2)

    for copy in own:
        copy.wait()

    low_row = slab * 16 + cell * 8

    def cell_row_of(slot, k, which):
        return ci[slot, which, k : k + 1, :]

    def make_cells(slot, halves, masked):
        bins = lax.broadcasted_iota(I32, (128, 128), 0).astype(F32).astype(BF)
        line = lax.broadcasted_iota(I32, (16, 128), 0)
        rows = (jnp.bitwise_and(line, 3) + low_row).astype(F32)
        region_of = lax.shift_right_logical(line, 2)
        for k in range(4):
            at = slice(128 * k, 128 * k + 128)
            col = cell_row_of(slot, k, 1)
            high_bits = lax.shift_right_logical(col, 7)
            low_bits = (col - high_bits * 128).astype(F32).astype(BF)
            start = co[slot, 0:1, at]
            width = cell_row_of(slot, k, 2).astype(F32)
            first = (1.0 - start).astype(BF)
            last = ((start + width) - width).astype(BF)
            width = width.astype(BF)
            reach = bins - low_bits
            for far in range(2):
                if far:
                    reach = reach + BF(128.0)
                got = jnp.minimum(reach + first, (width - reach) + last)
                pq[slot, 128 * far : 128 * far + 128, at] = jnp.clip(got, BF(0.0), BF(1.0))
            start = co[slot, 1:2, at]
            end = start + cell_row_of(slot, k, 3).astype(F32)
            reach = rows - cell_row_of(slot, k, 0).astype(F32)
            here = cell_row_of(slot, k, 4) == region_of
            for half in range(halves):
                got = jnp.where(here, overlap(reach + 4.0 * half, start, end), 0.0)
                yr[slot, 16 * half : 16 * half + 16, at] = got.astype(BF).astype(F32)
                for a in range(16):
                    to = slice(256 * half + 16 * a, 256 * half + 16 * a + 16)
                    masked[to, at] = jnp.where(high_bits == a, got, 0.0).astype(BF)

    def send(src, dst, s_sem, r_sem, device):
        return pltpu.make_async_remote_copy(
            src_ref=src, dst_ref=dst, send_sem=s_sem, recv_sem=r_sem, device_id=device, device_id_type=MESH
        )

    pl.semaphore_wait(barrier, 21 + has_next.astype(I32))
    partner = (slab, other)
    give = [
        send(ci.at[mine], ci.at[mine], cell_s.at[0], cell_r.at[0, mine], partner),
        send(co.at[mine], co.at[mine], cell_s.at[1], cell_r.at[1, mine], partner),
    ]
    give_next = [
        send(ci.at[mine], ci.at[2 + mine], cell_s.at[2], cell_r.at[0, 2 + mine], (slab + 1, 0)),
        send(co.at[mine], co.at[2 + mine], cell_s.at[3], cell_r.at[1, 2 + mine], (slab + 1, 0)),
    ]
    for copy in give:
        copy.start()

    @pl.when(has_next)
    def _():
        for copy in give_next:
            copy.start()

    for device in x_line:
        signal_at(met.at[0], device)

    fetched = [
        pltpu.make_async_copy(src, dst, const_sem.at[k])
        for k, (src, dst) in enumerate(
            (
                (tx_h, tx), (wt_h, wt), (w_h, w), (w_h.at[:, 0, 0], w2.at[:, 0:128]), (w_h.at[:, 0, 0], w2.at[:, 128:256]),
                (cyf_h, cyf), (ty_h, ty), (bf_h, bf), (bi_h, bi),
                (bi_h.at[:, 0, 0], bi2.at[:, 0:128]), (bi_h.at[:, 0, 0], bi2.at[:, 128:256]),
            )
        )
    ]
    for copy in fetched:
        copy.start()

    def arrive(slot):
        send(ci.at[slot], ci.at[slot], cell_s.at[0], cell_r.at[0, slot], partner).wait_recv()
        send(co.at[slot], co.at[slot], cell_s.at[1], cell_r.at[1, slot], partner).wait_recv()

    make_cells(mine, 2, ym.at[0])
    for rows in in_two(512):
        d2[rows] = dot_nt(ym[0, rows], pq[mine])
    arrive(other)
    pl.semaphore_wait(met.at[0], 3)
    for device in y_line:
        signal_at(met.at[1], device)
    make_cells(other, 2, ym.at[0])
    for rows in in_two(512):
        d2[rows] += dot_nt(ym[0, rows], pq[other])

    zero8 = jnp.zeros((8, 128), F32)
    lane = lax.broadcasted_iota(I32, (1, 128), 1)
    first_group = lane < 32

    def x_forward(half, excess, area):
        here = []
        for a in range(16):
            at = 256 * half + 16 * a
            value = d2[at : at + 16, 0:128]
            if a:
                value = value + d2[at - 16 : at, 128:256]
            here.append(value)
            over = jnp.maximum(value - 1.0, 0.0)
            excess = excess + (over[0:8] + over[8:16])
            area = area + (value[0:8] + value[8:16])
        got = real_spectrum(here)
        for kap in range(16):
            at = slice(256 * half + 16 * kap, 256 * half + 16 * kap + 16)
            if kap == 0:
                pair = (got[0], got[16])
            else:
                (re, im), c, s = got[kap], tx[0, kap : kap + 1, :], tx[1, kap : kap + 1, :]
                pair = (re * c + im * s, im * c - re * s)
            for part, value in enumerate(pair):
                parts = split(value)
                for k in range(2):
                    zs[k, at, 128 * part : 128 * part + 128] = parts[k]

        def product(rows, kind):
            got = dot(zs[0, rows], wt[kind])
            return got[:, 0:128] + (got[:, 128:256] + dot(zs[1, rows], wt[kind, :, 0:128]))

        for rows in in_two(256, 256 * half):
            gs[rows] = product(rows, 0)
        first = slice(256 * half, 256 * half + 16)
        gs[first] = product(first, 1)
        return excess, area

    fetched[0].wait()
    fetched[1].wait()
    excess, area = x_forward(1, zero8, zero8)

    @pl.when(has_prev)
    def _():
        for k in range(2):
            arrive(2 + k)
        for k in range(2):
            make_cells(2 + k, 1, ym.at[1 + k])
        for rows in in_two(256):
            d2[rows] += dot_nt(ym[1, rows], pq[2]) + dot_nt(ym[2, rows], pq[3])

    excess, area = x_forward(0, excess, area)
    tiles = []
    for t in range(4):
        rows = [gs[256 * half + 16 * kap : 256 * half + 16 * kap + 16] for kap in range(4 * t, 4 * t + 4) for half in range(2)]
        tiles.append(jnp.concatenate(rows, axis=0).T)
    for t in range(2):
        s1[128 * t : 128 * t + 128, :] = encode(tiles[t], tiles[t + 2])

    pl.semaphore_wait(met.at[1], 3)
    planes = [[ys[dy] * 4 + xs[dx] for dx in range(4)] for dy in range(4)]
    z_there = [lax.rem(z + k, 8) for k in range(8)]
    z_parts = [(lax.div(k, 2), lax.rem(k, 2)) for k in z_there]

    def exchange(src, dst, s_sem, r_sem, part=slice(None)):
        for dz, dy, dx, dc in send_order()[part]:
            zh, zl = z_parts[dz]
            slab_to = planes[dy][dx] * 8 + (zh * 2 + (core if dc == 0 else 1 - core))
            send(src(slab_to, zl), dst, s_sem, r_sem, (slab_to, zl)).start()

    def reach(value, count):
        return jnp.minimum(value, count - value)

    y_reach, x_reach = [reach(v, 4) for v in ys], [jnp.minimum(v, 1) for v in xs]
    z_reach = [jnp.where(v < 3, 0, jnp.where(v == 3, 3, reach(v, 8))) for v in z_there]

    def exchange_rest(src, dst, s_sem, r_sem, part=slice(None)):
        for dz, dy, dx, dc in send_order()[part]:
            zh, zl = z_parts[dz]
            slab_to = planes[dy][dx] * 8 + (zh * 2 + (core if dc == 0 else 1 - core))
            start = send(src(slab_to, zl), dst, s_sem, r_sem, (slab_to, zl)).start
            pl.when(y_reach[dy] + x_reach[dx] + z_reach[dz] > NEAR)(start)

    def exchange_first(src, dst, s_sem, r_sem, part=slice(None)):
        for slab_to, cell_to in first_devices()[part]:
            pl.when(me != slab_to * 2 + cell_to)(send(src(slab_to, cell_to), dst, s_sem, r_sem, (slab_to, cell_to)).start)

    exchange(lambda slab_to, cell_to: s1.at[pl.ds(slab_to * 2 + cell_to, 1)], r1.at[cell, pl.ds(slab, 1)], a1_s, a1_r.at[cell])
    r1[cell, pl.ds(slab, 1), :] = s1[pl.ds(me, 1), :]

    tile, k2c = lax.div(me, 128), lax.rem(me, 128)
    lower = k2c < 64
    group = lax.div(lane, 32)
    order = lax.rem(lane, 8)

    def q_of(h):
        kap = 4 * (tile + 2 * h) + group
        return jnp.where(
            kap == 0,
            jnp.where(lower, 32 * k2c, 16 + 32 * (k2c - 64)),
            jnp.where(lower, kap + 32 * k2c, 32 - kap + 32 * (k2c - 64)),
        )

    qs = [q_of(h) for h in range(2)]

    def weigh(i, carry):
        at = pl.multiple_of(i * 16, 16)
        p1 = lax.broadcasted_iota(I32, (16, 128), 0) + at
        up = order < 4
        p = jnp.where(up, p1 + 512 * order, 512 - p1 + 512 * (order - 4))
        p = jnp.where(jnp.logical_and(p1 == 0, jnp.logical_not(up)), 256 + 512 * (order - 4), p)
        p_float = p.astype(F32)
        pt[pl.ds(at, 16), :] = p_float
        for h in range(2):
            q_float = qs[h].astype(F32)
            k2 = p_float * p_float + q_float * q_float
            scale = jnp.where(p == 0, 1.0 / M, 2.0 / M) * jnp.where(qs[h] == 0, 1.0 / M, 2.0 / M) * (1.0 / STEP)
            aw[pl.ds(256 * h + at, 16), :] = jnp.where(k2 == 0.0, 0.0, scale / jnp.where(k2 == 0.0, 1.0, k2))
        return carry

    lax.fori_loop(0, 16, weigh, 0)

    for copy in fetched[2:]:
        copy.wait()
    for k in range(2):
        for i in range(4):
            for j in range(2):
                rows, lanes = slice(128 * i, 128 * i + 128), slice(128 * j, 128 * j + 128)
                cyi[k, lanes, rows] = cyf[k, rows, lanes].T
    def half_arrived(k):
        for count, here in ((127, cell == k), (128, cell != k)):

            @pl.when(here)
            def _(count=count):
                send(s1.at[pl.ds(0, count)], r1.at[k, pl.ds(0, count)], a1_s, a1_r.at[k], partner).wait_recv()

    def half_of(k):
        high, low = zip(*(split(v) for v in decode(r1[k])))
        whole = (jnp.concatenate(high, axis=1), jnp.concatenate(low, axis=1))
        at = slice(128 * k, 128 * k + 128)
        return [(rows, dot3((cyf[0, rows, at], cyf[1, rows, at]), whole)) for rows in in_two(512)]

    half_arrived(1)
    for rows, got in half_of(1):
        us[rows] = got
    half_arrived(0)
    send(s1.at[pl.ds(0, 255)], s1.at[pl.ds(0, 255)], a1_s, a1_r.at[0], partner).wait_send()

    for rows, got in half_of(0):
        us[rows] += got

    def y_chunk(i, carry):
        at = i * 16
        c, s = ty[0, pl.ds(at, 16), :], ty[1, pl.ds(at, 16), :]
        for h in range(2):
            lanes = slice(128 * h, 128 * h + 128)
            re, im = us[pl.ds(at, 16), lanes], us[pl.ds(256 + at, 16), lanes]
            for half, value in enumerate((re * c + im * s, im * c - re * s)):
                parts = split(value)
                for k in range(2):
                    vs[k, pl.ds(256 * h + at, 16), 128 * half : 128 * half + 128] = parts[k]
        return carry

    for i in range(16):
        y_chunk(i, 0)

    def y_out(rows, table):
        got = dot(vs[0, rows], table)
        return got[:, 0:128] + (got[:, 128:256] + dot(vs[1, rows], table[:, 0:128]))

    for rows in in_two(512):
        gs[rows] = y_out(rows, bf[0])
    top_row = lax.broadcasted_iota(I32, (16, 1), 0) == 0
    for h in range(2):
        at = slice(256 * h, 256 * h + 16)
        gs[at, :] = jnp.where(top_row, y_out(at, bf[1]), gs[at, :])

    q_floats = [q.astype(F32) for q in qs]

    def scale_chunk(i, energy):
        at = i * 16
        p_float = pt[pl.ds(at, 16), :]
        for h in range(2):
            value = gs[pl.ds(256 * h + at, 16), :]
            weighted = value * aw[pl.ds(256 * h + at, 16), :]
            work = weighted * value
            energy = energy + (work[0:8] + work[8:16])
            for f, part in enumerate((weighted * q_floats[h], weighted * p_float)):
                parts = split(part)
                for k in range(2):
                    vs[f, pl.ds(256 * h + at, 16), 128 * k : 128 * k + 128] = parts[k]
        return energy

    energy = zero8
    for i in range(16):
        energy = scale_chunk(i, energy)

    def top_rows(f, h):
        at = slice(256 * h, 256 * h + 16)
        return dot3((vs[f, at, 0:128], vs[f, at, 128:256]), (bi[f, 1, 0], bi[f, 1, 1]))

    def turned(values, c, s):
        re, im = values[:, 0:128], values[:, 128:256]
        return [split(value) for value in (re * c - im * s, re * s + im * c)]

    def keep_turned(values, h, at):
        for half in range(2):
            for k in range(2):
                zs[k, pl.ds(256 * half + at, values[half][k].shape[0]), 128 * h : 128 * h + 128] = values[half][k]

    def copies_of(f):
        return (
            lambda slab_to, cell_to: s2.at[f, cell_to, pl.ds(slab_to, 1)], r2.at[f, pl.ds(me, 1)], a2_s.at[f], a2_r.at[f]
        )

    for rows in in_two(512):
        us[rows] = dot(vs[0, rows], bi2[0]) + dot(vs[0, rows, 0:128], bi[0, 0, 1])
    for h in range(2):
        at = slice(256 * h, 256 * h + 16)
        us[at, :] = jnp.where(top_row, top_rows(0, h), us[at, :])
    for i in range(16):
        for h in range(2):
            at = slice(16 * i, 16 * i + 16)
            keep_turned(turned(us[256 * h + 16 * i : 256 * h + 16 * i + 16, :], ty[0, at, :], ty[1, at, :]), h, 16 * i)
    def back_in_y(f):
        for k, rows in enumerate(in_two(256)):
            got = dot3((cyi[0, rows], cyi[1, rows]), (zs[0], zs[1]))
            s2[f, k] = encode(got[:, 0:128], got[:, 128:256])

    back_in_y(0)
    r2[0, pl.ds(me, 1), :] = s2[0, cell, pl.ds(slab, 1), :]

    exchange_first(*copies_of(0), part=slice(0, LEAD))
    for i in range(2):
        at = 128 * i
        rows = [vs[1, 256 * h + at : 256 * h + at + 128, :] for h in range(2)]
        c, s = ty[0, at : at + 128, :], ty[1, at : at + 128, :]
        top = [top_rows(1, h) for h in range(2)] if i == 0 else None
        got = [dot(r, bi2[1]) + dot(r[:, 0:128], bi[1, 0, 1]) for r in rows]
        values = []
        for h in range(2):
            value = got[h]
            if i == 0:
                value = jnp.concatenate([jnp.where(top_row, top[h], value[0:16]), value[16:]], axis=0)
            values.append(turned(value, c, s))
        count = len(first_devices()) - LEAD
        exchange_first(*copies_of(0), part=slice(LEAD + count // 2 * i, LEAD + count // 2 if i == 0 else None))
        exchange_rest(*copies_of(0), part=slice(FAR // 2 * i, FAR // 2 * i + FAR // 2))
        for h in range(2):
            keep_turned(values[h], h, at)

    back_in_y(1)
    def total(x):
        return jnp.sum(jnp.sum(x, axis=1, keepdims=True), axis=0, keepdims=True)

    row = jnp.where(
        lane == 0, total(excess), jnp.where(lane == 1, total(area), total(energy) * (1.0 / (STEP * M * M)))
    )
    es[0] = row
    e1[plane] = row
    for i in range(1, 16):
        send(es.at[0], e1.at[plane], e_s.at[0], e_r.at[0], device_at(lax.rem(plane + i, 16), column)).start()

    exchange_first(*copies_of(1))
    exchange_rest(*copies_of(1), part=slice(0, NEXT))
    exchange_rest(*copies_of(0), part=slice(FAR, None))
    exchange_rest(*copies_of(1), part=slice(NEXT, None))
    r2[1, pl.ds(me, 1), :] = s2[1, cell, pl.ds(slab, 1), :]

    def push(slot, f, halves):
        got = dot(fb[f, 0 : 256 * halves], pq[slot])
        for k in range(4):
            at = slice(128 * k, 128 * k + 128)
            high_bits = lax.shift_right_logical(cell_row_of(slot, k, 1), 7)
            force = jnp.zeros((1, 128), F32)
            for half in range(halves):
                kept = got[256 * half : 256 * half + 16, at]
                for a in range(1, 16):
                    kept = jnp.where(high_bits == a, got[256 * half + 16 * a : 256 * half + 16 * a + 16, at], kept)
                force = force + jnp.sum(kept * yr[slot, 16 * half : 16 * half + 16, at], axis=0, keepdims=True)
            pf[slot, f : f + 1, at] = force

    def x_gather(f):
        for t in range(2):
            for h, value in enumerate(decode(r2[f, 128 * t : 128 * t + 128, :])):
                parts = split(value.T)
                for k in range(2):
                    for j in range(4):
                        for half in range(2):
                            to = 256 * half + 16 * (4 * (t + 2 * h) + j)
                            zx[to : to + 16, 128 * k : 128 * k + 128] = parts[k][32 * j + 16 * half : 32 * j + 16 * half + 16]

    def x_product(f, halves):
        base, count = 256 * halves[0], 256 * len(halves)
        for rows in in_two(count, base):
            us[rows, :] = dot(zx[rows], w2[f]) + dot(zx[rows, 0:128], w[f, 0, 1])
        for half in halves:
            first = slice(256 * half, 256 * half + 16)
            us[first, :] = dot3((zx[first, 0:128], zx[first, 128:256]), (w[f, 1, 0], w[f, 1, 1]))

    def x_inverse(f, out, half):
        base = 256 * half
        got = {}
        for kap in range(16):
            rows = slice(base + 16 * kap, base + 16 * kap + 16)
            re, im = us[rows, 0:128], us[rows, 128:256]
            if kap == 0:
                got[0], got[16] = re, im
            else:
                c, s = tx[0, kap : kap + 1, :], tx[1, kap : kap + 1, :]
                got[kap] = (re * c - im * s, re * s + im * c)
        for a, value in enumerate(real_back(got, 16)):
            lanes = slice(128 * a, 128 * a + 128)
            for g in range(REGIONS):
                out[g, 4 * half : 4 * half + 4, lanes] = value[4 * g : 4 * g + 4]
            near = value.astype(BF)
            fb[f, base + 16 * a : base + 16 * a + 16, 0:128] = near
            if a:
                fb[f, base + 16 * a - 16 : base + 16 * a, 128:256] = near
        fb[f, base + 240 : base + 256, 128:256] = jnp.zeros((16, 128), BF)

    def give_back(slot, device, sem, into):
        return send(pf.at[slot], pr.at[into], f_s.at[sem], f_r.at[into], device)

    def arrived(f):
        whole = send(r2.at[f, pl.ds(0, 255)], r2.at[f, pl.ds(0, 255)], a2_s.at[f], a2_r.at[f], partner)
        whole.wait_recv()
        whole.wait_send()

    sums_wait = send(e1.at[pl.ds(0, 15)], e1.at[pl.ds(0, 15)], e_s.at[0], e_r.at[0], partner)
    sums_wait.wait_recv()
    sums_wait.wait_send()
    row = jnp.sum(e1[...], axis=0)
    es[1] = row
    e2[column] = row
    for i in range(1, 16):
        send(es.at[1], e2.at[column], e_s.at[1], e_r.at[1], device_at(plane, lax.rem(column + i, 16))).start()
    arrived(0)
    x_gather(0)
    x_product(0, (0, 1))
    for half in range(2):
        x_inverse(0, field_x, half)

    @pl.when(has_prev)
    def _():
        for k in range(2):
            push(2 + k, 0, 1)

    push(other, 0, 2)
    push(mine, 0, 2)
    arrived(1)
    x_gather(1)
    x_product(1, (0,))
    x_inverse(1, field_y, 0)

    @pl.when(has_prev)
    def _():
        for k in range(2):
            push(2 + k, 1, 1)
        for k in range(2):
            give_back(2 + k, (slab - 1, k), 1 + k, 1).start()

    x_product(1, (1,))
    x_inverse(1, field_y, 1)
    push(other, 1, 2)
    give_back(other, partner, 0, 0).start()
    push(mine, 1, 2)

    @pl.when(jnp.logical_not(has_next))
    def _():
        pr[1] = jnp.zeros((2, CELLS_DEV), F32)

    give_back(other, partner, 0, 0).wait_recv()

    @pl.when(has_next)
    def _():
        give_back(other, partner, 0, 1).wait_recv()

    force[...] = pf[mine] + pr[0] + pr[1]

    send(e2.at[pl.ds(0, 15)], e2.at[pl.ds(0, 15)], e_s.at[1], e_r.at[1], partner).wait()
    sums[...] = jnp.sum(e2[...], axis=0)

    give_back(other, partner, 0, 0).wait_send()
    for copy in give:
        copy.wait_send()

    @pl.when(has_prev)
    def _():
        for k in range(2):
            give_back(2 + k, (slab - 1, k), 1 + k, 1).wait_send()

    @pl.when(has_next)
    def _():
        for copy in give_next:
            copy.wait_send()


def finish(field_x, field_y, force, sums, out_x, out_y, out_force, energy, overflow, small, sem):
    pairs = ((field_x, out_x), (field_y, out_y), (force, out_force), (small.at[0], energy), (small.at[1], overflow))
    copies = [pltpu.make_async_copy(src, dst, sem.at[k]) for k, (src, dst) in enumerate(pairs)]
    for copy in copies[:3]:
        copy.start()
    row = sums[...]
    small[0] = row[:, 2:3]
    small[1] = row[:, 0:1] / row[:, 1:2]
    for copy in copies[3:]:
        copy.start()
    for copy in copies:
        copy.wait()


def body(cell_row, cell_col, cell_width, cell_height, cell_region, cell_offset):
    consts = [jnp.asarray(t) for t in tables()]
    whole = [v.reshape(4, 128) for v in (cell_row, cell_col, cell_width, cell_height, cell_region)]
    vmem = pl.BlockSpec(memory_space=pltpu.VMEM)
    hbm = pl.BlockSpec(memory_space=pltpu.HBM)
    V = pltpu.VMEM
    D = pltpu.SemaphoreType.DMA
    scratch = [
        V((4, 5, 4, 128), I32),
        V((4, 2, CELLS_DEV), F32),
        V((4, 256, 512), BF),
        V((3, 512, 512), BF),
        V((4, 32, CELLS_DEV), F32),
        V((512, 256), F32),
        V((2, 512, 256), BF),
        V((256, 128), I32),
        V((2, 128, 128), I32),
        V((512, 256), F32),
        V((2, 512, 256), BF),
        V((512, 128), F32),
        V((512, 128), F32),
        V((256, 128), F32),
        V((2, 2, 128, 128), I32),
        V((2, 256, 128), I32),
        V((512, 256), BF),
        V((2, 512, 256), BF),
        V((4, 2, CELLS_DEV), F32),
        V((2, 2, CELLS_DEV), F32),
        V((16, 1, 128), F32),
        V((16, 1, 128), F32),
        V((2, 1, 128), F32),
        V((2, 2, 2, 128, 256), BF),
        V((2, 256, 256), BF),
        V((2, 256, 256), BF),
        V((2, 16, 128), F32),
        V((2, 512, 256), BF),
        V((2, 256, 512), BF),
        V((2, 256, 128), F32),
        V((2, 256, 256), BF),
        V((2, 2, 2, 128, 256), BF),
        V((2, 256, 256), BF),
        D((11,)), D((6,)),
        pltpu.SemaphoreType.REGULAR((2,)),
        D((4,)), D((2, 4)),
        D, D((2,)), D((2,)), D((2,)),
        D((3,)), D((2,)),
        D((2,)), D((2,)),
    ]
    field = (REGIONS, 8, M)
    results = pl.pallas_call(
        kernel,
        out_shape=(V(field, F32), V(field, F32), V((2, CELLS_DEV), F32), V((1, 128), F32)),
        in_specs=[hbm] * (6 + len(consts)),
        out_specs=(vmem,) * 4,
        scratch_shapes=scratch,
        compiler_params=pltpu.CompilerParams(
            collective_id=0, has_side_effects=True, vmem_limit_bytes=66300000
        ),
        name="placement",
    )(*whole, cell_offset, *consts)
    S = jax.ShapeDtypeStruct
    field_x, field_y, force, energy, overflow = pl.pallas_call(
        finish,
        out_shape=(S(field, F32), S(field, F32), S((2, CELLS_DEV), F32), S((1, 1), F32), S((1, 1), F32)),
        in_specs=[vmem] * 4,
        out_specs=(hbm,) * 5,
        scratch_shapes=[V((2, 1, 1), F32), D((5,))],
        compiler_params=pltpu.CompilerParams(vmem_limit_bytes=4 * 1024 * 1024),
        name="finish",
    )(*results)
    return (field_x, field_y, force, energy.reshape(()), overflow.reshape(()))


def solution(mesh):
    both = ("slab", "cell")
    placed = (P(both),) * 5 + (P(None, both),)
    return jax.shard_map(
        body,
        mesh=mesh,
        in_specs=placed,
        out_specs=(P(None, both, None), P(None, both, None), P(None, both), P(), P()),
        check_vma=False,
    )
```

```python
import functools
import math

import jax
import jax.numpy as jnp
import numpy as np
from jax import lax
from jax.experimental import pallas as pl
from jax.experimental.pallas import tpu as pltpu
from jax.sharding import PartitionSpec as P

M = 2048
REGIONS = 4
SLABS = 128
CELLS_DEV = 512
BF = jnp.bfloat16
F32 = jnp.float32
I32 = jnp.int32
MESH = pl.DeviceIdType.MESH
STEP = math.pi / M
FAR = 98
NEXT = 14
NEAR = 1
LEAD = 4


def c_add(x,y): return (x[0]+y[0], x[1]+y[1])
def c_sub(x,y): return (x[0]-y[0], x[1]-y[1])
def c_turn(x,angle):
    c,s=math.cos(angle),math.sin(angle)
    if abs(s)<1e-12: return x if c>0 else (-x[0],-x[1])
    if abs(c)<1e-12: return (-x[1],x[0]) if s>0 else (x[1],-x[0])
    if abs(abs(c)-abs(s))<1e-12:
        h=abs(c); a,b=x[0],x[1]
        sc,ss=(1 if c>0 else -1),(1 if s>0 else -1)
        def lin(p,a,q,b):
            if p>0: return (a+b)*h if q>0 else (a-b)*h
            return (b-a)*h if q>0 else (a+b)*(-h)
        return (lin(sc,a,-ss,b), lin(ss,a,sc,b))
    return (x[0]*c-x[1]*s, x[0]*s+x[1]*c)
def c_fft(xs,sign):
    n=len(xs)
    if n==1: return xs
    even,odd=c_fft(xs[0::2],sign),c_fft(xs[1::2],sign)
    out=[None]*n
    for k in range(n//2):
        t=c_turn(odd[k],sign*2*math.pi*k/n)
        out[k],out[k+n//2]=c_add(even[k],t),c_sub(even[k],t)
    return out
def real_spectrum(d):
    n=len(d)
    if n==2:
        return {0:d[0]+d[1],1:(d[0],-d[1]),2:d[0]-d[1]}
    half=n//2
    out={}
    z=[c_turn((d[a],-d[a+half]),-math.pi*a/n) for a in range(half)]
    f=c_fft(z,-1)
    for m in range(half):
        k=1+4*m
        if k<n: out[k]=f[m]
        else: out[2*n-k]=(f[m][0],-f[m][1])
    s=[d[a]+d[a+half] for a in range(half)]
    e=[d[a]-d[a+half] for a in range(half)]
    q=half//2
    z=[c_turn((e[a],-e[a+q]),-2*math.pi*a/n) for a in range(q)]
    f=c_fft(z,-1)
    for l in range(q):
        m=1+4*l
        if m<=half: out[2*m]=f[l]
        else: out[2*(n-m)]=(f[l][0],-f[l][1])
    sub=real_full(s)
    for l,v in sub.items(): out[4*l]=v
    return out
def real_full(s):
    n=len(s)
    if n==2: return {0:s[0]+s[1],1:s[0]-s[1]}
    half=n//2
    p=[s[a]+s[a+half] for a in range(half)]
    e=[s[a]-s[a+half] for a in range(half)]
    out={}
    for l,v in real_full(p).items(): out[2*l]=v
    q=half//2
    if q==0: return out
    z=[c_turn((e[a],-e[a+q]),-2*math.pi*a/n) for a in range(q)] if q else []
    f=c_fft(z,-1)
    for k in range(q):
        l=1+4*k
        if l<=half: out[l]=f[k]
        else: out[n-l]=(f[k][0],-f[k][1])
    return out
def real_full_back(v,n):
    if n==2: return [v[0]+v[1],v[0]-v[1]]
    half=n//2; q=half//2
    p=real_full_back({l//2:x for l,x in v.items() if l%2==0},half)
    if n==4:
        g=[v[1]]
    else:
        g=[v[1+4*k] if 1+4*k<=half else (v[n-1-4*k][0],-v[n-1-4*k][1]) for k in range(q)]
    f=c_fft(g,1)
    odd=[None]*half
    for a in range(q):
        t=c_turn(f[a],2*math.pi*a/n)
        odd[a],odd[a+q]=t[0],-t[1]
    out=[None]*n
    for a in range(half):
        out[a],out[a+half]=p[a]+odd[a],p[a]-odd[a]
    return out
def real_back(y,n):
    half=n//2
    even=real_full_back({k//2:v for k,v in y.items() if k%2==0},n)
    g=[y[1+4*m] if 1+4*m<n else (y[2*n-1-4*m][0],-y[2*n-1-4*m][1]) for m in range(half)]
    f=c_fft(g,1)
    out=[None]*n
    for a in range(half):
        t=c_turn(f[a],math.pi*a/n)
        out[a],out[a+half]=even[a]+t[0],even[a+half]-t[1]
    return out


def split_np(table):
    high = table.astype(np.float32).astype(BF)
    low = (table - high.astype(np.float64)).astype(np.float32).astype(BF)
    return np.stack([high, low])


@functools.lru_cache(None)
def tables():
    pi = np.pi
    k2 = np.arange(64)[:, None]
    b = np.arange(128)[None, :]
    c1, s1 = np.cos(pi * k2 * (2 * b + 1) / 128), np.sin(pi * k2 * (2 * b + 1) / 128)
    c2, s2 = np.cos(pi * (k2 + 1) * (2 * b + 1) / 128), np.sin(pi * (k2 + 1) * (2 * b + 1) / 128)
    cm, sm = np.cos(pi * (2 * k2 + 1) * (2 * b + 1) / 256), np.sin(pi * (2 * k2 + 1) * (2 * b + 1) / 256)
    zero = np.zeros_like(c1)
    wc = np.block([[c1, s1], [c2, -s2]])
    wc0 = np.block([[c1, zero], [zero, cm]])
    ws = np.block([[s1, -c1], [s2, c2]])
    ws0 = np.block([[s1, zero], [zero, sm]])
    w = np.stack([split_np(m) for m in (ws, ws0, wc, wc0)]).reshape(2, 2, 2, 128, 256)
    wt = np.stack([np.concatenate(list(split_np(m.T)), axis=1) for m in (wc, wc0)])
    kap = np.arange(16)[:, None]
    ang = pi * kap * (2 * b + 1) / 4096
    tx = np.stack([np.cos(ang), np.sin(ang)]).astype(np.float32)
    p1 = np.arange(256)[:, None]
    d = np.arange(256)[None, :]
    cre, cim = np.cos(2 * pi * p1 * d / 512), -np.sin(2 * pi * p1 * d / 512)
    cim[0] = (-1.0) ** np.arange(256)
    cy = np.concatenate([cre, cim], 0)[:, np.arange(256).reshape(128, 2).T.reshape(-1)]
    ours = np.arange(128).reshape(4, 4, 2, 4).transpose(0, 2, 1, 3).reshape(-1)
    cy_fwd = split_np(cy)
    r = np.arange(8)
    angy = pi * p1 * (2 * r[None, :] + 1) / 4096
    ty = np.stack([np.tile(np.cos(angy), (1, 16)), np.tile(np.sin(angy), (1, 16))])[:, :, ours].astype(np.float32)
    p2 = np.arange(4)[None, :]
    rr = r[:, None]
    e0, e1 = pi * p2 * (2 * rr + 1) / 8, pi * (p2 + 1) * (2 * rr + 1) / 8
    em = pi * (2 * rr + 1) * (1 + 2 * p2) / 16
    z8 = np.zeros((8, 4))
    bc = (np.block([np.cos(e0), np.cos(e1)]), np.block([np.sin(e0), -np.sin(e1)]))
    bc0 = (np.block([np.cos(e0), z8]), np.block([z8, np.cos(em)]))
    bs = (np.block([np.sin(e0), np.sin(e1)]), np.block([-np.cos(e0), np.cos(e1)]))
    bs0 = (np.block([np.sin(e0), z8]), np.block([z8, np.sin(em)]))

    def wide(pair):
        return np.concatenate([np.kron(np.eye(16), part)[ours] for part in pair], 0)

    b_fwd = np.stack([np.concatenate(list(split_np(wide(m))), axis=1) for m in (bc, bc0)])
    b_inv = np.stack([split_np(wide(m).T) for m in (bc, bc0, bs, bs0)]).reshape(2, 2, 2, 128, 256)
    return w, wt, tx, cy_fwd, ty, b_fwd, b_inv


def dot(x, y):
    return lax.dot_general(x, y, (((1,), (0,)), ((), ())), preferred_element_type=F32)


def dot_nt(x, y):
    return lax.dot_general(x, y, (((1,), (1,)), ((), ())), preferred_element_type=F32)


def split(x):
    high = x.astype(BF)
    return high, (x - high.astype(F32)).astype(BF)


def dot3(x, y):
    return dot(x[0], y[0]) + (dot(x[0], y[1]) + dot(x[1], y[0]))


def dot3_nt(x, y):
    return dot_nt(x[0], y[0]) + (dot_nt(x[0], y[1]) + dot_nt(x[1], y[0]))


def encode(x, y):
    top = jnp.maximum(jnp.maximum(jnp.abs(x), jnp.abs(y)), 2.0**-31)
    exponent = jnp.minimum(jnp.floor(jnp.log2(top)), 31.0)
    scale = jnp.exp2(11.0 - exponent)

    def code(v):
        return jnp.clip(jnp.round(v * scale), -4095.0, 4095.0).astype(I32)

    high = jnp.left_shift(exponent.astype(I32) + 32, 26)
    return high | jnp.left_shift(code(y) & 0x1FFF, 13) | (code(x) & 0x1FFF)


def decode(word):
    scale = jnp.exp2(lax.shift_right_logical(word, 26).astype(F32) - 43.0)
    x = lax.shift_right_arithmetic(jnp.left_shift(word, 19), 19).astype(F32)
    y = lax.shift_right_arithmetic(jnp.left_shift(word, 6), 19).astype(F32)
    return x * scale, y * scale


@functools.lru_cache(None)
def send_order():
    rng = np.random.default_rng(0)
    every = [(dz, dy, dx, dc) for dz in range(8) for dy in range(4) for dx in range(4) for dc in range(2)]
    every = [d for d in every if any(d)]
    hops = {d: min(d[0], 8 - d[0]) + min(d[1], 4 - d[1]) + min(d[2], 4 - d[2]) + 0.5 * d[3] for d in every}
    return sorted(every, key=lambda d: (-hops[d], rng.random()))


def in_two(count, base=0):
    return [slice(base + k * count // 2, base + (k + 1) * count // 2) for k in range(2)]


@functools.lru_cache(None)
def first_devices():
    def reach(value, count):
        return min(value, count - value)

    found = []
    for slab in range(SLABS):
        for cell in range(2):
            y, x, z = slab // 32, slab // 8 % 4, slab // 2 % 4 * 2 + cell
            plane = reach(y, 4) + reach(x, 4)
            if reach(y, 4) + min(x, 1) + (0 if z < 3 else 3 if z == 3 else reach(z, 8)) <= NEAR:
                own = slab in (1, 2) and (slab, cell) != (2, 1)
                found.append((0 if own and plane == 0 else 1 + plane + reach(z, 8) - 0.5 * (slab % 2), slab, cell))
    return [(slab, cell) for _, slab, cell in sorted(found)]


def place():
    slab = lax.axis_index("slab")
    cell = lax.axis_index("cell")
    return slab, cell, lax.div(slab, 8), lax.rem(slab, 8) * 2 + cell


def device_at(plane, column):
    return (plane * 8 + lax.div(column, 2), lax.rem(column, 2))


def overlap(bins, low, high):
    return jnp.maximum(jnp.minimum(bins + 1.0, high) - jnp.maximum(bins, low), 0.0)


def kernel(
    row_h, col_h, width_h, height_h, region_h, offset_h,
    w_h, wt_h, tx_h, cyf_h, ty_h, bf_h, bi_h,
    field_x, field_y, force, sums,
    ci, co, pq, ym, yr, d2, zs, s1, r1, us, vs, gs, aw, pt, s2, r2, zx, fb, pf, pr, e1, e2, es,
    w, w2, wt, tx, cyf, cyi, ty, bf, bi, bi2,
    const_sem, in_sem, met, cell_s, cell_r, a1_s, a1_r, a2_s, a2_r, f_s, f_r, e_s, e_r,
):
    slab, cell, plane, column = place()
    me = plane * 16 + column
    mine, other = cell, 1 - cell
    has_prev = jnp.logical_and(cell == 0, slab > 0)
    has_next = slab < SLABS - 1
    barrier = pltpu.get_barrier_semaphore()

    own = [
        pltpu.make_async_copy(src, ci.at[mine, k], in_sem.at[k])
        for k, src in enumerate((row_h, col_h, width_h, height_h, region_h))
    ]
    own.append(pltpu.make_async_copy(offset_h, co.at[mine], in_sem.at[5]))
    for copy in own:
        copy.start()

    def signal_at(sem, device):
        pl.semaphore_signal(sem, inc=1, device_id=device, device_id_type=MESH)

    py, px = lax.div(plane, 4), lax.rem(plane, 4)
    ys = [lax.rem(py + k, 4) for k in range(4)]
    xs = [lax.rem(px + k, 4) for k in range(4)]
    x_line = [device_at(py * 4 + xs[k], column) for k in (2, 1, 3)]
    y_line = [device_at(ys[k] * 4 + px, column) for k in (2, 1, 3)]
    column_peers = [device_at(plane, lax.rem(column + i, 16)) for i in (8, 7, 9, 6, 10, 5, 11, 4, 12, 3, 13, 2, 14, 1, 15)]
    for device in column_peers + x_line + y_line:
        signal_at(barrier, device)

    @pl.when(has_prev)
    def _():
        signal_at(barrier, (slab - 1, 0))
        signal_at(barrier, (slab - 1, 1))

    z, core = lax.div(column, 4) * 2 + cell, lax.rem(lax.div(column, 2), 2)

    for copy in own:
        copy.wait()

    low_row = slab * 16 + cell * 8

    def cell_row_of(slot, k, which):
        return ci[slot, which, k : k + 1, :]

    def make_cells(slot, halves, masked):
        bins = lax.broadcasted_iota(I32, (128, 128), 0).astype(F32).astype(BF)
        line = lax.broadcasted_iota(I32, (16, 128), 0)
        rows = (jnp.bitwise_and(line, 3) + low_row).astype(F32)
        region_of = lax.shift_right_logical(line, 2)
        for k in range(4):
            at = slice(128 * k, 128 * k + 128)
            col = cell_row_of(slot, k, 1)
            high_bits = lax.shift_right_logical(col, 7)
            low_bits = (col - high_bits * 128).astype(F32).astype(BF)
            start = co[slot, 0:1, at]
            width = cell_row_of(slot, k, 2).astype(F32)
            first = (1.0 - start).astype(BF)
            last = ((start + width) - width).astype(BF)
            width = width.astype(BF)
            reach = bins - low_bits
            for far in range(2):
                if far:
                    reach = reach + BF(128.0)
                got = jnp.minimum(reach + first, (width - reach) + last)
                pq[slot, 128 * far : 128 * far + 128, at] = jnp.clip(got, BF(0.0), BF(1.0))
            start = co[slot, 1:2, at]
            end = start + cell_row_of(slot, k, 3).astype(F32)
            reach = rows - cell_row_of(slot, k, 0).astype(F32)
            here = cell_row_of(slot, k, 4) == region_of
            for half in range(halves):
                got = jnp.where(here, overlap(reach + 4.0 * half, start, end), 0.0)
                yr[slot, 16 * half : 16 * half + 16, at] = got.astype(BF).astype(F32)
                for a in range(16):
                    to = slice(256 * half + 16 * a, 256 * half + 16 * a + 16)
                    masked[to, at] = jnp.where(high_bits == a, got, 0.0).astype(BF)

    def send(src, dst, s_sem, r_sem, device):
        return pltpu.make_async_remote_copy(
            src_ref=src, dst_ref=dst, send_sem=s_sem, recv_sem=r_sem, device_id=device, device_id_type=MESH
        )

    pl.semaphore_wait(barrier, 21 + has_next.astype(I32))
    partner = (slab, other)
    give = [
        send(ci.at[mine], ci.at[mine], cell_s.at[0], cell_r.at[0, mine], partner),
        send(co.at[mine], co.at[mine], cell_s.at[1], cell_r.at[1, mine], partner),
    ]
    give_next = [
        send(ci.at[mine], ci.at[2 + mine], cell_s.at[2], cell_r.at[0, 2 + mine], (slab + 1, 0)),
        send(co.at[mine], co.at[2 + mine], cell_s.at[3], cell_r.at[1, 2 + mine], (slab + 1, 0)),
    ]
    for copy in give:
        copy.start()

    @pl.when(has_next)
    def _():
        for copy in give_next:
            copy.start()

    for device in x_line:
        signal_at(met.at[0], device)

    fetched = [
        pltpu.make_async_copy(src, dst, const_sem.at[k])
        for k, (src, dst) in enumerate(
            (
                (tx_h, tx), (wt_h, wt), (w_h, w), (w_h.at[:, 0, 0], w2.at[:, 0:128]), (w_h.at[:, 0, 0], w2.at[:, 128:256]),
                (cyf_h, cyf), (ty_h, ty), (bf_h, bf), (bi_h, bi),
                (bi_h.at[:, 0, 0], bi2.at[:, 0:128]), (bi_h.at[:, 0, 0], bi2.at[:, 128:256]),
            )
        )
    ]
    for copy in fetched:
        copy.start()

    def arrive(slot):
        send(ci.at[slot], ci.at[slot], cell_s.at[0], cell_r.at[0, slot], partner).wait_recv()
        send(co.at[slot], co.at[slot], cell_s.at[1], cell_r.at[1, slot], partner).wait_recv()

    make_cells(mine, 2, ym.at[0])
    for rows in in_two(512):
        d2[rows] = dot_nt(ym[0, rows], pq[mine])
    arrive(other)
    pl.semaphore_wait(met.at[0], 3)
    for device in y_line:
        signal_at(met.at[1], device)
    make_cells(other, 2, ym.at[0])
    for rows in in_two(512):
        d2[rows] += dot_nt(ym[0, rows], pq[other])

    zero8 = jnp.zeros((8, 128), F32)
    lane = lax.broadcasted_iota(I32, (1, 128), 1)
    first_group = lane < 32

    def x_forward(half, excess, area):
        here = []
        for a in range(16):
            at = 256 * half + 16 * a
            value = d2[at : at + 16, 0:128]
            if a:
                value = value + d2[at - 16 : at, 128:256]
            here.append(value)
            over = jnp.maximum(value - 1.0, 0.0)
            excess = excess + (over[0:8] + over[8:16])
            area = area + (value[0:8] + value[8:16])
        got = real_spectrum(here)
        for kap in range(16):
            at = slice(256 * half + 16 * kap, 256 * half + 16 * kap + 16)
            if kap == 0:
                pair = (got[0], got[16])
            else:
                (re, im), c, s = got[kap], tx[0, kap : kap + 1, :], tx[1, kap : kap + 1, :]
                pair = (re * c + im * s, im * c - re * s)
            for part, value in enumerate(pair):
                parts = split(value)
                for k in range(2):
                    zs[k, at, 128 * part : 128 * part + 128] = parts[k]

        return excess, area

    def x_product_forward(rows, kind):
        got = dot(zs[0, rows], wt[kind])
        return got[:, 0:128] + (got[:, 128:256] + dot(zs[1, rows], wt[kind, :, 0:128]))

    fetched[0].wait()
    fetched[1].wait()
    excess, area = x_forward(1, zero8, zero8)

    @pl.when(has_prev)
    def _():
        for k in range(2):
            arrive(2 + k)
        for k in range(2):
            make_cells(2 + k, 1, ym.at[1 + k])
        for rows in in_two(256):
            d2[rows] += dot_nt(ym[1, rows], pq[2]) + dot_nt(ym[2, rows], pq[3])

    excess, area = x_forward(0, excess, area)
    for rows in in_two(512):
        gs[rows] = x_product_forward(rows, 0)
    for half in range(2):
        first = slice(256 * half, 256 * half + 16)
        gs[first] = x_product_forward(first, 1)
    tiles = []
    for t in range(4):
        rows = [gs[256 * half + 16 * kap : 256 * half + 16 * kap + 16] for kap in range(4 * t, 4 * t + 4) for half in range(2)]
        tiles.append(jnp.concatenate(rows, axis=0).T)
    for t in range(2):
        s1[128 * t : 128 * t + 128, :] = encode(tiles[t], tiles[t + 2])

    pl.semaphore_wait(met.at[1], 3)
    planes = [[ys[dy] * 4 + xs[dx] for dx in range(4)] for dy in range(4)]
    z_there = [lax.rem(z + k, 8) for k in range(8)]
    z_parts = [(lax.div(k, 2), lax.rem(k, 2)) for k in z_there]

    def exchange(src, dst, s_sem, r_sem, part=slice(None)):
        for dz, dy, dx, dc in send_order()[part]:
            zh, zl = z_parts[dz]
            slab_to = planes[dy][dx] * 8 + (zh * 2 + (core if dc == 0 else 1 - core))
            send(src(slab_to, zl), dst, s_sem, r_sem, (slab_to, zl)).start()

    def reach(value, count):
        return jnp.minimum(value, count - value)

    y_reach, x_reach = [reach(v, 4) for v in ys], [jnp.minimum(v, 1) for v in xs]
    z_reach = [jnp.where(v < 3, 0, jnp.where(v == 3, 3, reach(v, 8))) for v in z_there]

    def exchange_rest(src, dst, s_sem, r_sem, part=slice(None)):
        for dz, dy, dx, dc in send_order()[part]:
            zh, zl = z_parts[dz]
            slab_to = planes[dy][dx] * 8 + (zh * 2 + (core if dc == 0 else 1 - core))
            start = send(src(slab_to, zl), dst, s_sem, r_sem, (slab_to, zl)).start
            pl.when(y_reach[dy] + x_reach[dx] + z_reach[dz] > NEAR)(start)

    def exchange_first(src, dst, s_sem, r_sem, part=slice(None)):
        for slab_to, cell_to in first_devices()[part]:
            pl.when(me != slab_to * 2 + cell_to)(send(src(slab_to, cell_to), dst, s_sem, r_sem, (slab_to, cell_to)).start)

    exchange(lambda slab_to, cell_to: s1.at[pl.ds(slab_to * 2 + cell_to, 1)], r1.at[cell, pl.ds(slab, 1)], a1_s, a1_r.at[cell])
    r1[cell, pl.ds(slab, 1), :] = s1[pl.ds(me, 1), :]

    tile, k2c = lax.div(me, 128), lax.rem(me, 128)
    lower = k2c < 64
    group = lax.div(lane, 32)
    order = lax.rem(lane, 8)

    def q_of(h):
        kap = 4 * (tile + 2 * h) + group
        return jnp.where(
            kap == 0,
            jnp.where(lower, 32 * k2c, 16 + 32 * (k2c - 64)),
            jnp.where(lower, kap + 32 * k2c, 32 - kap + 32 * (k2c - 64)),
        )

    qs = [q_of(h) for h in range(2)]

    def weigh(i, carry):
        at = pl.multiple_of(i * 16, 16)
        p1 = lax.broadcasted_iota(I32, (16, 128), 0) + at
        up = order < 4
        p = jnp.where(up, p1 + 512 * order, 512 - p1 + 512 * (order - 4))
        p = jnp.where(jnp.logical_and(p1 == 0, jnp.logical_not(up)), 256 + 512 * (order - 4), p)
        p_float = p.astype(F32)
        pt[pl.ds(at, 16), :] = p_float
        for h in range(2):
            q_float = qs[h].astype(F32)
            k2 = p_float * p_float + q_float * q_float
            scale = jnp.where(p == 0, 1.0 / M, 2.0 / M) * jnp.where(qs[h] == 0, 1.0 / M, 2.0 / M) * (1.0 / STEP)
            aw[pl.ds(256 * h + at, 16), :] = jnp.where(k2 == 0.0, 0.0, scale / jnp.where(k2 == 0.0, 1.0, k2))
        return carry

    lax.fori_loop(0, 16, weigh, 0)

    for copy in fetched[2:]:
        copy.wait()
    for k in range(2):
        for i in range(4):
            for j in range(2):
                rows, lanes = slice(128 * i, 128 * i + 128), slice(128 * j, 128 * j + 128)
                cyi[k, lanes, rows] = cyf[k, rows, lanes].T
    def half_arrived(k):
        for count, here in ((127, cell == k), (128, cell != k)):

            @pl.when(here)
            def _(count=count):
                send(s1.at[pl.ds(0, count)], r1.at[k, pl.ds(0, count)], a1_s, a1_r.at[k], partner).wait_recv()

    def half_of(k):
        high, low = zip(*(split(v) for v in decode(r1[k])))
        whole = (jnp.concatenate(high, axis=1), jnp.concatenate(low, axis=1))
        at = slice(128 * k, 128 * k + 128)
        return [(rows, dot3((cyf[0, rows, at], cyf[1, rows, at]), whole)) for rows in in_two(512)]

    half_arrived(1)
    for rows, got in half_of(1):
        us[rows] = got
    half_arrived(0)
    send(s1.at[pl.ds(0, 255)], s1.at[pl.ds(0, 255)], a1_s, a1_r.at[0], partner).wait_send()

    for rows, got in half_of(0):
        us[rows] += got

    def y_chunk(i, carry):
        at = i * 16
        c, s = ty[0, pl.ds(at, 16), :], ty[1, pl.ds(at, 16), :]
        for h in range(2):
            lanes = slice(128 * h, 128 * h + 128)
            re, im = us[pl.ds(at, 16), lanes], us[pl.ds(256 + at, 16), lanes]
            for half, value in enumerate((re * c + im * s, im * c - re * s)):
                parts = split(value)
                for k in range(2):
                    vs[k, pl.ds(256 * h + at, 16), 128 * half : 128 * half + 128] = parts[k]
        return carry

    for i in range(16):
        y_chunk(i, 0)

    def y_out(rows, table):
        got = dot(vs[0, rows], table)
        return got[:, 0:128] + (got[:, 128:256] + dot(vs[1, rows], table[:, 0:128]))

    for rows in in_two(512):
        gs[rows] = y_out(rows, bf[0])
    top_row = lax.broadcasted_iota(I32, (16, 1), 0) == 0
    for h in range(2):
        at = slice(256 * h, 256 * h + 16)
        gs[at, :] = jnp.where(top_row, y_out(at, bf[1]), gs[at, :])

    q_floats = [q.astype(F32) for q in qs]

    def scale_chunk(i, energy):
        at = i * 16
        p_float = pt[pl.ds(at, 16), :]
        for h in range(2):
            value = gs[pl.ds(256 * h + at, 16), :]
            weighted = value * aw[pl.ds(256 * h + at, 16), :]
            work = weighted * value
            energy = energy + (work[0:8] + work[8:16])
            for f, part in enumerate((weighted * q_floats[h], weighted * p_float)):
                parts = split(part)
                for k in range(2):
                    vs[f, pl.ds(256 * h + at, 16), 128 * k : 128 * k + 128] = parts[k]
        return energy

    energy = zero8
    for i in range(16):
        energy = scale_chunk(i, energy)

    def top_rows(f, h):
        at = slice(256 * h, 256 * h + 16)
        return dot3((vs[f, at, 0:128], vs[f, at, 128:256]), (bi[f, 1, 0], bi[f, 1, 1]))

    def turned(values, c, s):
        re, im = values[:, 0:128], values[:, 128:256]
        return [split(value) for value in (re * c - im * s, re * s + im * c)]

    def keep_turned(values, h, at):
        for half in range(2):
            for k in range(2):
                zs[k, pl.ds(256 * half + at, values[half][k].shape[0]), 128 * h : 128 * h + 128] = values[half][k]

    def copies_of(f):
        return (
            lambda slab_to, cell_to: s2.at[f, cell_to, pl.ds(slab_to, 1)], r2.at[f, pl.ds(me, 1)], a2_s.at[f], a2_r.at[f]
        )

    for rows in in_two(512):
        us[rows] = dot(vs[0, rows], bi2[0]) + dot(vs[0, rows, 0:128], bi[0, 0, 1])
    for h in range(2):
        at = slice(256 * h, 256 * h + 16)
        us[at, :] = jnp.where(top_row, top_rows(0, h), us[at, :])
    for i in range(16):
        for h in range(2):
            at = slice(16 * i, 16 * i + 16)
            keep_turned(turned(us[256 * h + 16 * i : 256 * h + 16 * i + 16, :], ty[0, at, :], ty[1, at, :]), h, 16 * i)
    def back_in_y(f):
        for k, rows in enumerate(in_two(256)):
            got = dot3((cyi[0, rows], cyi[1, rows]), (zs[0], zs[1]))
            s2[f, k] = encode(got[:, 0:128], got[:, 128:256])

    back_in_y(0)
    r2[0, pl.ds(me, 1), :] = s2[0, cell, pl.ds(slab, 1), :]

    exchange_first(*copies_of(0), part=slice(0, LEAD))
    for i in range(2):
        at = 128 * i
        rows = [vs[1, 256 * h + at : 256 * h + at + 128, :] for h in range(2)]
        c, s = ty[0, at : at + 128, :], ty[1, at : at + 128, :]
        top = [top_rows(1, h) for h in range(2)] if i == 0 else None
        got = [dot(r, bi2[1]) + dot(r[:, 0:128], bi[1, 0, 1]) for r in rows]
        values = []
        for h in range(2):
            value = got[h]
            if i == 0:
                value = jnp.concatenate([jnp.where(top_row, top[h], value[0:16]), value[16:]], axis=0)
            values.append(turned(value, c, s))
        count = len(first_devices()) - LEAD
        exchange_first(*copies_of(0), part=slice(LEAD + count // 2 * i, LEAD + count // 2 if i == 0 else None))
        exchange_rest(*copies_of(0), part=slice(FAR // 2 * i, FAR // 2 * i + FAR // 2))
        for h in range(2):
            keep_turned(values[h], h, at)

    back_in_y(1)
    exchange_first(*copies_of(1))
    def total(x):
        return jnp.sum(jnp.sum(x, axis=1, keepdims=True), axis=0, keepdims=True)

    row = jnp.where(
        lane == 0, total(excess), jnp.where(lane == 1, total(area), total(energy) * (1.0 / (STEP * M * M)))
    )
    es[0] = row
    e1[plane] = row
    for i in range(1, 16):
        send(es.at[0], e1.at[plane], e_s.at[0], e_r.at[0], device_at(lax.rem(plane + i, 16), column)).start()
    exchange_rest(*copies_of(1), part=slice(0, NEXT))
    exchange_rest(*copies_of(0), part=slice(FAR, None))
    exchange_rest(*copies_of(1), part=slice(NEXT, None))
    r2[1, pl.ds(me, 1), :] = s2[1, cell, pl.ds(slab, 1), :]

    def push(slot, f, halves):
        got = dot(fb[f, 0 : 256 * halves], pq[slot])
        for k in range(4):
            at = slice(128 * k, 128 * k + 128)
            high_bits = lax.shift_right_logical(cell_row_of(slot, k, 1), 7)
            force = jnp.zeros((1, 128), F32)
            for half in range(halves):
                kept = got[256 * half : 256 * half + 16, at]
                for a in range(1, 16):
                    kept = jnp.where(high_bits == a, got[256 * half + 16 * a : 256 * half + 16 * a + 16, at], kept)
                force = force + jnp.sum(kept * yr[slot, 16 * half : 16 * half + 16, at], axis=0, keepdims=True)
            pf[slot, f : f + 1, at] = force

    def x_gather(f):
        for t in range(2):
            for h, value in enumerate(decode(r2[f, 128 * t : 128 * t + 128, :])):
                parts = split(value.T)
                for k in range(2):
                    for j in range(4):
                        for half in range(2):
                            to = 256 * half + 16 * (4 * (t + 2 * h) + j)
                            zx[to : to + 16, 128 * k : 128 * k + 128] = parts[k][32 * j + 16 * half : 32 * j + 16 * half + 16]

    def x_product(f, halves):
        base, count = 256 * halves[0], 256 * len(halves)
        for rows in in_two(count, base):
            us[rows, :] = dot(zx[rows], w2[f]) + dot(zx[rows, 0:128], w[f, 0, 1])
        for half in halves:
            first = slice(256 * half, 256 * half + 16)
            us[first, :] = dot3((zx[first, 0:128], zx[first, 128:256]), (w[f, 1, 0], w[f, 1, 1]))

    def x_inverse(f, out, half):
        base = 256 * half
        got = {}
        for kap in range(16):
            rows = slice(base + 16 * kap, base + 16 * kap + 16)
            re, im = us[rows, 0:128], us[rows, 128:256]
            if kap == 0:
                got[0], got[16] = re, im
            else:
                c, s = tx[0, kap : kap + 1, :], tx[1, kap : kap + 1, :]
                got[kap] = (re * c - im * s, re * s + im * c)
        for a, value in enumerate(real_back(got, 16)):
            lanes = slice(128 * a, 128 * a + 128)
            for g in range(REGIONS):
                out[g, 4 * half : 4 * half + 4, lanes] = value[4 * g : 4 * g + 4]
            near = value.astype(BF)
            fb[f, base + 16 * a : base + 16 * a + 16, 0:128] = near
            if a:
                fb[f, base + 16 * a - 16 : base + 16 * a, 128:256] = near
        fb[f, base + 240 : base + 256, 128:256] = jnp.zeros((16, 128), BF)

    def give_back(slot, device, sem, into):
        return send(pf.at[slot], pr.at[into], f_s.at[sem], f_r.at[into], device)

    def arrived(f):
        whole = send(r2.at[f, pl.ds(0, 255)], r2.at[f, pl.ds(0, 255)], a2_s.at[f], a2_r.at[f], partner)
        whole.wait_recv()
        whole.wait_send()

    sums_wait = send(e1.at[pl.ds(0, 15)], e1.at[pl.ds(0, 15)], e_s.at[0], e_r.at[0], partner)
    sums_wait.wait_recv()
    sums_wait.wait_send()
    row = jnp.sum(e1[...], axis=0)
    es[1] = row
    e2[column] = row
    for i in range(1, 16):
        send(es.at[1], e2.at[column], e_s.at[1], e_r.at[1], device_at(plane, lax.rem(column + i, 16))).start()
    arrived(0)
    x_gather(0)
    x_product(0, (0, 1))
    for half in range(2):
        x_inverse(0, field_x, half)

    @pl.when(has_prev)
    def _():
        for k in range(2):
            push(2 + k, 0, 1)

    push(other, 0, 2)
    push(mine, 0, 2)
    arrived(1)
    x_gather(1)
    x_product(1, (0,))
    x_inverse(1, field_y, 0)

    @pl.when(has_prev)
    def _():
        for k in range(2):
            push(2 + k, 1, 1)
            give_back(2 + k, (slab - 1, k), 1 + k, 1).start()

    x_product(1, (1,))
    x_inverse(1, field_y, 1)
    push(other, 1, 2)
    give_back(other, partner, 0, 0).start()
    push(mine, 1, 2)

    @pl.when(jnp.logical_not(has_next))
    def _():
        pr[1] = jnp.zeros((2, CELLS_DEV), F32)

    give_back(other, partner, 0, 0).wait_recv()

    @pl.when(has_next)
    def _():
        give_back(other, partner, 0, 1).wait_recv()

    force[...] = pf[mine] + pr[0] + pr[1]

    send(e2.at[pl.ds(0, 15)], e2.at[pl.ds(0, 15)], e_s.at[1], e_r.at[1], partner).wait()
    sums[...] = jnp.sum(e2[...], axis=0)

    give_back(other, partner, 0, 0).wait_send()
    for copy in give:
        copy.wait_send()

    @pl.when(has_prev)
    def _():
        for k in range(2):
            give_back(2 + k, (slab - 1, k), 1 + k, 1).wait_send()

    @pl.when(has_next)
    def _():
        for copy in give_next:
            copy.wait_send()


def finish(field_x, field_y, force, sums, out_x, out_y, out_force, energy, overflow, small, sem):
    pairs = ((field_x, out_x), (field_y, out_y), (force, out_force), (small.at[0], energy), (small.at[1], overflow))
    copies = [pltpu.make_async_copy(src, dst, sem.at[k]) for k, (src, dst) in enumerate(pairs)]
    for copy in copies[:3]:
        copy.start()
    row = sums[...]
    small[0] = row[:, 2:3]
    small[1] = row[:, 0:1] / row[:, 1:2]
    for copy in copies[3:]:
        copy.start()
    for copy in copies:
        copy.wait()


def body(cell_row, cell_col, cell_width, cell_height, cell_region, cell_offset):
    consts = [jnp.asarray(t) for t in tables()]
    whole = [v.reshape(4, 128) for v in (cell_row, cell_col, cell_width, cell_height, cell_region)]
    vmem = pl.BlockSpec(memory_space=pltpu.VMEM)
    hbm = pl.BlockSpec(memory_space=pltpu.HBM)
    V = pltpu.VMEM
    D = pltpu.SemaphoreType.DMA
    scratch = [
        V((4, 5, 4, 128), I32),
        V((4, 2, CELLS_DEV), F32),
        V((4, 256, 512), BF),
        V((3, 512, 512), BF),
        V((4, 32, CELLS_DEV), F32),
        V((512, 256), F32),
        V((2, 512, 256), BF),
        V((256, 128), I32),
        V((2, 128, 128), I32),
        V((512, 256), F32),
        V((2, 512, 256), BF),
        V((512, 128), F32),
        V((512, 128), F32),
        V((256, 128), F32),
        V((2, 2, 128, 128), I32),
        V((2, 256, 128), I32),
        V((512, 256), BF),
        V((2, 512, 256), BF),
        V((4, 2, CELLS_DEV), F32),
        V((2, 2, CELLS_DEV), F32),
        V((16, 1, 128), F32),
        V((16, 1, 128), F32),
        V((2, 1, 128), F32),
        V((2, 2, 2, 128, 256), BF),
        V((2, 256, 256), BF),
        V((2, 256, 256), BF),
        V((2, 16, 128), F32),
        V((2, 512, 256), BF),
        V((2, 256, 512), BF),
        V((2, 256, 128), F32),
        V((2, 256, 256), BF),
        V((2, 2, 2, 128, 256), BF),
        V((2, 256, 256), BF),
        D((11,)), D((6,)),
        pltpu.SemaphoreType.REGULAR((2,)),
        D((4,)), D((2, 4)),
        D, D((2,)), D((2,)), D((2,)),
        D((3,)), D((2,)),
        D((2,)), D((2,)),
    ]
    field = (REGIONS, 8, M)
    results = pl.pallas_call(
        kernel,
        out_shape=(V(field, F32), V(field, F32), V((2, CELLS_DEV), F32), V((1, 128), F32)),
        in_specs=[hbm] * (6 + len(consts)),
        out_specs=(vmem,) * 4,
        scratch_shapes=scratch,
        compiler_params=pltpu.CompilerParams(
            collective_id=0, has_side_effects=True, vmem_limit_bytes=66300000
        ),
        name="placement",
    )(*whole, cell_offset, *consts)
    S = jax.ShapeDtypeStruct
    field_x, field_y, force, energy, overflow = pl.pallas_call(
        finish,
        out_shape=(S(field, F32), S(field, F32), S((2, CELLS_DEV), F32), S((1, 1), F32), S((1, 1), F32)),
        in_specs=[vmem] * 4,
        out_specs=(hbm,) * 5,
        scratch_shapes=[V((2, 1, 1), F32), D((5,))],
        compiler_params=pltpu.CompilerParams(vmem_limit_bytes=4 * 1024 * 1024),
        name="finish",
    )(*results)
    return (field_x, field_y, force, energy.reshape(()), overflow.reshape(()))


def solution(mesh):
    both = ("slab", "cell")
    placed = (P(both),) * 5 + (P(None, both),)
    return jax.shard_map(
        body,
        mesh=mesh,
        in_specs=placed,
        out_specs=(P(None, both, None), P(None, both, None), P(None, both), P(), P()),
        check_vma=False,
    )
```

```python
import functools
import math

import jax
import jax.numpy as jnp
import numpy as np
from jax import lax
from jax.experimental import pallas as pl
from jax.experimental.pallas import tpu as pltpu
from jax.sharding import PartitionSpec as P

M = 2048
REGIONS = 4
SLABS = 128
CELLS_DEV = 512
BF = jnp.bfloat16
F32 = jnp.float32
I32 = jnp.int32
MESH = pl.DeviceIdType.MESH
STEP = math.pi / M
FAR = 98
NEXT = 14
NEAR = 1
LEAD = 4


def c_add(x,y): return (x[0]+y[0], x[1]+y[1])
def c_sub(x,y): return (x[0]-y[0], x[1]-y[1])
def c_turn(x,angle):
    c,s=math.cos(angle),math.sin(angle)
    if abs(s)<1e-12: return x if c>0 else (-x[0],-x[1])
    if abs(c)<1e-12: return (-x[1],x[0]) if s>0 else (x[1],-x[0])
    if abs(abs(c)-abs(s))<1e-12:
        h=abs(c); a,b=x[0],x[1]
        sc,ss=(1 if c>0 else -1),(1 if s>0 else -1)
        def lin(p,a,q,b):
            if p>0: return (a+b)*h if q>0 else (a-b)*h
            return (b-a)*h if q>0 else (a+b)*(-h)
        return (lin(sc,a,-ss,b), lin(ss,a,sc,b))
    return (x[0]*c-x[1]*s, x[0]*s+x[1]*c)
def c_fft(xs,sign):
    n=len(xs)
    if n==1: return xs
    even,odd=c_fft(xs[0::2],sign),c_fft(xs[1::2],sign)
    out=[None]*n
    for k in range(n//2):
        t=c_turn(odd[k],sign*2*math.pi*k/n)
        out[k],out[k+n//2]=c_add(even[k],t),c_sub(even[k],t)
    return out
def real_spectrum(d):
    n=len(d)
    if n==2:
        return {0:d[0]+d[1],1:(d[0],-d[1]),2:d[0]-d[1]}
    half=n//2
    out={}
    z=[c_turn((d[a],-d[a+half]),-math.pi*a/n) for a in range(half)]
    f=c_fft(z,-1)
    for m in range(half):
        k=1+4*m
        if k<n: out[k]=f[m]
        else: out[2*n-k]=(f[m][0],-f[m][1])
    s=[d[a]+d[a+half] for a in range(half)]
    e=[d[a]-d[a+half] for a in range(half)]
    q=half//2
    z=[c_turn((e[a],-e[a+q]),-2*math.pi*a/n) for a in range(q)]
    f=c_fft(z,-1)
    for l in range(q):
        m=1+4*l
        if m<=half: out[2*m]=f[l]
        else: out[2*(n-m)]=(f[l][0],-f[l][1])
    sub=real_full(s)
    for l,v in sub.items(): out[4*l]=v
    return out
def real_full(s):
    n=len(s)
    if n==2: return {0:s[0]+s[1],1:s[0]-s[1]}
    half=n//2
    p=[s[a]+s[a+half] for a in range(half)]
    e=[s[a]-s[a+half] for a in range(half)]
    out={}
    for l,v in real_full(p).items(): out[2*l]=v
    q=half//2
    if q==0: return out
    z=[c_turn((e[a],-e[a+q]),-2*math.pi*a/n) for a in range(q)] if q else []
    f=c_fft(z,-1)
    for k in range(q):
        l=1+4*k
        if l<=half: out[l]=f[k]
        else: out[n-l]=(f[k][0],-f[k][1])
    return out
def real_full_back(v,n):
    if n==2: return [v[0]+v[1],v[0]-v[1]]
    half=n//2; q=half//2
    p=real_full_back({l//2:x for l,x in v.items() if l%2==0},half)
    if n==4:
        g=[v[1]]
    else:
        g=[v[1+4*k] if 1+4*k<=half else (v[n-1-4*k][0],-v[n-1-4*k][1]) for k in range(q)]
    f=c_fft(g,1)
    odd=[None]*half
    for a in range(q):
        t=c_turn(f[a],2*math.pi*a/n)
        odd[a],odd[a+q]=t[0],-t[1]
    out=[None]*n
    for a in range(half):
        out[a],out[a+half]=p[a]+odd[a],p[a]-odd[a]
    return out
def real_back(y,n):
    half=n//2
    even=real_full_back({k//2:v for k,v in y.items() if k%2==0},n)
    g=[y[1+4*m] if 1+4*m<n else (y[2*n-1-4*m][0],-y[2*n-1-4*m][1]) for m in range(half)]
    f=c_fft(g,1)
    out=[None]*n
    for a in range(half):
        t=c_turn(f[a],math.pi*a/n)
        out[a],out[a+half]=even[a]+t[0],even[a+half]-t[1]
    return out


def split_np(table):
    high = table.astype(np.float32).astype(BF)
    low = (table - high.astype(np.float64)).astype(np.float32).astype(BF)
    return np.stack([high, low])


@functools.lru_cache(None)
def tables():
    pi = np.pi
    k2 = np.arange(64)[:, None]
    b = np.arange(128)[None, :]
    c1, s1 = np.cos(pi * k2 * (2 * b + 1) / 128), np.sin(pi * k2 * (2 * b + 1) / 128)
    c2, s2 = np.cos(pi * (k2 + 1) * (2 * b + 1) / 128), np.sin(pi * (k2 + 1) * (2 * b + 1) / 128)
    cm, sm = np.cos(pi * (2 * k2 + 1) * (2 * b + 1) / 256), np.sin(pi * (2 * k2 + 1) * (2 * b + 1) / 256)
    zero = np.zeros_like(c1)
    wc = np.block([[c1, s1], [c2, -s2]])
    wc0 = np.block([[c1, zero], [zero, cm]])
    ws = np.block([[s1, -c1], [s2, c2]])
    ws0 = np.block([[s1, zero], [zero, sm]])
    w = np.stack([split_np(m) for m in (ws, ws0, wc, wc0)]).reshape(2, 2, 2, 128, 256)
    wt = np.stack([np.concatenate(list(split_np(m.T)), axis=1) for m in (wc, wc0)])
    kap = np.arange(16)[:, None]
    ang = pi * kap * (2 * b + 1) / 4096
    tx = np.stack([np.cos(ang), np.sin(ang)]).astype(np.float32)
    p1 = np.arange(256)[:, None]
    d = np.arange(256)[None, :]
    cre, cim = np.cos(2 * pi * p1 * d / 512), -np.sin(2 * pi * p1 * d / 512)
    cim[0] = (-1.0) ** np.arange(256)
    cy = np.concatenate([cre, cim], 0)[:, np.arange(256).reshape(128, 2).T.reshape(-1)]
    ours = np.arange(128).reshape(4, 4, 2, 4).transpose(0, 2, 1, 3).reshape(-1)
    cy_fwd = split_np(cy)
    r = np.arange(8)
    angy = pi * p1 * (2 * r[None, :] + 1) / 4096
    ty = np.stack([np.tile(np.cos(angy), (1, 16)), np.tile(np.sin(angy), (1, 16))])[:, :, ours].astype(np.float32)
    p2 = np.arange(4)[None, :]
    rr = r[:, None]
    e0, e1 = pi * p2 * (2 * rr + 1) / 8, pi * (p2 + 1) * (2 * rr + 1) / 8
    em = pi * (2 * rr + 1) * (1 + 2 * p2) / 16
    z8 = np.zeros((8, 4))
    bc = (np.block([np.cos(e0), np.cos(e1)]), np.block([np.sin(e0), -np.sin(e1)]))
    bc0 = (np.block([np.cos(e0), z8]), np.block([z8, np.cos(em)]))
    bs = (np.block([np.sin(e0), np.sin(e1)]), np.block([-np.cos(e0), np.cos(e1)]))
    bs0 = (np.block([np.sin(e0), z8]), np.block([z8, np.sin(em)]))

    def wide(pair):
        return np.concatenate([np.kron(np.eye(16), part)[ours] for part in pair], 0)

    b_fwd = np.stack([np.concatenate(list(split_np(wide(m))), axis=1) for m in (bc, bc0)])
    b_inv = np.stack([split_np(wide(m).T) for m in (bc, bc0, bs, bs0)]).reshape(2, 2, 2, 128, 256)
    return w, wt, tx, cy_fwd, ty, b_fwd, b_inv


def dot(x, y):
    return lax.dot_general(x, y, (((1,), (0,)), ((), ())), preferred_element_type=F32)


def dot_nt(x, y):
    return lax.dot_general(x, y, (((1,), (1,)), ((), ())), preferred_element_type=F32)


def split(x):
    high = x.astype(BF)
    return high, (x - high.astype(F32)).astype(BF)


def dot3(x, y):
    return dot(x[0], y[0]) + (dot(x[0], y[1]) + dot(x[1], y[0]))


def dot3_nt(x, y):
    return dot_nt(x[0], y[0]) + (dot_nt(x[0], y[1]) + dot_nt(x[1], y[0]))


def encode(x, y):
    top = jnp.maximum(jnp.maximum(jnp.abs(x), jnp.abs(y)), 2.0**-31)
    exponent = jnp.minimum(jnp.floor(jnp.log2(top)), 31.0)
    scale = jnp.exp2(11.0 - exponent)

    def code(v):
        return jnp.clip(jnp.round(v * scale), -4095.0, 4095.0).astype(I32)

    high = jnp.left_shift(exponent.astype(I32) + 32, 26)
    return high | jnp.left_shift(code(y) & 0x1FFF, 13) | (code(x) & 0x1FFF)


def decode(word):
    scale = jnp.exp2(lax.shift_right_logical(word, 26).astype(F32) - 43.0)
    x = lax.shift_right_arithmetic(jnp.left_shift(word, 19), 19).astype(F32)
    y = lax.shift_right_arithmetic(jnp.left_shift(word, 6), 19).astype(F32)
    return x * scale, y * scale


@functools.lru_cache(None)
def send_order():
    rng = np.random.default_rng(0)
    every = [(dz, dy, dx, dc) for dz in range(8) for dy in range(4) for dx in range(4) for dc in range(2)]
    every = [d for d in every if any(d)]
    hops = {d: min(d[0], 8 - d[0]) + min(d[1], 4 - d[1]) + min(d[2], 4 - d[2]) + 0.5 * d[3] for d in every}
    return sorted(every, key=lambda d: (-hops[d], rng.random()))


def in_two(count, base=0):
    return [slice(base + k * count // 2, base + (k + 1) * count // 2) for k in range(2)]


@functools.lru_cache(None)
def first_devices():
    def reach(value, count):
        return min(value, count - value)

    found = []
    for slab in range(SLABS):
        for cell in range(2):
            y, x, z = slab // 32, slab // 8 % 4, slab // 2 % 4 * 2 + cell
            plane = reach(y, 4) + reach(x, 4)
            if reach(y, 4) + min(x, 1) + (0 if z < 3 else 3 if z == 3 else reach(z, 8)) <= NEAR:
                own = slab in (1, 2) and (slab, cell) != (2, 1)
                found.append((0 if own and plane == 0 else 1 + plane + reach(z, 8) - 0.5 * (slab % 2), slab, cell))
    return [(slab, cell) for _, slab, cell in sorted(found)]


def place():
    slab = lax.axis_index("slab")
    cell = lax.axis_index("cell")
    return slab, cell, lax.div(slab, 8), lax.rem(slab, 8) * 2 + cell


def device_at(plane, column):
    return (plane * 8 + lax.div(column, 2), lax.rem(column, 2))


def overlap(bins, low, high):
    return jnp.maximum(jnp.minimum(bins + 1.0, high) - jnp.maximum(bins, low), 0.0)


def kernel(
    row_h, col_h, width_h, height_h, region_h, offset_h,
    w_h, wt_h, tx_h, cyf_h, ty_h, bf_h, bi_h,
    field_x, field_y, force, sums,
    ci, co, pq, ym, yr, d2, zs, s1, r1, us, vs, gs, aw, pt, s2, r2, zx, fb, pf, pr, e1, e2, es,
    w, w2, wt, tx, cyf, cyi, ty, bf, bi, bi2,
    const_sem, in_sem, met, cell_s, cell_r, a1_s, a1_r, a2_s, a2_r, f_s, f_r, e_s, e_r,
):
    slab, cell, plane, column = place()
    me = plane * 16 + column
    mine, other = cell, 1 - cell
    has_prev = jnp.logical_and(cell == 0, slab > 0)
    has_next = slab < SLABS - 1
    barrier = pltpu.get_barrier_semaphore()

    own = [
        pltpu.make_async_copy(src, ci.at[mine, k], in_sem.at[k])
        for k, src in enumerate((row_h, col_h, width_h, height_h, region_h))
    ]
    own.append(pltpu.make_async_copy(offset_h, co.at[mine], in_sem.at[5]))
    for copy in own:
        copy.start()

    def signal_at(sem, device):
        pl.semaphore_signal(sem, inc=1, device_id=device, device_id_type=MESH)

    py, px = lax.div(plane, 4), lax.rem(plane, 4)
    ys = [lax.rem(py + k, 4) for k in range(4)]
    xs = [lax.rem(px + k, 4) for k in range(4)]
    x_line = [device_at(py * 4 + xs[k], column) for k in (2, 1, 3)]
    y_line = [device_at(ys[k] * 4 + px, column) for k in (2, 1, 3)]
    column_peers = [device_at(plane, lax.rem(column + i, 16)) for i in (8, 7, 9, 6, 10, 5, 11, 4, 12, 3, 13, 2, 14, 1, 15)]
    for device in column_peers + x_line + y_line:
        signal_at(barrier, device)

    @pl.when(has_prev)
    def _():
        signal_at(barrier, (slab - 1, 0))
        signal_at(barrier, (slab - 1, 1))

    z, core = lax.div(column, 4) * 2 + cell, lax.rem(lax.div(column, 2), 2)

    for copy in own:
        copy.wait()

    low_row = slab * 16 + cell * 8

    def cell_row_of(slot, k, which):
        return ci[slot, which, k : k + 1, :]

    def make_cells(slot, halves, masked):
        bins = lax.broadcasted_iota(I32, (128, 128), 0).astype(F32).astype(BF)
        line = lax.broadcasted_iota(I32, (16, 128), 0)
        rows = (jnp.bitwise_and(line, 3) + low_row).astype(F32)
        region_of = lax.shift_right_logical(line, 2)
        for k in range(4):
            at = slice(128 * k, 128 * k + 128)
            col = cell_row_of(slot, k, 1)
            high_bits = lax.shift_right_logical(col, 7)
            low_bits = (col - high_bits * 128).astype(F32).astype(BF)
            start = co[slot, 0:1, at]
            width = cell_row_of(slot, k, 2).astype(F32)
            first = (1.0 - start).astype(BF)
            last = ((start + width) - width).astype(BF)
            width = width.astype(BF)
            reach = bins - low_bits
            for far in range(2):
                if far:
                    reach = reach + BF(128.0)
                got = jnp.minimum(reach + first, (width - reach) + last)
                pq[slot, 128 * far : 128 * far + 128, at] = jnp.clip(got, BF(0.0), BF(1.0))
            start = co[slot, 1:2, at]
            end = start + cell_row_of(slot, k, 3).astype(F32)
            reach = rows - cell_row_of(slot, k, 0).astype(F32)
            here = cell_row_of(slot, k, 4) == region_of
            for half in range(halves):
                got = jnp.where(here, overlap(reach + 4.0 * half, start, end), 0.0)
                yr[slot, 16 * half : 16 * half + 16, at] = got.astype(BF).astype(F32)
                for a in range(16):
                    to = slice(256 * half + 16 * a, 256 * half + 16 * a + 16)
                    masked[to, at] = jnp.where(high_bits == a, got, 0.0).astype(BF)

    def send(src, dst, s_sem, r_sem, device):
        return pltpu.make_async_remote_copy(
            src_ref=src, dst_ref=dst, send_sem=s_sem, recv_sem=r_sem, device_id=device, device_id_type=MESH
        )

    pl.semaphore_wait(barrier, 21 + has_next.astype(I32))
    partner = (slab, other)
    give = [
        send(ci.at[mine], ci.at[mine], cell_s.at[0], cell_r.at[0, mine], partner),
        send(co.at[mine], co.at[mine], cell_s.at[1], cell_r.at[1, mine], partner),
    ]
    give_next = [
        send(ci.at[mine], ci.at[2 + mine], cell_s.at[2], cell_r.at[0, 2 + mine], (slab + 1, 0)),
        send(co.at[mine], co.at[2 + mine], cell_s.at[3], cell_r.at[1, 2 + mine], (slab + 1, 0)),
    ]
    for copy in give:
        copy.start()

    @pl.when(has_next)
    def _():
        for copy in give_next:
            copy.start()

    for device in x_line:
        signal_at(met.at[0], device)

    fetched = [
        pltpu.make_async_copy(src, dst, const_sem.at[k])
        for k, (src, dst) in enumerate(
            (
                (tx_h, tx), (wt_h, wt), (w_h, w), (w_h.at[:, 0, 0], w2.at[:, 0:128]), (w_h.at[:, 0, 0], w2.at[:, 128:256]),
                (cyf_h, cyf), (ty_h, ty), (bf_h, bf), (bi_h, bi),
                (bi_h.at[:, 0, 0], bi2.at[:, 0:128]), (bi_h.at[:, 0, 0], bi2.at[:, 128:256]),
            )
        )
    ]
    for copy in fetched:
        copy.start()

    def arrive(slot):
        send(ci.at[slot], ci.at[slot], cell_s.at[0], cell_r.at[0, slot], partner).wait_recv()
        send(co.at[slot], co.at[slot], cell_s.at[1], cell_r.at[1, slot], partner).wait_recv()

    make_cells(mine, 2, ym.at[0])
    for rows in in_two(512):
        d2[rows] = dot_nt(ym[0, rows], pq[mine])
    arrive(other)
    pl.semaphore_wait(met.at[0], 3)
    for device in y_line:
        signal_at(met.at[1], device)
    make_cells(other, 2, ym.at[0])
    for rows in in_two(512):
        d2[rows] += dot_nt(ym[0, rows], pq[other])

    zero8 = jnp.zeros((8, 128), F32)
    lane = lax.broadcasted_iota(I32, (1, 128), 1)
    first_group = lane < 32

    def x_forward(half, excess, area):
        here = []
        for a in range(16):
            at = 256 * half + 16 * a
            value = d2[at : at + 16, 0:128]
            if a:
                value = value + d2[at - 16 : at, 128:256]
            here.append(value)
            over = jnp.maximum(value - 1.0, 0.0)
            excess = excess + (over[0:8] + over[8:16])
            area = area + (value[0:8] + value[8:16])
        got = real_spectrum(here)
        for kap in range(16):
            at = slice(256 * half + 16 * kap, 256 * half + 16 * kap + 16)
            if kap == 0:
                pair = (got[0], got[16])
            else:
                (re, im), c, s = got[kap], tx[0, kap : kap + 1, :], tx[1, kap : kap + 1, :]
                pair = (re * c + im * s, im * c - re * s)
            for part, value in enumerate(pair):
                parts = split(value)
                for k in range(2):
                    zs[k, at, 128 * part : 128 * part + 128] = parts[k]

        return excess, area

    def x_product_forward(rows, kind):
        got = dot(zs[0, rows], wt[kind])
        return got[:, 0:128] + (got[:, 128:256] + dot(zs[1, rows], wt[kind, :, 0:128]))

    fetched[0].wait()
    fetched[1].wait()
    excess, area = x_forward(1, zero8, zero8)

    @pl.when(has_prev)
    def _():
        for k in range(2):
            arrive(2 + k)
        for k in range(2):
            make_cells(2 + k, 1, ym.at[1 + k])
        for rows in in_two(256):
            d2[rows] += dot_nt(ym[1, rows], pq[2]) + dot_nt(ym[2, rows], pq[3])

    excess, area = x_forward(0, excess, area)
    for rows in in_two(512):
        gs[rows] = x_product_forward(rows, 0)
    for half in range(2):
        first = slice(256 * half, 256 * half + 16)
        gs[first] = x_product_forward(first, 1)
    tiles = []
    for t in range(4):
        rows = [gs[256 * half + 16 * kap : 256 * half + 16 * kap + 16] for kap in range(4 * t, 4 * t + 4) for half in range(2)]
        tiles.append(jnp.concatenate(rows, axis=0).T)
    for t in range(2):
        s1[128 * t : 128 * t + 128, :] = encode(tiles[t], tiles[t + 2])

    pl.semaphore_wait(met.at[1], 3)
    planes = [[ys[dy] * 4 + xs[dx] for dx in range(4)] for dy in range(4)]
    z_there = [lax.rem(z + k, 8) for k in range(8)]
    z_parts = [(lax.div(k, 2), lax.rem(k, 2)) for k in z_there]

    def exchange(src, dst, s_sem, r_sem, part=slice(None)):
        for dz, dy, dx, dc in send_order()[part]:
            zh, zl = z_parts[dz]
            slab_to = planes[dy][dx] * 8 + (zh * 2 + (core if dc == 0 else 1 - core))
            send(src(slab_to, zl), dst, s_sem, r_sem, (slab_to, zl)).start()

    def reach(value, count):
        return jnp.minimum(value, count - value)

    y_reach, x_reach = [reach(v, 4) for v in ys], [jnp.minimum(v, 1) for v in xs]
    z_reach = [jnp.where(v < 3, 0, jnp.where(v == 3, 3, reach(v, 8))) for v in z_there]

    def exchange_rest(src, dst, s_sem, r_sem, part=slice(None)):
        for dz, dy, dx, dc in send_order()[part]:
            zh, zl = z_parts[dz]
            slab_to = planes[dy][dx] * 8 + (zh * 2 + (core if dc == 0 else 1 - core))
            start = send(src(slab_to, zl), dst, s_sem, r_sem, (slab_to, zl)).start
            pl.when(y_reach[dy] + x_reach[dx] + z_reach[dz] > NEAR)(start)

    def exchange_first(src, dst, s_sem, r_sem, part=slice(None)):
        for slab_to, cell_to in first_devices()[part]:
            pl.when(me != slab_to * 2 + cell_to)(send(src(slab_to, cell_to), dst, s_sem, r_sem, (slab_to, cell_to)).start)

    exchange(lambda slab_to, cell_to: s1.at[pl.ds(slab_to * 2 + cell_to, 1)], r1.at[cell, pl.ds(slab, 1)], a1_s, a1_r.at[cell])
    r1[cell, pl.ds(slab, 1), :] = s1[pl.ds(me, 1), :]

    tile, k2c = lax.div(me, 128), lax.rem(me, 128)
    lower = k2c < 64
    group = lax.div(lane, 32)
    order = lax.rem(lane, 8)

    def q_of(h):
        kap = 4 * (tile + 2 * h) + group
        return jnp.where(
            kap == 0,
            jnp.where(lower, 32 * k2c, 16 + 32 * (k2c - 64)),
            jnp.where(lower, kap + 32 * k2c, 32 - kap + 32 * (k2c - 64)),
        )

    qs = [q_of(h) for h in range(2)]

    def weigh(i, carry):
        at = pl.multiple_of(i * 16, 16)
        p1 = lax.broadcasted_iota(I32, (16, 128), 0) + at
        up = order < 4
        p = jnp.where(up, p1 + 512 * order, 512 - p1 + 512 * (order - 4))
        p = jnp.where(jnp.logical_and(p1 == 0, jnp.logical_not(up)), 256 + 512 * (order - 4), p)
        p_float = p.astype(F32)
        pt[pl.ds(at, 16), :] = p_float
        for h in range(2):
            q_float = qs[h].astype(F32)
            k2 = p_float * p_float + q_float * q_float
            scale = jnp.where(p == 0, 1.0 / M, 2.0 / M) * jnp.where(qs[h] == 0, 1.0 / M, 2.0 / M) * (1.0 / STEP)
            aw[pl.ds(256 * h + at, 16), :] = jnp.where(k2 == 0.0, 0.0, scale / jnp.where(k2 == 0.0, 1.0, k2))
        return carry

    lax.fori_loop(0, 16, weigh, 0)

    for copy in fetched[2:]:
        copy.wait()
    for k in range(2):
        for i in range(4):
            for j in range(2):
                rows, lanes = slice(128 * i, 128 * i + 128), slice(128 * j, 128 * j + 128)
                cyi[k, lanes, rows] = cyf[k, rows, lanes].T
    def half_arrived(k):
        for count, here in ((127, cell == k), (128, cell != k)):

            @pl.when(here)
            def _(count=count):
                send(s1.at[pl.ds(0, count)], r1.at[k, pl.ds(0, count)], a1_s, a1_r.at[k], partner).wait_recv()

    def half_of(k):
        high, low = zip(*(split(v) for v in decode(r1[k])))
        whole = (jnp.concatenate(high, axis=1), jnp.concatenate(low, axis=1))
        at = slice(128 * k, 128 * k + 128)
        return [(rows, dot3((cyf[0, rows, at], cyf[1, rows, at]), whole)) for rows in in_two(512)]

    half_arrived(1)
    for rows, got in half_of(1):
        us[rows] = got
    half_arrived(0)
    send(s1.at[pl.ds(0, 255)], s1.at[pl.ds(0, 255)], a1_s, a1_r.at[0], partner).wait_send()

    for rows, got in half_of(0):
        us[rows] += got

    def y_chunk(i, carry):
        at = i * 16
        c, s = ty[0, pl.ds(at, 16), :], ty[1, pl.ds(at, 16), :]
        for h in range(2):
            lanes = slice(128 * h, 128 * h + 128)
            re, im = us[pl.ds(at, 16), lanes], us[pl.ds(256 + at, 16), lanes]
            for half, value in enumerate((re * c + im * s, im * c - re * s)):
                parts = split(value)
                for k in range(2):
                    vs[k, pl.ds(256 * h + at, 16), 128 * half : 128 * half + 128] = parts[k]
        return carry

    for i in range(16):
        y_chunk(i, 0)

    def y_out(rows, table):
        got = dot(vs[0, rows], table)
        return got[:, 0:128] + (got[:, 128:256] + dot(vs[1, rows], table[:, 0:128]))

    for rows in in_two(512):
        gs[rows] = y_out(rows, bf[0])
    top_row = lax.broadcasted_iota(I32, (16, 1), 0) == 0
    for h in range(2):
        at = slice(256 * h, 256 * h + 16)
        gs[at, :] = jnp.where(top_row, y_out(at, bf[1]), gs[at, :])

    q_floats = [q.astype(F32) for q in qs]

    def scale_chunk(i, energy):
        at = i * 16
        p_float = pt[pl.ds(at, 16), :]
        for h in range(2):
            value = gs[pl.ds(256 * h + at, 16), :]
            weighted = value * aw[pl.ds(256 * h + at, 16), :]
            work = weighted * value
            energy = energy + (work[0:8] + work[8:16])
            for f, part in enumerate((weighted * q_floats[h], weighted * p_float)):
                parts = split(part)
                for k in range(2):
                    vs[f, pl.ds(256 * h + at, 16), 128 * k : 128 * k + 128] = parts[k]
        return energy

    energy = zero8
    for i in range(16):
        energy = scale_chunk(i, energy)

    def top_rows(f, h):
        at = slice(256 * h, 256 * h + 16)
        return dot3((vs[f, at, 0:128], vs[f, at, 128:256]), (bi[f, 1, 0], bi[f, 1, 1]))

    def turned(values, c, s):
        re, im = values[:, 0:128], values[:, 128:256]
        return [split(value) for value in (re * c - im * s, re * s + im * c)]

    def keep_turned(values, h, at):
        for half in range(2):
            for k in range(2):
                zs[k, pl.ds(256 * half + at, values[half][k].shape[0]), 128 * h : 128 * h + 128] = values[half][k]

    def copies_of(f):
        return (
            lambda slab_to, cell_to: s2.at[f, cell_to, pl.ds(slab_to, 1)], r2.at[f, pl.ds(me, 1)], a2_s.at[f], a2_r.at[f]
        )

    for rows in in_two(512):
        us[rows] = dot(vs[0, rows], bi2[0]) + dot(vs[0, rows, 0:128], bi[0, 0, 1])
    for h in range(2):
        at = slice(256 * h, 256 * h + 16)
        us[at, :] = jnp.where(top_row, top_rows(0, h), us[at, :])
    for i in range(16):
        for h in range(2):
            at = slice(16 * i, 16 * i + 16)
            keep_turned(turned(us[256 * h + 16 * i : 256 * h + 16 * i + 16, :], ty[0, at, :], ty[1, at, :]), h, 16 * i)
    def back_in_y(f):
        for k, rows in enumerate(in_two(256)):
            got = dot3((cyi[0, rows], cyi[1, rows]), (zs[0], zs[1]))
            s2[f, k] = encode(got[:, 0:128], got[:, 128:256])

    back_in_y(0)
    r2[0, pl.ds(me, 1), :] = s2[0, cell, pl.ds(slab, 1), :]

    exchange_first(*copies_of(0), part=slice(0, LEAD))
    for i in range(2):
        at = 128 * i
        rows = [vs[1, 256 * h + at : 256 * h + at + 128, :] for h in range(2)]
        c, s = ty[0, at : at + 128, :], ty[1, at : at + 128, :]
        top = [top_rows(1, h) for h in range(2)] if i == 0 else None
        got = [dot(r, bi2[1]) + dot(r[:, 0:128], bi[1, 0, 1]) for r in rows]
        values = []
        for h in range(2):
            value = got[h]
            if i == 0:
                value = jnp.concatenate([jnp.where(top_row, top[h], value[0:16]), value[16:]], axis=0)
            values.append(turned(value, c, s))
        count = len(first_devices()) - LEAD
        exchange_first(*copies_of(0), part=slice(LEAD + count // 2 * i, LEAD + count // 2 if i == 0 else None))
        exchange_rest(*copies_of(0), part=slice(FAR // 2 * i, FAR // 2 * i + FAR // 2))
        for h in range(2):
            keep_turned(values[h], h, at)

    back_in_y(1)
    exchange_first(*copies_of(1))
    def total(x):
        return jnp.sum(jnp.sum(x, axis=1, keepdims=True), axis=0, keepdims=True)

    row = jnp.where(
        lane == 0, total(excess), jnp.where(lane == 1, total(area), total(energy) * (1.0 / (STEP * M * M)))
    )
    es[0] = row
    e1[plane] = row
    for i in range(1, 16):
        send(es.at[0], e1.at[plane], e_s.at[0], e_r.at[0], device_at(lax.rem(plane + i, 16), column)).start()
    exchange_rest(*copies_of(1), part=slice(0, NEXT))
    exchange_rest(*copies_of(0), part=slice(FAR, None))
    exchange_rest(*copies_of(1), part=slice(NEXT, None))
    r2[1, pl.ds(me, 1), :] = s2[1, cell, pl.ds(slab, 1), :]

    def push(slot, f, halves):
        got = dot(fb[f, 0 : 256 * halves], pq[slot])
        for k in range(4):
            at = slice(128 * k, 128 * k + 128)
            high_bits = lax.shift_right_logical(cell_row_of(slot, k, 1), 7)
            force = jnp.zeros((1, 128), F32)
            for half in range(halves):
                kept = got[256 * half : 256 * half + 16, at]
                for a in range(1, 16):
                    kept = jnp.where(high_bits == a, got[256 * half + 16 * a : 256 * half + 16 * a + 16, at], kept)
                force = force + jnp.sum(kept * yr[slot, 16 * half : 16 * half + 16, at], axis=0, keepdims=True)
            pf[slot, f : f + 1, at] = force

    def x_gather(f):
        for t in range(2):
            for h, value in enumerate(decode(r2[f, 128 * t : 128 * t + 128, :])):
                parts = split(value.T)
                for k in range(2):
                    for j in range(4):
                        for half in range(2):
                            to = 256 * half + 16 * (4 * (t + 2 * h) + j)
                            zx[to : to + 16, 128 * k : 128 * k + 128] = parts[k][32 * j + 16 * half : 32 * j + 16 * half + 16]

    def x_product(f, halves):
        base, count = 256 * halves[0], 256 * len(halves)
        for rows in in_two(count, base):
            us[rows, :] = dot(zx[rows], w2[f]) + dot(zx[rows, 0:128], w[f, 0, 1])
        for half in halves:
            first = slice(256 * half, 256 * half + 16)
            us[first, :] = dot3((zx[first, 0:128], zx[first, 128:256]), (w[f, 1, 0], w[f, 1, 1]))

    def x_inverse(f, out, half):
        base = 256 * half
        got = {}
        for kap in range(16):
            rows = slice(base + 16 * kap, base + 16 * kap + 16)
            re, im = us[rows, 0:128], us[rows, 128:256]
            if kap == 0:
                got[0], got[16] = re, im
            else:
                c, s = tx[0, kap : kap + 1, :], tx[1, kap : kap + 1, :]
                got[kap] = (re * c - im * s, re * s + im * c)
        for a, value in enumerate(real_back(got, 16)):
            lanes = slice(128 * a, 128 * a + 128)
            for g in range(REGIONS):
                out[g, 4 * half : 4 * half + 4, lanes] = value[4 * g : 4 * g + 4]
            near = value.astype(BF)
            fb[f, base + 16 * a : base + 16 * a + 16, 0:128] = near
            if a:
                fb[f, base + 16 * a - 16 : base + 16 * a, 128:256] = near
        fb[f, base + 240 : base + 256, 128:256] = jnp.zeros((16, 128), BF)

    def give_back(slot, device, sem, into):
        return send(pf.at[slot], pr.at[into], f_s.at[sem], f_r.at[into], device)

    def arrived(f):
        whole = send(r2.at[f, pl.ds(0, 255)], r2.at[f, pl.ds(0, 255)], a2_s.at[f], a2_r.at[f], partner)
        whole.wait_recv()
        whole.wait_send()

    sums_wait = send(e1.at[pl.ds(0, 15)], e1.at[pl.ds(0, 15)], e_s.at[0], e_r.at[0], partner)
    sums_wait.wait_recv()
    sums_wait.wait_send()
    row = jnp.sum(e1[...], axis=0)
    es[1] = row
    e2[column] = row
    for i in range(1, 16):
        send(es.at[1], e2.at[column], e_s.at[1], e_r.at[1], device_at(plane, lax.rem(column + i, 16))).start()
    arrived(0)
    x_gather(0)
    x_product(0, (0, 1))
    for half in range(2):
        x_inverse(0, field_x, half)

    @pl.when(has_prev)
    def _():
        for k in range(2):
            push(2 + k, 0, 1)

    push(other, 0, 2)
    arrived(1)
    x_gather(1)
    x_product(1, (0,))
    x_inverse(1, field_y, 0)

    @pl.when(has_prev)
    def _():
        for k in range(2):
            push(2 + k, 1, 1)
            give_back(2 + k, (slab - 1, k), 1 + k, 1).start()

    x_product(1, (1,))
    x_inverse(1, field_y, 1)
    push(other, 1, 2)
    give_back(other, partner, 0, 0).start()
    for f in range(2):
        push(mine, f, 2)

    @pl.when(jnp.logical_not(has_next))
    def _():
        pr[1] = jnp.zeros((2, CELLS_DEV), F32)

    give_back(other, partner, 0, 0).wait_recv()

    @pl.when(has_next)
    def _():
        give_back(other, partner, 0, 1).wait_recv()

    force[...] = pf[mine] + pr[0] + pr[1]

    send(e2.at[pl.ds(0, 15)], e2.at[pl.ds(0, 15)], e_s.at[1], e_r.at[1], partner).wait()
    sums[...] = jnp.sum(e2[...], axis=0)

    give_back(other, partner, 0, 0).wait_send()
    for copy in give:
        copy.wait_send()

    @pl.when(has_prev)
    def _():
        for k in range(2):
            give_back(2 + k, (slab - 1, k), 1 + k, 1).wait_send()

    @pl.when(has_next)
    def _():
        for copy in give_next:
            copy.wait_send()


def finish(field_x, field_y, force, sums, out_x, out_y, out_force, energy, overflow, small, sem):
    pairs = ((field_x, out_x), (field_y, out_y), (force, out_force), (small.at[0], energy), (small.at[1], overflow))
    copies = [pltpu.make_async_copy(src, dst, sem.at[k]) for k, (src, dst) in enumerate(pairs)]
    for copy in copies[:3]:
        copy.start()
    row = sums[...]
    small[0] = row[:, 2:3]
    small[1] = row[:, 0:1] / row[:, 1:2]
    for copy in copies[3:]:
        copy.start()
    for copy in copies:
        copy.wait()


def body(cell_row, cell_col, cell_width, cell_height, cell_region, cell_offset):
    consts = [jnp.asarray(t) for t in tables()]
    whole = [v.reshape(4, 128) for v in (cell_row, cell_col, cell_width, cell_height, cell_region)]
    vmem = pl.BlockSpec(memory_space=pltpu.VMEM)
    hbm = pl.BlockSpec(memory_space=pltpu.HBM)
    V = pltpu.VMEM
    D = pltpu.SemaphoreType.DMA
    scratch = [
        V((4, 5, 4, 128), I32),
        V((4, 2, CELLS_DEV), F32),
        V((4, 256, 512), BF),
        V((3, 512, 512), BF),
        V((4, 32, CELLS_DEV), F32),
        V((512, 256), F32),
        V((2, 512, 256), BF),
        V((256, 128), I32),
        V((2, 128, 128), I32),
        V((512, 256), F32),
        V((2, 512, 256), BF),
        V((512, 128), F32),
        V((512, 128), F32),
        V((256, 128), F32),
        V((2, 2, 128, 128), I32),
        V((2, 256, 128), I32),
        V((512, 256), BF),
        V((2, 512, 256), BF),
        V((4, 2, CELLS_DEV), F32),
        V((2, 2, CELLS_DEV), F32),
        V((16, 1, 128), F32),
        V((16, 1, 128), F32),
        V((2, 1, 128), F32),
        V((2, 2, 2, 128, 256), BF),
        V((2, 256, 256), BF),
        V((2, 256, 256), BF),
        V((2, 16, 128), F32),
        V((2, 512, 256), BF),
        V((2, 256, 512), BF),
        V((2, 256, 128), F32),
        V((2, 256, 256), BF),
        V((2, 2, 2, 128, 256), BF),
        V((2, 256, 256), BF),
        D((11,)), D((6,)),
        pltpu.SemaphoreType.REGULAR((2,)),
        D((4,)), D((2, 4)),
        D, D((2,)), D((2,)), D((2,)),
        D((3,)), D((2,)),
        D((2,)), D((2,)),
    ]
    field = (REGIONS, 8, M)
    results = pl.pallas_call(
        kernel,
        out_shape=(V(field, F32), V(field, F32), V((2, CELLS_DEV), F32), V((1, 128), F32)),
        in_specs=[hbm] * (6 + len(consts)),
        out_specs=(vmem,) * 4,
        scratch_shapes=scratch,
        compiler_params=pltpu.CompilerParams(
            collective_id=0, has_side_effects=True, vmem_limit_bytes=66300000
        ),
        name="placement",
    )(*whole, cell_offset, *consts)
    S = jax.ShapeDtypeStruct
    field_x, field_y, force, energy, overflow = pl.pallas_call(
        finish,
        out_shape=(S(field, F32), S(field, F32), S((2, CELLS_DEV), F32), S((1, 1), F32), S((1, 1), F32)),
        in_specs=[vmem] * 4,
        out_specs=(hbm,) * 5,
        scratch_shapes=[V((2, 1, 1), F32), D((5,))],
        compiler_params=pltpu.CompilerParams(vmem_limit_bytes=4 * 1024 * 1024),
        name="finish",
    )(*results)
    return (field_x, field_y, force, energy.reshape(()), overflow.reshape(()))


def solution(mesh):
    both = ("slab", "cell")
    placed = (P(both),) * 5 + (P(None, both),)
    return jax.shard_map(
        body,
        mesh=mesh,
        in_specs=placed,
        out_specs=(P(None, both, None), P(None, both, None), P(None, both), P(), P()),
        check_vma=False,
    )
```
